256 devices in a mesh: group: 2 (over z), expert: 128 (over x, y, core).
Axes of the slice: x: 8, y: 8, z: 2, core: 2. Of those that a mesh axis runs over, the one named last changes fastest.
The devices are a block of a 8x8x16 slice.
Arguments:
- query: bfloat16 [256, 2048], P(('group', 'expert')), parts along dimension 0, may hold values from -600 to 600
- key_new: bfloat16 [256, 2048], P(('group', 'expert')), parts along dimension 0, may hold values from -6 to 6
- value_new: bfloat16 [256, 2048], P(('group', 'expert')), parts along dimension 0, may hold values from -6 to 6
- key_cache: bfloat16 [256, 256, 2048], P(('group', 'expert')), parts along dimension 0, may hold values from -6 to 6
- value_cache: bfloat16 [256, 256, 2048], P(('group', 'expert')), parts along dimension 0, may hold values from -6 to 6
- lengths: int32 [256], P(('group', 'expert')), parts along dimension 0, may hold values from 1 to 256
- hidden: bfloat16 [256, 2048], P(('group', 'expert')), parts along dimension 0, may hold values from -6 to 6
- routes: int32 [256], P('group'), parts along dimension 0, may hold values from 0 to 31, as said below
- w_out: bfloat16 [2048, 2048], P(None, 'expert'), may hold values from -0.125 to 0.125
- ln_gain: bfloat16 [2048], replicated, may hold values from 0.099609375 to 1.8984375
- router: bfloat16 [2048, 32], replicated, may hold values from -0.125 to 0.125
- shared_up: bfloat16 [2048, 8192], P(None, 'expert'), may hold values from -0.125 to 0.125
- shared_down: bfloat16 [8192, 2048], P('expert'), may hold values from -0.0625 to 0.0625
- expert_up: bfloat16 [2048, 131072], P(None, 'expert'), may hold values from -0.125 to 0.125
- expert_down: bfloat16 [131072, 2048], P('expert'), may hold values from -0.09375 to 0.09375
Outputs:
- layer_out: bfloat16 [256, 2048], P(('group', 'expert')), parts along dimension 0
The draws below stay inside these ranges and needn't reach their ends.
There are 2 independent parts, one for each index of `group`. The reference program is written for one: setup_inputs(seed, part) draws one part's arguments, and reference() takes and returns one part's arrays. A program takes and returns all parts, laid end to end along the dimension named above; an argument that names none is the same for every part. Nothing has to cross between parts.
Inputs may be any that keep to these rules, and one draw needn't show every extreme that they name: `routes`: no expert is named by more than 16 tokens of the group, and in every draw some expert is named by exactly 16.
All inputs are finite; a program needn't handle non-finite values.
Results may differ from the reference program's by a relative error of at most 0.0085.
Values may be sent and summed in bfloat16 or wider, within the bound.
A program may use at most 64 MiB of HBM per device.

```python
import math
import jax
import jax.numpy as jnp
from jax import lax

D = 2048
HEADS = 16
HEAD_DIM = 128
FF = 4096
EXPERTS = 32
SHARED_FF = 8192
CACHE = 256
S = 128
CAP = 16


def draw_query(key, part):
    base = jnp.clip(jax.random.normal(key, (S, D), jnp.float32), -6.0, 6.0)
    return base.astype(jnp.bfloat16)


def draw_routes(key, part):
    order_key = jax.random.fold_in(key, 11)
    hot_key = jax.random.fold_in(key, 12)
    second_key = jax.random.fold_in(key, 13)
    count_key = jax.random.fold_in(key, 14)
    shuffle_key = jax.random.fold_in(key, 15)
    offset_key = jax.random.fold_in(key, 16)
    token_order = jax.random.permutation(order_key, S)
    hottest = jax.random.randint(hot_key, (), 0, EXPERTS)
    second = (hottest + 1 + jax.random.randint(second_key, (), 0, EXPERTS - 1)) % EXPERTS
    second_count = jax.random.randint(count_key, (), 1, CAP + 1)
    expert_index = jnp.arange(EXPERTS, dtype=jnp.int32)
    shuffled = jax.random.permutation(shuffle_key, EXPERTS).astype(jnp.int32)
    shuffled = jnp.where(expert_index == hottest, EXPERTS, shuffled)
    shuffled = jnp.where(expert_index == second, EXPERTS + 1, shuffled)
    others = jnp.argsort(shuffled, stable=True).astype(jnp.int32)
    offset = jax.random.randint(offset_key, (), 0, EXPERTS - 2)
    position = jnp.arange(S, dtype=jnp.int32)
    remaining = (position - CAP - second_count + offset) % (EXPERTS - 2)
    chosen = jnp.where(position < CAP, hottest, jnp.where(position < CAP + second_count, second, others[remaining]))
    return jnp.zeros((S,), jnp.int32).at[token_order].set(chosen.astype(jnp.int32))


def place_ends(entries, own_key, smallest, largest):
    shape = entries.shape
    place = [jax.random.randint(jax.random.fold_in(own_key, axis), (), 0, shape[axis]) for axis in range(len(shape))]
    entries = entries.at[tuple(place)].set(smallest)
    longest = shape.index(max(shape))
    place[longest] = (place[longest] + 1) % shape[longest]
    return entries.at[tuple(place)].set(largest)


def block_levels(own_key, shape, pieces, low, top_value):
    loudness = 1.0
    for dim, parts in pieces:
        heights = jax.random.uniform(jax.random.fold_in(jax.random.fold_in(own_key, 6), dim), (parts,), jnp.float32, low / len(pieces), top_value / len(pieces))
        loudness = loudness * jnp.repeat(jnp.exp(heights), shape[dim] // parts).reshape((-1,) + (1,) * (len(shape) - 1 - dim))
    return loudness


def gaussian(stream_key, shape, width, bound, pieces=(), held_as=jnp.bfloat16):
    drawn = jax.random.normal(stream_key, shape, jnp.float32) * width
    if len(pieces) > 0:
        drawn = block_levels(stream_key, shape, pieces, -0.22, 0.18) * drawn
    return jnp.clip(drawn, min=-bound, max=bound).astype(held_as)


def setup_inputs(seed: int = 0, part: int = 0) -> dict:
    keys = jax.random.split(jax.random.key(seed), 16)
    part_splits = jax.random.split(jax.random.fold_in(keys[15], part), 16)
    return {
        "query": draw_query(jax.random.fold_in(jax.random.fold_in(keys[15], part), 71), part),
        "key_new": gaussian(part_splits[1], (S, D), 1.0, 6.0, ((0, 128),)),
        "value_new": gaussian(part_splits[2], (S, D), 1.0, 6.0, ((0, 128),)),
        "key_cache": gaussian(part_splits[3], (S, CACHE, D), 1.0, 6.0, ((0, 128),)),
        "value_cache": gaussian(part_splits[4], (S, CACHE, D), 1.0, 6.0, ((0, 128),)),
        "lengths": place_ends(jax.random.randint(part_splits[5], (S,), 1, CACHE + 1), jax.random.fold_in(part_splits[5], 1), 1, CACHE).astype(jnp.int32),
        "hidden": gaussian(part_splits[6], (S, D), 1.0, 6.0, ((0, 128),)),
        "routes": draw_routes(jax.random.fold_in(jax.random.fold_in(keys[15], part), 71), part),
        "w_out": gaussian(keys[8], (D, D), D ** -0.5, 0.125, ((1, 128),)),
        "ln_gain": jnp.clip(1.0 + 0.18 * jax.random.normal(keys[9], (D,), jnp.float32), 0.099609375, 1.8984375).astype(jnp.bfloat16),
        "router": gaussian(keys[10], (D, EXPERTS), D ** -0.5, 0.125),
        "shared_up": gaussian(keys[11], (D, SHARED_FF), D ** -0.5, 0.125, ((1, 128),)),
        "shared_down": gaussian(keys[12], (SHARED_FF, D), SHARED_FF ** -0.5, 0.0625, ((0, 128),)),
        "expert_up": gaussian(keys[13], (D, EXPERTS * FF), D ** -0.5, 0.125, ((1, 128),)),
        "expert_down": gaussian(keys[14], (EXPERTS * FF, D), FF ** -0.5, 0.09375, ((0, 128),)),
    }


def attend_one(packed):
    query_row, key_rows, value_rows, key_self, value_self, valid = packed
    scale_factor = 1.0 / math.sqrt(HEAD_DIM)
    head_query = query_row.astype(jnp.float32).reshape(HEADS, HEAD_DIM)
    head_keys = key_rows.astype(jnp.float32).reshape(CACHE, HEADS, HEAD_DIM)
    head_values = value_rows.astype(jnp.float32).reshape(CACHE, HEADS, HEAD_DIM)
    scores = jnp.einsum('hd,chd->hc', head_query, head_keys) * scale_factor
    own_score = lax.optimization_barrier(jnp.sum(head_query * key_self.astype(jnp.float32).reshape(HEADS, HEAD_DIM), axis=1)) * scale_factor
    positions = jnp.arange(CACHE, dtype=jnp.int32)
    scores = jnp.where(positions[None, :] < valid, scores, -1e+30)
    top_score = jnp.maximum(lax.optimization_barrier(jnp.max(scores, axis=1)), own_score)
    weights = jnp.exp(scores - top_score[:, None])
    own_weight = jnp.exp(own_score - top_score)
    normalizer = lax.optimization_barrier(jnp.sum(weights, axis=1)) + own_weight
    weights = lax.optimization_barrier((weights / normalizer[:, None]).astype(jnp.bfloat16)).astype(jnp.float32)
    own_weight = lax.optimization_barrier((own_weight / normalizer).astype(jnp.bfloat16)).astype(jnp.float32)
    mixed_values = jnp.einsum('hc,chd->hd', weights, head_values)
    mixed_values = mixed_values + own_weight[:, None] * value_self.astype(jnp.float32).reshape(HEADS, HEAD_DIM)
    return mixed_values.reshape(D).astype(jnp.bfloat16)

def reference(query, key_new, value_new, key_cache, value_cache, lengths, hidden, routes, w_out, ln_gain, router, shared_up, shared_down, expert_up, expert_down):
    attended = lax.map(attend_one, (query, key_cache, value_cache, key_new, value_new, lengths))
    projected = jnp.dot(attended, w_out, preferred_element_type=jnp.float32).astype(jnp.bfloat16)
    projected = lax.optimization_barrier(projected).astype(jnp.float32)
    residual = hidden.astype(jnp.float32) + projected
    centered = residual - lax.optimization_barrier(jnp.mean(residual, axis=1, keepdims=True))
    variance = lax.optimization_barrier(jnp.mean(centered * centered, axis=1, keepdims=True))
    normed = (centered / jnp.sqrt(jnp.maximum(variance, 0.25)) * ln_gain.astype(jnp.float32)).astype(jnp.bfloat16)
    logits = jnp.dot(normed, router, preferred_element_type=jnp.float32)
    expert_ids = jnp.arange(EXPERTS, dtype=jnp.int32)
    chosen = lax.optimization_barrier(jnp.sum(jnp.where(routes[:, None] == expert_ids[None, :], logits, 0.0), axis=1))
    gate_value = jax.nn.sigmoid(chosen)
    shared_hidden = jax.nn.gelu(jnp.dot(normed, shared_up, preferred_element_type=jnp.float32), approximate=True).astype(jnp.bfloat16)
    shared_out = jnp.dot(shared_hidden, shared_down, preferred_element_type=jnp.float32)
    slot_ids = jnp.arange(CAP, dtype=jnp.int32)

    def one_expert(running, expert_id):
        member = routes == expert_id
        slot_rank = jnp.cumsum(member.astype(jnp.int32)) - 1
        placed = member[:, None] & (slot_rank[:, None] == slot_ids[None, :])
        picked = jnp.dot(placed.astype(jnp.bfloat16).T, normed, preferred_element_type=jnp.float32).astype(jnp.bfloat16)
        up_cols = lax.dynamic_slice_in_dim(expert_up, (expert_id * FF).astype(jnp.int32), FF, 1)
        down_rows = lax.dynamic_slice_in_dim(expert_down, (expert_id * FF).astype(jnp.int32), FF, 0)
        inner_act = jax.nn.gelu(jnp.dot(picked, up_cols, preferred_element_type=jnp.float32), approximate=True).astype(jnp.bfloat16)
        result = jnp.dot(inner_act, down_rows, preferred_element_type=jnp.float32)
        spread = placed.astype(jnp.float32) * gate_value[:, None]
        return (running + jnp.dot(spread, result, precision=lax.Precision.HIGHEST), None)
    expert_out, ignored = lax.scan(one_expert, jnp.zeros((S, D), jnp.float32), expert_ids)
    return (residual + shared_out + expert_out).astype(jnp.bfloat16)
```

```python
import functools
import math

import jax
import jax.numpy as jnp
from jax import lax
from jax.experimental import pallas as pl
from jax.experimental.pallas import tpu as pltpu
from jax.sharding import Mesh
from jax.sharding import PartitionSpec as P

HEADS = 16
HEAD_DIM = 128
FF = 4096
RING = 8
TOKENS = 2 * RING * RING
HALF = RING * RING
EXPERT = ("expert_0", "expert_1", "expert_2")
GROUP_EXPERT = ("group", "expert_0", "expert_1", "expert_2")
MESH = pl.DeviceIdType.MESH
F32 = jnp.float32
BF16 = jnp.bfloat16
FAR_FIRST = (4, 3, 5, 2, 6, 1, 7)
NEAR_FIRST = (1, 7, 2, 6, 3, 5, 4)


def dot(a, b):
    return jnp.dot(a, b, preferred_element_type=F32)


def dot_nt(a, b):
    return lax.dot_general(a, b, (((1,), (1,)), ((), ())), preferred_element_type=F32)


def eye(n):
    return (
        lax.broadcasted_iota(jnp.int32, (n, n), 0) == lax.broadcasted_iota(jnp.int32, (n, n), 1)
    ).astype(BF16)


def diagonal(x):
    row = lax.broadcasted_iota(jnp.int32, (HEADS, HEAD_DIM), 0)
    out = jnp.zeros((HEADS, HEAD_DIM), F32)
    for h in range(HEADS):
        out = jnp.where(row == h, x[:, h * HEAD_DIM : (h + 1) * HEAD_DIM], out)
    return out


def kernel(*refs):
    ins, out_ref, (vm, sems) = refs[:15], refs[15], (refs[16:-8], refs[-8:])
    (
        q_v, kn_v, vn_v, k_v, v_v, len_v, hid_v, rt_v, wo_v, gain_v, router_v, sup_v, rhs, eup_v,
        edn_v, att, hid, pro, big, hid_t, gain_b, nat, res, proj_n, norm_t, up_t, wo_t, part, d_send,
        d_recv, p_send, p_recv, tok, t_recv, lhs,
    ) = vm
    load_sem, att_sem, hid_sem, pro_sem, d_sem, p_sem, t_sem, partner_sem = sems
    d_model = q_v.shape[1]
    shared_units = sup_v.shape[1]
    slots = TOKENS * 4 // 32

    x = lax.axis_index("expert_0")
    y = lax.axis_index("expert_1")
    core = lax.axis_index("expert_2")
    first = x * (1 - core) + y * core
    second = y * (1 - core) + x * core
    me = core * HALF + second * RING + first

    def on_first(k):
        return {
            "expert_0": (x + k * (1 - core)) % RING,
            "expert_1": (y + k * core) % RING,
            "expert_2": core,
        }

    def on_second(k):
        return {
            "expert_0": (x + k * core) % RING,
            "expert_1": (y + k * (1 - core)) % RING,
            "expert_2": core,
        }

    partner = {"expert_0": x, "expert_1": y, "expert_2": 1 - core}

    targets = (
        q_v, kn_v, vn_v, k_v, v_v, len_v, hid_v, rt_v, wo_v, gain_v, router_v, sup_v,
        rhs.at[pl.ds(0, shared_units)], eup_v, edn_v,
    )
    loads = [pltpu.make_async_copy(ins[i], targets[i], load_sem.at[i]) for i in range(15)]
    order = (0, 1, 2, 5, 6, 3, 4, 8, 11, 10, 9, 7, 12, 13, 14)
    for i in order:
        loads[i].start()

    barrier = pltpu.get_barrier_semaphore()
    for k in range(1, RING):
        pl.semaphore_signal(barrier, inc=1, device_id=on_first(k), device_id_type=MESH)
        pl.semaphore_signal(barrier, inc=1, device_id=on_second(k), device_id_type=MESH)
    pl.semaphore_signal(barrier, inc=1, device_id=partner, device_id_type=MESH)

    sent = []

    def send(src, dst, send_sem, recv_sem, to):
        copy = pltpu.make_async_remote_copy(
            src_ref=src, dst_ref=dst, send_sem=send_sem, recv_sem=recv_sem, device_id=to,
            device_id_type=MESH,
        )
        copy.start()
        sent.append(copy)

    def arrived(dst, send_sem, recv_sem):
        pltpu.make_async_remote_copy(
            src_ref=dst, dst_ref=dst, send_sem=send_sem, recv_sem=recv_sem, device_id=partner,
            device_id_type=MESH,
        ).wait_recv()

    def gather_1(buf, sem):
        slot = buf.at[pl.ds(me, 1)]
        for k in FAR_FIRST:
            send(slot, slot, sem.at[0, k], sem.at[1, k], on_first(k))

    def gather_2(buf, sem):
        for k in NEAR_FIRST:
            slot = core * HALF + second * RING + (first - k + RING) % RING
            arrived(buf.at[pl.ds(slot, 1)], sem.at[0, k], sem.at[1, k])
        row = buf.at[pl.ds(core * HALF + second * RING, RING)]
        for k in FAR_FIRST:
            send(row, row, sem.at[2, k], sem.at[3, k], on_second(k))
        send(row, row, sem.at[4, 0], sem.at[5, 0], partner)

    def gather_3(buf, sem):
        for k in NEAR_FIRST:
            row = buf.at[pl.ds(core * HALF + ((second - k + RING) % RING) * RING, RING)]
            arrived(row, sem.at[2, k], sem.at[3, k])
            send(row, row, sem.at[4, k], sem.at[5, k], partner)

    def gather_4(buf, sem):
        for k in (0,) + NEAR_FIRST:
            row = buf.at[pl.ds((1 - core) * HALF + ((first - k + RING) % RING) * RING, RING)]
            arrived(row, sem.at[4, k], sem.at[5, k])

    for i in (0, 1, 2, 5, 6):
        loads[i].wait()
    head_row = lax.broadcasted_iota(jnp.int32, (HEADS, d_model), 0)
    head_of_lane = lax.broadcasted_iota(jnp.int32, (HEADS, d_model), 1) // HEAD_DIM
    own_head = head_row == head_of_lane
    scale = 1.0 / math.sqrt(HEAD_DIM)

    def spread(ref):
        return jnp.broadcast_to(ref[...].astype(F32), (HEADS, d_model))

    hid_tile = diagonal(spread(hid_v))
    hid[pl.ds(me, 1)] = hid_tile.astype(BF16)[None]
    query = jnp.where(own_head, spread(q_v), 0.0)
    own_score = jnp.sum(query * spread(kn_v), axis=1, keepdims=True) * scale
    query = query.astype(BF16)
    loads[3].wait()
    scores = dot_nt(query, k_v[...]) * scale
    position = lax.broadcasted_iota(jnp.int32, scores.shape, 1)
    scores = jnp.where(position < jnp.broadcast_to(len_v[...], scores.shape), scores, -1e30)
    top = jnp.maximum(jnp.max(scores, axis=1, keepdims=True), own_score)
    weights = jnp.exp(scores - top)
    own_weight = jnp.exp(own_score - top)
    normalizer = jnp.sum(weights, axis=1, keepdims=True) + own_weight
    weights = (weights / normalizer).astype(BF16)
    own_weight = (own_weight / normalizer).astype(BF16).astype(F32)
    loads[4].wait()
    mixed = dot(weights, v_v[...]) + own_weight * spread(vn_v)
    att[pl.ds(me, 1)] = diagonal(mixed).astype(BF16)[None]

    pl.semaphore_wait(barrier, 2 * (RING - 1) + 1)
    gather_1(att, att_sem)
    gather_1(hid, hid_sem)

    loads[8].wait()
    wo_t[...] = dot_nt(eye(HEADS), wo_v[...]).astype(BF16)
    gather_2(att, att_sem)
    gather_2(hid, hid_sem)
    loads[11].wait()
    loads[10].wait()
    up_t[0:shared_units, :] = dot_nt(eye(shared_units), sup_v[...]).astype(BF16)
    experts = router_v.shape[1]
    up_t[shared_units:, :] = dot_nt(eye(experts), router_v[...]).astype(BF16)
    loads[9].wait()
    for h in range(HEADS):
        block = gain_v[:, h * HEAD_DIM : (h + 1) * HEAD_DIM].astype(F32)
        gain_b[h * HEAD_DIM : (h + 1) * HEAD_DIM, :] = jnp.broadcast_to(
            block, (HEAD_DIM, TOKENS)
        ).T
    loads[7].wait()
    nat_id = lax.broadcasted_iota(jnp.int32, (TOKENS, TOKENS), 0)
    lane = lax.broadcasted_iota(jnp.int32, (TOKENS, TOKENS), 1)
    lane_core, lane_second, lane_first = lane // HALF, (lane // RING) % RING, lane % RING
    lane_x = lane_first * (1 - lane_core) + lane_second * lane_core
    lane_y = lane_second * (1 - lane_core) + lane_first * lane_core
    to_slot = (nat_id == (lane_x * RING + lane_y) * 2 + lane_core).astype(BF16)
    routes = dot(
        jnp.broadcast_to(rt_v[...], (8, TOKENS)).astype(F32).astype(BF16), to_slot
    )[0:1].astype(jnp.int32)
    device = (x * RING + y) * 2 + core
    mine = device * eup_v.shape[1] // FF
    member = routes == mine
    rank = dot(
        jnp.broadcast_to(member.astype(F32), (8, TOKENS)).astype(BF16), (nat_id <= lane).astype(BF16)
    )[0:1].astype(jnp.int32) - 1
    slot_id = lax.broadcasted_iota(jnp.int32, (slots, TOKENS), 0)
    placed = jnp.where(
        jnp.broadcast_to(member, (slots, TOKENS))
        & (jnp.broadcast_to(rank, (slots, TOKENS)) == slot_id),
        1.0,
        0.0,
    )
    lhs[shared_units:, :] = placed.astype(BF16)

    gather_3(att, att_sem)
    gather_4(att, att_sem)
    big[...] = att[...].reshape(TOKENS * HEADS, HEAD_DIM).astype(F32)
    for h in range(HEADS):
        nat[:, h * HEAD_DIM : (h + 1) * HEAD_DIM] = big[pl.ds(h, TOKENS, stride=HEADS), :].astype(
            BF16
        )
    pro[pl.ds(me, 1)] = dot_nt(wo_t[...], nat[...]).astype(BF16)[None]
    gather_1(pro, pro_sem)
    gather_3(hid, hid_sem)
    gather_2(pro, pro_sem)
    gather_4(hid, hid_sem)
    big[...] = hid[...].reshape(TOKENS * HEADS, HEAD_DIM).astype(F32)
    for h in range(HEADS):
        hid_t[h * HEAD_DIM : (h + 1) * HEAD_DIM, :] = big[pl.ds(h, TOKENS, stride=HEADS), :].T
    gather_3(pro, pro_sem)
    gather_4(pro, pro_sem)

    cols = wo_v.shape[1]
    total = jnp.zeros((cols, TOKENS), F32)
    for n in range(TOKENS):
        n_core, n_y, n_x = n % 2, (n // 2) % RING, n // (2 * RING)
        slot = n_core * HALF + (n_x * RING + n_y if n_core else n_y * RING + n_x)
        rows = slice(n * cols, (n + 1) * cols)
        block = pro[slot]
        proj_n[rows, :] = block
        block = hid_t[rows, :] + block.astype(F32)
        res[rows, :] = block
        total = total + block
    mean = jnp.sum(total, axis=0, keepdims=True) / d_model
    total = jnp.zeros((HEAD_DIM, TOKENS), F32)
    for h in range(HEADS):
        centered = res[h * HEAD_DIM : (h + 1) * HEAD_DIM, :] - mean
        total = total + centered * centered
    variance = jnp.sum(total, axis=0, keepdims=True) / d_model
    inverse = 1.0 / jnp.sqrt(jnp.maximum(variance, 0.25))
    for h in range(HEADS):
        rows = slice(h * HEAD_DIM, (h + 1) * HEAD_DIM)
        norm_t[rows, :] = ((res[rows, :] - mean) * inverse * gain_b[rows, :]).astype(BF16)

    normed = norm_t[...]
    picked = dot_nt(placed.astype(BF16), normed).astype(BF16)
    both = dot(up_t[...], normed)
    lhs[0:shared_units, :] = jax.nn.gelu(both[0:shared_units], approximate=True).astype(BF16)
    expert_row = lax.broadcasted_iota(jnp.int32, (experts, TOKENS), 0)
    chosen = jnp.sum(
        jnp.where(jnp.broadcast_to(routes, (experts, TOKENS)) == expert_row, both[shared_units:], 0.0),
        axis=0,
        keepdims=True,
    )
    gate = 1.0 / (1.0 + jnp.exp(-chosen))
    slot_gate = jnp.sum(placed * gate, axis=1, keepdims=True)
    left = dot_nt(eye(TOKENS), lhs[...]).astype(BF16)
    nat[:, 0 : lhs.shape[0]] = left
    loads[13].wait()
    inner = jax.nn.gelu(dot(picked, eup_v[...]), approximate=True).astype(BF16)
    loads[14].wait()
    result = dot(inner, edn_v[...])
    loads[12].wait()
    rhs[shared_units:, :] = (result * slot_gate).astype(BF16)

    other = pl.multiple_of((1 - core) * HALF, HALF)
    mine_at = pl.multiple_of(core * HALF, HALF)
    depth = lhs.shape[0]
    step = 256
    theirs = nat[pl.ds(other, HALF), 0:depth]
    for at in range(0, d_model, step):
        piece = dot(theirs, rhs[:, at : at + step]).astype(BF16)
        d_send[:, :, at : at + step] = piece.reshape(RING, RING, step)
    for k in FAR_FIRST + (0,):
        block = (first + k) % RING
        send(d_send.at[block], d_recv.at[block], d_sem.at[0, k], d_sem.at[1, k], partner)
    ours = nat[pl.ds(mine_at, HALF), 0:depth]
    for at in range(0, d_model, step):
        part[:, at : at + step] = dot(ours, rhs[:, at : at + step])
    for k in FAR_FIRST + (0,):
        block = (second + k) % RING
        arrived(d_recv.at[block], d_sem.at[0, k], d_sem.at[1, k])
        rows = pl.ds(pl.multiple_of(block * RING, RING), RING)
        both_cores = part[rows, :] + d_recv[block].astype(F32)
        if k:
            p_send[k - 1] = both_cores.astype(BF16)
            send(p_send.at[k - 1], p_recv.at[k - 1], p_sem.at[0, k], p_sem.at[1, k], on_second(k))
        else:
            summed = both_cores
    own_column = (
        lax.broadcasted_iota(jnp.int32, (HEADS, TOKENS), 1) == me
    ).astype(BF16)
    own = hid_tile + diagonal(dot_nt(own_column, proj_n[...]))
    for k in NEAR_FIRST:
        arrived(p_recv.at[k - 1], p_sem.at[0, k], p_sem.at[1, k])
        summed = summed + p_recv[k - 1].astype(F32)
    for h in range(HEADS):
        tok[pl.ds(h, RING, stride=HEADS), :] = summed[:, h * HEAD_DIM : (h + 1) * HEAD_DIM]
    for k in FAR_FIRST:
        to = pl.multiple_of(((first + k) % RING) * HEADS, HEADS)
        send(tok.at[pl.ds(to, HEADS)], t_recv.at[k - 1], t_sem.at[0, k], t_sem.at[1, k], on_first(k))
    own = own + tok[pl.ds(pl.multiple_of(first * HEADS, HEADS), HEADS), :]
    for k in NEAR_FIRST:
        arrived(t_recv.at[k - 1], t_sem.at[0, k], t_sem.at[1, k])
        own = own + t_recv[k - 1]
    for h in range(HEADS):
        out_ref[:, h * HEAD_DIM : (h + 1) * HEAD_DIM] = own[h : h + 1, :].astype(BF16)
    for copy in sent:
        copy.wait_send()


def body(
    query, key_new, value_new, key_cache, value_cache, lengths, hidden, routes, w_out, ln_gain,
    router, shared_up, shared_down, expert_up, expert_down,
):
    key_cache = key_cache.reshape(key_cache.shape[1:])
    value_cache = value_cache.reshape(value_cache.shape[1:])
    lengths = lengths.reshape(1, 1)
    routes = routes.reshape(1, -1)
    ln_gain = ln_gain.reshape(1, -1)
    args = (
        query, key_new, value_new, key_cache, value_cache, lengths, hidden, routes, w_out, ln_gain,
        router, shared_up, shared_down, expert_up, expert_down,
    )
    d = query.shape[1]
    units = shared_up.shape[1]
    slots = TOKENS * 4 // 32
    tile = (TOKENS, HEADS, HEAD_DIM)

    def own(a):
        return pltpu.VMEM(a.shape, a.dtype)

    dma = pltpu.SemaphoreType.DMA
    scratch = [own(a) for a in args[:12]]
    scratch += [
        pltpu.VMEM((units + slots, d), BF16),
        own(expert_up),
        own(expert_down),
        pltpu.VMEM(tile, BF16),
        pltpu.VMEM(tile, BF16),
        pltpu.VMEM((TOKENS, w_out.shape[1], TOKENS), BF16),
        pltpu.VMEM((TOKENS * HEADS, HEAD_DIM), F32),
        pltpu.VMEM((d, TOKENS), F32),
        pltpu.VMEM((d, TOKENS), F32),
        pltpu.VMEM((TOKENS, d), BF16),
        pltpu.VMEM((d, TOKENS), F32),
        pltpu.VMEM((d, TOKENS), BF16),
        pltpu.VMEM((d, TOKENS), BF16),
        pltpu.VMEM((units + router.shape[1], d), BF16),
        pltpu.VMEM((w_out.shape[1], d), BF16),
        pltpu.VMEM((HALF, d), F32),
        pltpu.VMEM((RING, RING, d), BF16),
        pltpu.VMEM((RING, RING, d), BF16),
        pltpu.VMEM((RING - 1, RING, d), BF16),
        pltpu.VMEM((RING - 1, RING, d), BF16),
        pltpu.VMEM((RING * HEADS, HEAD_DIM), F32),
        pltpu.VMEM((RING - 1, HEADS, HEAD_DIM), F32),
        pltpu.VMEM((units + slots, TOKENS), BF16),
        dma((15,)),
        dma((6, RING)),
        dma((6, RING)),
        dma((6, RING)),
        dma((2, RING)),
        dma((2, RING)),
        dma((2, RING)),
        dma((1,)),
    ]
    return pl.pallas_call(
        kernel,
        out_shape=jax.ShapeDtypeStruct((1, d), BF16),
        in_specs=[pl.BlockSpec(memory_space=pl.ANY)] * 15,
        out_specs=pl.BlockSpec(memory_space=pltpu.VMEM),
        scratch_shapes=scratch,
        compiler_params=pltpu.CompilerParams(collective_id=0, has_side_effects=True),
        name="decode_layer",
    )(*args)


def solution(mesh):
    torus = Mesh(
        mesh.devices.reshape(mesh.shape["group"], RING, RING, 2),
        ("group", "expert_0", "expert_1", "expert_2"),
    )
    placed = (
        P(GROUP_EXPERT, None),
        P(GROUP_EXPERT, None),
        P(GROUP_EXPERT, None),
        P(GROUP_EXPERT, None, None),
        P(GROUP_EXPERT, None, None),
        P(GROUP_EXPERT),
        P(GROUP_EXPERT, None),
        P("group"),
        P(None, EXPERT),
        P(),
        P(),
        P(None, EXPERT),
        P(EXPERT, None),
        P(None, EXPERT),
        P(EXPERT, None),
    )
    return jax.shard_map(
        body, mesh=torus, in_specs=placed, out_specs=P(GROUP_EXPERT, None), check_vma=False
    )
```

```python
import functools
import math

import jax
import jax.numpy as jnp
from jax import lax
from jax.experimental import pallas as pl
from jax.experimental.pallas import tpu as pltpu
from jax.sharding import Mesh
from jax.sharding import PartitionSpec as P

HEADS = 16
HEAD_DIM = 128
FF = 4096
RING = 8
TOKENS = 2 * RING * RING
HALF = RING * RING
EXPERT = ("expert_0", "expert_1", "expert_2")
GROUP_EXPERT = ("group", "expert_0", "expert_1", "expert_2")
MESH = pl.DeviceIdType.MESH
F32 = jnp.float32
BF16 = jnp.bfloat16
FAR_FIRST = (4, 3, 5, 2, 6, 1, 7)
NEAR_FIRST = (1, 7, 2, 6, 3, 5, 4)


def dot(a, b):
    return jnp.dot(a, b, preferred_element_type=F32)


def dot_nt(a, b):
    return lax.dot_general(a, b, (((1,), (1,)), ((), ())), preferred_element_type=F32)


def eye(n):
    return (
        lax.broadcasted_iota(jnp.int32, (n, n), 0) == lax.broadcasted_iota(jnp.int32, (n, n), 1)
    ).astype(BF16)


def diagonal(x):
    row = lax.broadcasted_iota(jnp.int32, (HEADS, HEAD_DIM), 0)
    out = jnp.zeros((HEADS, HEAD_DIM), F32)
    for h in range(HEADS):
        out = jnp.where(row == h, x[:, h * HEAD_DIM : (h + 1) * HEAD_DIM], out)
    return out


def kernel(*refs):
    ins, out_ref, (vm, sems) = refs[:15], refs[15], (refs[16:-8], refs[-8:])
    (
        q_v, kn_v, vn_v, k_v, v_v, len_v, hid_v, rt_v, wo_t, gain_v, up_t, rhs, eup_v, edn_v, att, hid,
        pro, big, hid_t, gain_b, nat, res, proj_n, norm_t, part, d_send, d_recv, p_send, p_recv, tok,
        t_recv, lhs,
    ) = vm
    load_sem, att_sem, hid_sem, pro_sem, d_sem, p_sem, t_sem, partner_sem = sems
    d_model = q_v.shape[1]
    experts, shared_units = ins[10].shape[0], ins[11].shape[0]
    slots = TOKENS * 4 // 32

    x = lax.axis_index("expert_0")
    y = lax.axis_index("expert_1")
    core = lax.axis_index("expert_2")
    first = x * (1 - core) + y * core
    second = y * (1 - core) + x * core
    me = core * HALF + second * RING + first

    def on_first(k):
        return {
            "expert_0": (x + k * (1 - core)) % RING,
            "expert_1": (y + k * core) % RING,
            "expert_2": core,
        }

    def on_second(k):
        return {
            "expert_0": (x + k * core) % RING,
            "expert_1": (y + k * (1 - core)) % RING,
            "expert_2": core,
        }

    partner = {"expert_0": x, "expert_1": y, "expert_2": 1 - core}

    targets = (
        q_v, kn_v, vn_v, k_v, v_v, len_v, hid_v, rt_v, wo_t, gain_v,
        up_t.at[pl.ds(shared_units, experts)], up_t.at[pl.ds(0, shared_units)], rhs.at[pl.ds(0, shared_units)], eup_v, edn_v,
    )
    loads = [pltpu.make_async_copy(ins[i], targets[i], load_sem.at[i]) for i in range(15)]
    order = (0, 1, 2, 5, 6, 3, 4, 8, 11, 10, 9, 7, 12, 13, 14)
    for i in order:
        loads[i].start()

    barrier = pltpu.get_barrier_semaphore()
    for k in range(1, RING):
        pl.semaphore_signal(barrier, inc=1, device_id=on_first(k), device_id_type=MESH)
        pl.semaphore_signal(barrier, inc=1, device_id=on_second(k), device_id_type=MESH)
    pl.semaphore_signal(barrier, inc=1, device_id=partner, device_id_type=MESH)

    sent = []

    def send(src, dst, send_sem, recv_sem, to):
        copy = pltpu.make_async_remote_copy(
            src_ref=src, dst_ref=dst, send_sem=send_sem, recv_sem=recv_sem, device_id=to,
            device_id_type=MESH,
        )
        copy.start()
        sent.append(copy)

    def arrived(dst, send_sem, recv_sem):
        pltpu.make_async_remote_copy(
            src_ref=dst, dst_ref=dst, send_sem=send_sem, recv_sem=recv_sem, device_id=partner,
            device_id_type=MESH,
        ).wait_recv()

    def gather_1(buf, sem):
        slot = buf.at[pl.ds(me, 1)]
        for k in FAR_FIRST:
            send(slot, slot, sem.at[0, k], sem.at[1, k], on_first(k))

    def gather_2(buf, sem):
        for k in NEAR_FIRST:
            slot = core * HALF + second * RING + (first - k + RING) % RING
            arrived(buf.at[pl.ds(slot, 1)], sem.at[0, k], sem.at[1, k])
        row = buf.at[pl.ds(core * HALF + second * RING, RING)]
        for k in FAR_FIRST:
            send(row, row, sem.at[2, k], sem.at[3, k], on_second(k))
        send(row, row, sem.at[4, 0], sem.at[5, 0], partner)

    def gather_3(buf, sem):
        for k in NEAR_FIRST:
            row = buf.at[pl.ds(core * HALF + ((second - k + RING) % RING) * RING, RING)]
            arrived(row, sem.at[2, k], sem.at[3, k])
            send(row, row, sem.at[4, k], sem.at[5, k], partner)

    def gather_4(buf, sem):
        for k in (0,) + NEAR_FIRST:
            row = buf.at[pl.ds((1 - core) * HALF + ((first - k + RING) % RING) * RING, RING)]
            arrived(row, sem.at[4, k], sem.at[5, k])

    for i in (0, 1, 2, 5, 6):
        loads[i].wait()
    head_row = lax.broadcasted_iota(jnp.int32, (HEADS, d_model), 0)
    head_of_lane = lax.broadcasted_iota(jnp.int32, (HEADS, d_model), 1) // HEAD_DIM
    own_head = head_row == head_of_lane
    scale = 1.0 / math.sqrt(HEAD_DIM)

    def spread(ref):
        return jnp.broadcast_to(ref[...].astype(F32), (HEADS, d_model))

    hid_tile = diagonal(spread(hid_v))
    hid[pl.ds(me, 1)] = hid_tile.astype(BF16)[None]
    query = jnp.where(own_head, spread(q_v), 0.0)
    own_score = jnp.sum(query * spread(kn_v), axis=1, keepdims=True) * scale
    query = query.astype(BF16)
    loads[3].wait()
    scores = dot_nt(query, k_v[...]) * scale
    position = lax.broadcasted_iota(jnp.int32, scores.shape, 1)
    scores = jnp.where(position < jnp.broadcast_to(len_v[...], scores.shape), scores, -1e30)
    top = jnp.maximum(jnp.max(scores, axis=1, keepdims=True), own_score)
    weights = jnp.exp(scores - top)
    own_weight = jnp.exp(own_score - top)
    normalizer = jnp.sum(weights, axis=1, keepdims=True) + own_weight
    weights = (weights / normalizer).astype(BF16)
    own_weight = (own_weight / normalizer).astype(BF16).astype(F32)
    loads[4].wait()
    mixed = dot(weights, v_v[...]) + own_weight * spread(vn_v)
    att[pl.ds(me, 1)] = diagonal(mixed).astype(BF16)[None]

    pl.semaphore_wait(barrier, 2 * (RING - 1) + 1)
    gather_1(att, att_sem)
    gather_1(hid, hid_sem)

    gather_2(att, att_sem)
    gather_2(hid, hid_sem)
    loads[9].wait()
    for h in range(HEADS):
        block = gain_v[h : h + 1, :].astype(F32)
        gain_b[h * HEAD_DIM : (h + 1) * HEAD_DIM, :] = jnp.broadcast_to(
            block, (HEAD_DIM, TOKENS)
        ).T
    loads[7].wait()
    nat_id = lax.broadcasted_iota(jnp.int32, (TOKENS, TOKENS), 0)
    lane = lax.broadcasted_iota(jnp.int32, (TOKENS, TOKENS), 1)
    lane_core, lane_second, lane_first = lane // HALF, (lane // RING) % RING, lane % RING
    lane_x = lane_first * (1 - lane_core) + lane_second * lane_core
    lane_y = lane_second * (1 - lane_core) + lane_first * lane_core
    to_slot = (nat_id == (lane_x * RING + lane_y) * 2 + lane_core).astype(BF16)
    routes = dot(
        jnp.broadcast_to(rt_v[...], (8, TOKENS)).astype(F32).astype(BF16), to_slot
    )[0:1].astype(jnp.int32)
    device = (x * RING + y) * 2 + core
    mine = device * eup_v.shape[1] // FF
    member = routes == mine
    rank = dot(
        jnp.broadcast_to(member.astype(F32), (8, TOKENS)).astype(BF16), (nat_id <= lane).astype(BF16)
    )[0:1].astype(jnp.int32) - 1
    slot_id = lax.broadcasted_iota(jnp.int32, (slots, TOKENS), 0)
    placed = jnp.where(
        jnp.broadcast_to(member, (slots, TOKENS))
        & (jnp.broadcast_to(rank, (slots, TOKENS)) == slot_id),
        1.0,
        0.0,
    )
    lhs[shared_units:, :] = placed.astype(BF16)

    gather_3(att, att_sem)
    gather_4(att, att_sem)
    big[...] = att[...].reshape(TOKENS * HEADS, HEAD_DIM).astype(F32)
    for h in range(HEADS):
        nat[:, h * HEAD_DIM : (h + 1) * HEAD_DIM] = big[pl.ds(h, TOKENS, stride=HEADS), :].astype(
            BF16
        )
    loads[8].wait()
    pro[pl.ds(me, 1)] = dot_nt(wo_t[...], nat[...]).astype(BF16)[None]
    gather_1(pro, pro_sem)
    gather_3(hid, hid_sem)
    gather_2(pro, pro_sem)
    gather_4(hid, hid_sem)
    big[...] = hid[...].reshape(TOKENS * HEADS, HEAD_DIM).astype(F32)
    for h in range(HEADS):
        hid_t[h * HEAD_DIM : (h + 1) * HEAD_DIM, :] = big[pl.ds(h, TOKENS, stride=HEADS), :].T
    gather_3(pro, pro_sem)
    gather_4(pro, pro_sem)

    cols = wo_t.shape[0]
    total = jnp.zeros((cols, TOKENS), F32)
    for n in range(TOKENS):
        n_core, n_y, n_x = n % 2, (n // 2) % RING, n // (2 * RING)
        slot = n_core * HALF + (n_x * RING + n_y if n_core else n_y * RING + n_x)
        rows = slice(n * cols, (n + 1) * cols)
        block = pro[slot]
        proj_n[rows, :] = block
        block = hid_t[rows, :] + block.astype(F32)
        res[rows, :] = block
        total = total + block
    mean = jnp.sum(total, axis=0, keepdims=True) / d_model
    total = jnp.zeros((HEAD_DIM, TOKENS), F32)
    for h in range(HEADS):
        centered = res[h * HEAD_DIM : (h + 1) * HEAD_DIM, :] - mean
        total = total + centered * centered
    variance = jnp.sum(total, axis=0, keepdims=True) / d_model
    inverse = 1.0 / jnp.sqrt(jnp.maximum(variance, 0.25))
    for h in range(HEADS):
        rows = slice(h * HEAD_DIM, (h + 1) * HEAD_DIM)
        norm_t[rows, :] = ((res[rows, :] - mean) * inverse * gain_b[rows, :]).astype(BF16)

    loads[10].wait()
    loads[11].wait()
    normed = norm_t[...]
    picked = dot_nt(placed.astype(BF16), normed).astype(BF16)
    both = dot(up_t[...], normed)
    lhs[0:shared_units, :] = jax.nn.gelu(both[0:shared_units], approximate=True).astype(BF16)
    expert_row = lax.broadcasted_iota(jnp.int32, (experts, TOKENS), 0)
    chosen = jnp.sum(
        jnp.where(jnp.broadcast_to(routes, (experts, TOKENS)) == expert_row, both[shared_units:], 0.0),
        axis=0,
        keepdims=True,
    )
    gate = 1.0 / (1.0 + jnp.exp(-chosen))
    slot_gate = jnp.sum(placed * gate, axis=1, keepdims=True)
    left = dot_nt(eye(TOKENS), lhs[...]).astype(BF16)
    nat[:, 0 : lhs.shape[0]] = left
    loads[13].wait()
    inner = jax.nn.gelu(dot(picked, eup_v[...]), approximate=True).astype(BF16)
    loads[14].wait()
    result = dot(inner, edn_v[...])
    loads[12].wait()
    rhs[shared_units:, :] = (result * slot_gate).astype(BF16)

    other = pl.multiple_of((1 - core) * HALF, HALF)
    mine_at = pl.multiple_of(core * HALF, HALF)
    depth = lhs.shape[0]
    step = 256
    theirs = nat[pl.ds(other, HALF), 0:depth]
    for at in range(0, d_model, step):
        piece = dot(theirs, rhs[:, at : at + step]).astype(BF16)
        d_send[:, :, at : at + step] = piece.reshape(RING, RING, step)
    for k in FAR_FIRST + (0,):
        block = (first + k) % RING
        send(d_send.at[block], d_recv.at[block], d_sem.at[0, k], d_sem.at[1, k], partner)
    ours = nat[pl.ds(mine_at, HALF), 0:depth]
    for at in range(0, d_model, step):
        part[:, at : at + step] = dot(ours, rhs[:, at : at + step])
    for k in FAR_FIRST + (0,):
        block = (second + k) % RING
        arrived(d_recv.at[block], d_sem.at[0, k], d_sem.at[1, k])
        rows = pl.ds(pl.multiple_of(block * RING, RING), RING)
        both_cores = part[rows, :] + d_recv[block].astype(F32)
        if k:
            p_send[k - 1] = both_cores.astype(BF16)
            send(p_send.at[k - 1], p_recv.at[k - 1], p_sem.at[0, k], p_sem.at[1, k], on_second(k))
        else:
            summed = both_cores
    own_column = (
        lax.broadcasted_iota(jnp.int32, (HEADS, TOKENS), 1) == me
    ).astype(BF16)
    own = hid_tile + diagonal(dot_nt(own_column, proj_n[...]))
    for k in NEAR_FIRST:
        arrived(p_recv.at[k - 1], p_sem.at[0, k], p_sem.at[1, k])
        summed = summed + p_recv[k - 1].astype(F32)
    for h in range(HEADS):
        tok[pl.ds(h, RING, stride=HEADS), :] = summed[:, h * HEAD_DIM : (h + 1) * HEAD_DIM]
    for k in FAR_FIRST:
        to = pl.multiple_of(((first + k) % RING) * HEADS, HEADS)
        send(tok.at[pl.ds(to, HEADS)], t_recv.at[k - 1], t_sem.at[0, k], t_sem.at[1, k], on_first(k))
    own = own + tok[pl.ds(pl.multiple_of(first * HEADS, HEADS), HEADS), :]
    for k in NEAR_FIRST:
        arrived(t_recv.at[k - 1], t_sem.at[0, k], t_sem.at[1, k])
        own = own + t_recv[k - 1]
    for h in range(HEADS):
        out_ref[:, h * HEAD_DIM : (h + 1) * HEAD_DIM] = own[h : h + 1, :].astype(BF16)
    for copy in sent:
        copy.wait_send()


def body(
    query, key_new, value_new, key_cache, value_cache, lengths, hidden, routes, w_out, ln_gain,
    router, shared_up, shared_down, expert_up, expert_down,
):
    key_cache = key_cache.reshape(key_cache.shape[1:])
    value_cache = value_cache.reshape(value_cache.shape[1:])
    lengths = lengths.reshape(1, 1)
    routes = routes.reshape(1, -1)
    ln_gain = ln_gain.reshape(-1, HEAD_DIM)
    w_out, router, shared_up = w_out.T, router.T, shared_up.T
    args = (
        query, key_new, value_new, key_cache, value_cache, lengths, hidden, routes, w_out, ln_gain,
        router, shared_up, shared_down, expert_up, expert_down,
    )
    d = query.shape[1]
    units = shared_up.shape[0]
    slots = TOKENS * 4 // 32
    tile = (TOKENS, HEADS, HEAD_DIM)

    def own(a):
        return pltpu.VMEM(a.shape, a.dtype)

    dma = pltpu.SemaphoreType.DMA
    scratch = [own(a) for a in args[:10]]
    scratch += [
        pltpu.VMEM((units + router.shape[0], d), BF16),
        pltpu.VMEM((units + slots, d), BF16),
        own(expert_up),
        own(expert_down),
        pltpu.VMEM(tile, BF16),
        pltpu.VMEM(tile, BF16),
        pltpu.VMEM((TOKENS, w_out.shape[0], TOKENS), BF16),
        pltpu.VMEM((TOKENS * HEADS, HEAD_DIM), F32),
        pltpu.VMEM((d, TOKENS), F32),
        pltpu.VMEM((d, TOKENS), F32),
        pltpu.VMEM((TOKENS, d), BF16),
        pltpu.VMEM((d, TOKENS), F32),
        pltpu.VMEM((d, TOKENS), BF16),
        pltpu.VMEM((d, TOKENS), BF16),
        pltpu.VMEM((HALF, d), F32),
        pltpu.VMEM((RING, RING, d), BF16),
        pltpu.VMEM((RING, RING, d), BF16),
        pltpu.VMEM((RING - 1, RING, d), BF16),
        pltpu.VMEM((RING - 1, RING, d), BF16),
        pltpu.VMEM((RING * HEADS, HEAD_DIM), F32),
        pltpu.VMEM((RING - 1, HEADS, HEAD_DIM), F32),
        pltpu.VMEM((units + slots, TOKENS), BF16),
        dma((15,)),
        dma((6, RING)),
        dma((6, RING)),
        dma((6, RING)),
        dma((2, RING)),
        dma((2, RING)),
        dma((2, RING)),
        dma((1,)),
    ]
    return pl.pallas_call(
        kernel,
        out_shape=jax.ShapeDtypeStruct((1, d), BF16),
        in_specs=[pl.BlockSpec(memory_space=pl.ANY)] * 15,
        out_specs=pl.BlockSpec(memory_space=pltpu.VMEM),
        scratch_shapes=scratch,
        compiler_params=pltpu.CompilerParams(collective_id=0, has_side_effects=True),
        name="decode_layer",
    )(*args)


def solution(mesh):
    torus = Mesh(
        mesh.devices.reshape(mesh.shape["group"], RING, RING, 2),
        ("group", "expert_0", "expert_1", "expert_2"),
    )
    placed = (
        P(GROUP_EXPERT, None),
        P(GROUP_EXPERT, None),
        P(GROUP_EXPERT, None),
        P(GROUP_EXPERT, None, None),
        P(GROUP_EXPERT, None, None),
        P(GROUP_EXPERT),
        P(GROUP_EXPERT, None),
        P("group"),
        P(None, EXPERT),
        P(),
        P(),
        P(None, EXPERT),
        P(EXPERT, None),
        P(None, EXPERT),
        P(EXPERT, None),
    )
    return jax.shard_map(
        body, mesh=torus, in_specs=placed, out_specs=P(GROUP_EXPERT, None), check_vma=False
    )
```

```python
import functools
import math

import jax
import jax.numpy as jnp
from jax import lax
from jax.experimental import pallas as pl
from jax.experimental.pallas import tpu as pltpu
from jax.sharding import Mesh
from jax.sharding import PartitionSpec as P

HEADS = 16
HEAD_DIM = 128
FF = 4096
RING = 8
TOKENS = 2 * RING * RING
HALF = RING * RING
EXPERT = ("expert_0", "expert_1", "expert_2")
GROUP_EXPERT = ("group", "expert_0", "expert_1", "expert_2")
MESH = pl.DeviceIdType.MESH
F32 = jnp.float32
BF16 = jnp.bfloat16
FAR_FIRST = (4, 3, 5, 2, 6, 1, 7)
NEAR_FIRST = (1, 7, 2, 6, 3, 5, 4)
BY_HOPS = sorted(
    ((k, j) for k in range(RING) for j in range(RING)),
    key=lambda kj: min(kj[0], RING - kj[0]) + min(kj[1], RING - kj[1]),
)


def dot(a, b):
    return jnp.dot(a, b, preferred_element_type=F32)


def dot_nt(a, b):
    return lax.dot_general(a, b, (((1,), (1,)), ((), ())), preferred_element_type=F32)


def eye(n):
    return (
        lax.broadcasted_iota(jnp.int32, (n, n), 0) == lax.broadcasted_iota(jnp.int32, (n, n), 1)
    ).astype(BF16)


def diagonal(x):
    row = lax.broadcasted_iota(jnp.int32, (HEADS, HEAD_DIM), 0)
    out = jnp.zeros((HEADS, HEAD_DIM), F32)
    for h in range(HEADS):
        out = jnp.where(row == h, x[:, h * HEAD_DIM : (h + 1) * HEAD_DIM], out)
    return out


def kernel(*refs):
    ins, out_ref, (vm, sems) = refs[:15], refs[15], (refs[16:-17], refs[-17:])
    (
        q_v, kn_v, vn_v, k_v, v_v, len_v, hid_v, rt_v, wo_t, gain_v, up_t, rhs, eup_v, edn_v, att, hid,
        pro, big, hid_t, gain_b, nat, res, proj_n, norm_t, part, d_send, d_recv, p_send, p_recv, tok,
        t_recv, lhs,
    ) = vm
    load_sem, hid_sem, d_sem, p_sem, t_sem = sems[:5]
    att_sem, pro_sem = sems[5:11], sems[11:]
    d_model = q_v.shape[1]
    experts, shared_units = ins[10].shape[0], ins[11].shape[0]
    slots = TOKENS * 4 // 32

    x = lax.axis_index("expert_0")
    y = lax.axis_index("expert_1")
    core = lax.axis_index("expert_2")
    first = x * (1 - core) + y * core
    second = y * (1 - core) + x * core
    me = core * HALF + second * RING + first

    def on_first(k):
        return {
            "expert_0": (x + k * (1 - core)) % RING,
            "expert_1": (y + k * core) % RING,
            "expert_2": core,
        }

    def on_second(k):
        return {
            "expert_0": (x + k * core) % RING,
            "expert_1": (y + k * (1 - core)) % RING,
            "expert_2": core,
        }

    partner = {"expert_0": x, "expert_1": y, "expert_2": 1 - core}

    barrier = pltpu.get_barrier_semaphore()
    for k in range(1, RING):
        pl.semaphore_signal(barrier, inc=1, device_id=on_first(k), device_id_type=MESH)
        pl.semaphore_signal(barrier, inc=1, device_id=on_second(k), device_id_type=MESH)
    pl.semaphore_signal(barrier, inc=1, device_id=partner, device_id_type=MESH)

    targets = (
        q_v, kn_v, vn_v, k_v, v_v, len_v, hid_v, rt_v, wo_t, gain_v,
        up_t.at[pl.ds(shared_units, experts)], up_t.at[pl.ds(0, shared_units)], rhs.at[pl.ds(0, shared_units)], eup_v, edn_v,
    )
    loads = [pltpu.make_async_copy(ins[i], targets[i], load_sem.at[i]) for i in range(15)]
    order = (3, 0, 1, 2, 5, 6, 4, 9, 7, 8, 11, 10, 12, 13, 14)
    for i in order:
        loads[i].start()

    sent = []

    def send(src, dst, send_sem, recv_sem, to):
        copy = pltpu.make_async_remote_copy(
            src_ref=src, dst_ref=dst, send_sem=send_sem, recv_sem=recv_sem, device_id=to,
            device_id_type=MESH,
        )
        copy.start()
        sent.append(copy)

    def arrived(dst, send_sem, recv_sem):
        pltpu.make_async_remote_copy(
            src_ref=dst, dst_ref=dst, send_sem=send_sem, recv_sem=recv_sem, device_id=partner,
            device_id_type=MESH,
        ).wait_recv()

    def slot_of(k, second_k=0, of=core):
        return (
            of * HALF + ((second - second_k + RING) % RING) * RING + (first - k + RING) % RING
        )

    def pass_on(buf, sems, k):
        tile = buf.at[pl.ds(slot_of(k), 1)]
        for j in FAR_FIRST:
            send(tile, tile, sems[2].at[k, j], sems[3].at[k, j], on_second(j))
        send(tile, tile, sems[4].at[k, 0], sems[5].at[k, 0], partner)

    def tiles_1(buf, sems):
        tile = buf.at[pl.ds(me, 1)]
        for k in FAR_FIRST:
            send(tile, tile, sems[0].at[0, k], sems[1].at[0, k], on_first(k))
        pass_on(buf, sems, 0)

    def tiles_2(buf, sems):
        for k in NEAR_FIRST:
            arrived(buf.at[pl.ds(slot_of(k), 1)], sems[0].at[0, k], sems[1].at[0, k])
            pass_on(buf, sems, k)

    def tiles_3(buf, sems):
        for k, j in BY_HOPS:
            if j:
                tile = buf.at[pl.ds(slot_of(k, j), 1)]
                arrived(tile, sems[2].at[k, j], sems[3].at[k, j])
                send(tile, tile, sems[4].at[k, j], sems[5].at[k, j], partner)

    def tiles_4(buf, sems):
        for k, j in BY_HOPS:
            slot = (
                (1 - core) * HALF + ((first - j + RING) % RING) * RING + (second - k + RING) % RING
            )
            arrived(buf.at[pl.ds(slot, 1)], sems[4].at[k, j], sems[5].at[k, j])

    def gather_1(buf, sem):
        slot = buf.at[pl.ds(me, 1)]
        for k in FAR_FIRST:
            send(slot, slot, sem.at[0, k], sem.at[1, k], on_first(k))

    def gather_2(buf, sem):
        for k in NEAR_FIRST:
            slot = core * HALF + second * RING + (first - k + RING) % RING
            arrived(buf.at[pl.ds(slot, 1)], sem.at[0, k], sem.at[1, k])
        row = buf.at[pl.ds(core * HALF + second * RING, RING)]
        for k in FAR_FIRST:
            send(row, row, sem.at[2, k], sem.at[3, k], on_second(k))
        send(row, row, sem.at[4, 0], sem.at[5, 0], partner)

    def gather_3(buf, sem):
        for k in NEAR_FIRST:
            row = buf.at[pl.ds(core * HALF + ((second - k + RING) % RING) * RING, RING)]
            arrived(row, sem.at[2, k], sem.at[3, k])
            send(row, row, sem.at[4, k], sem.at[5, k], partner)

    def gather_4(buf, sem):
        for k in (0,) + NEAR_FIRST:
            row = buf.at[pl.ds((1 - core) * HALF + ((first - k + RING) % RING) * RING, RING)]
            arrived(row, sem.at[4, k], sem.at[5, k])

    for i in (0, 1, 2, 5, 6):
        loads[i].wait()
    head_row = lax.broadcasted_iota(jnp.int32, (HEADS, d_model), 0)
    head_of_lane = lax.broadcasted_iota(jnp.int32, (HEADS, d_model), 1) // HEAD_DIM
    own_head = head_row == head_of_lane
    scale = 1.0 / math.sqrt(HEAD_DIM)

    def spread(ref):
        return jnp.broadcast_to(ref[...].astype(F32), (HEADS, d_model))

    hid_tile = diagonal(spread(hid_v))
    hid[pl.ds(me, 1)] = hid_tile.astype(BF16)[None]
    query = jnp.where(own_head, spread(q_v), 0.0)
    own_score = jnp.sum(query * spread(kn_v), axis=1, keepdims=True) * scale
    query = query.astype(BF16)
    loads[3].wait()
    scores = dot_nt(query, k_v[...]) * scale
    position = lax.broadcasted_iota(jnp.int32, scores.shape, 1)
    scores = jnp.where(position < jnp.broadcast_to(len_v[...], scores.shape), scores, -1e30)
    top = jnp.maximum(jnp.max(scores, axis=1, keepdims=True), own_score)
    weights = jnp.exp(scores - top)
    own_weight = jnp.exp(own_score - top)
    normalizer = jnp.sum(weights, axis=1, keepdims=True) + own_weight
    weights = (weights / normalizer).astype(BF16)
    own_weight = (own_weight / normalizer).astype(BF16).astype(F32)
    loads[4].wait()
    mixed = dot(weights, v_v[...]) + own_weight * spread(vn_v)
    att[pl.ds(me, 1)] = diagonal(mixed).astype(BF16)[None]

    pl.semaphore_wait(barrier, 2 * (RING - 1) + 1)
    tiles_1(att, att_sem)
    gather_1(hid, hid_sem)

    loads[9].wait()
    for h in range(HEADS):
        block = gain_v[h : h + 1, :].astype(F32)
        gain_b[h * HEAD_DIM : (h + 1) * HEAD_DIM, :] = jnp.broadcast_to(
            block, (HEAD_DIM, TOKENS)
        ).T
    loads[7].wait()
    nat_id = lax.broadcasted_iota(jnp.int32, (TOKENS, TOKENS), 0)
    lane = lax.broadcasted_iota(jnp.int32, (TOKENS, TOKENS), 1)
    lane_core, lane_second, lane_first = lane // HALF, (lane // RING) % RING, lane % RING
    lane_x = lane_first * (1 - lane_core) + lane_second * lane_core
    lane_y = lane_second * (1 - lane_core) + lane_first * lane_core
    to_slot = (nat_id == (lane_x * RING + lane_y) * 2 + lane_core).astype(BF16)
    routes = dot(
        jnp.broadcast_to(rt_v[...], (8, TOKENS)).astype(F32).astype(BF16), to_slot
    )[0:1].astype(jnp.int32)
    device = (x * RING + y) * 2 + core
    mine = device * eup_v.shape[1] // FF
    member = routes == mine
    rank = dot(
        jnp.broadcast_to(member.astype(F32), (8, TOKENS)).astype(BF16), (nat_id <= lane).astype(BF16)
    )[0:1].astype(jnp.int32) - 1
    slot_id = lax.broadcasted_iota(jnp.int32, (slots, TOKENS), 0)
    placed = jnp.where(
        jnp.broadcast_to(member, (slots, TOKENS))
        & (jnp.broadcast_to(rank, (slots, TOKENS)) == slot_id),
        1.0,
        0.0,
    )
    lhs[shared_units:, :] = placed.astype(BF16)

    tiles_2(att, att_sem)
    tiles_3(att, att_sem)
    gather_2(hid, hid_sem)

    def relayout(buf, at):
        at = pl.multiple_of(at, HALF)
        rows = pl.ds(pl.multiple_of(at * HEADS, HALF * HEADS), HALF * HEADS)
        big[rows, :] = buf[pl.ds(at, HALF)].reshape(HALF * HEADS, HEAD_DIM).astype(F32)

    def att_rows(at):
        relayout(att, at)
        at = pl.multiple_of(at, HALF)
        for h in range(HEADS):
            nat[pl.ds(at, HALF), h * HEAD_DIM : (h + 1) * HEAD_DIM] = big[
                pl.ds(at * HEADS + h, HALF, stride=HEADS), :
            ].astype(BF16)

    att_rows(core * HALF)
    tiles_4(att, att_sem)
    att_rows((1 - core) * HALF)
    loads[8].wait()
    pro[pl.ds(me, 1)] = dot_nt(wo_t[...], nat[...]).astype(BF16)[None]
    tiles_1(pro, pro_sem)
    tiles_2(pro, pro_sem)
    gather_3(hid, hid_sem)
    gather_4(hid, hid_sem)
    big[...] = hid[...].reshape(TOKENS * HEADS, HEAD_DIM).astype(F32)
    for h in range(HEADS):
        hid_t[h * HEAD_DIM : (h + 1) * HEAD_DIM, :] = big[pl.ds(h, TOKENS, stride=HEADS), :].T
    tiles_3(pro, pro_sem)
    tiles_4(pro, pro_sem)

    cols = wo_t.shape[0]
    total = jnp.zeros((cols, TOKENS), F32)
    for n in range(TOKENS):
        n_core, n_y, n_x = n % 2, (n // 2) % RING, n // (2 * RING)
        slot = n_core * HALF + (n_x * RING + n_y if n_core else n_y * RING + n_x)
        rows = slice(n * cols, (n + 1) * cols)
        block = pro[slot]
        proj_n[rows, :] = block
        block = hid_t[rows, :] + block.astype(F32)
        res[rows, :] = block
        total = total + block
    mean = jnp.sum(total, axis=0, keepdims=True) / d_model
    total = jnp.zeros((HEAD_DIM, TOKENS), F32)
    for h in range(HEADS):
        centered = res[h * HEAD_DIM : (h + 1) * HEAD_DIM, :] - mean
        total = total + centered * centered
    variance = jnp.sum(total, axis=0, keepdims=True) / d_model
    inverse = 1.0 / jnp.sqrt(jnp.maximum(variance, 0.25))
    for h in range(HEADS):
        rows = slice(h * HEAD_DIM, (h + 1) * HEAD_DIM)
        norm_t[rows, :] = ((res[rows, :] - mean) * inverse * gain_b[rows, :]).astype(BF16)

    loads[10].wait()
    loads[11].wait()
    normed = norm_t[...]
    picked = dot_nt(placed.astype(BF16), normed).astype(BF16)
    both = dot(up_t[...], normed)
    lhs[0:shared_units, :] = jax.nn.gelu(both[0:shared_units], approximate=True).astype(BF16)
    expert_row = lax.broadcasted_iota(jnp.int32, (experts, TOKENS), 0)
    chosen = jnp.sum(
        jnp.where(jnp.broadcast_to(routes, (experts, TOKENS)) == expert_row, both[shared_units:], 0.0),
        axis=0,
        keepdims=True,
    )
    gate = 1.0 / (1.0 + jnp.exp(-chosen))
    slot_gate = jnp.sum(placed * gate, axis=1, keepdims=True)
    left = dot_nt(eye(TOKENS), lhs[...]).astype(BF16)
    nat[:, 0 : lhs.shape[0]] = left
    loads[13].wait()
    inner = jax.nn.gelu(dot(picked, eup_v[...]), approximate=True).astype(BF16)
    loads[14].wait()
    result = dot(inner, edn_v[...])
    loads[12].wait()
    rhs[shared_units:, :] = (result * slot_gate).astype(BF16)

    other = pl.multiple_of((1 - core) * HALF, HALF)
    mine_at = pl.multiple_of(core * HALF, HALF)
    depth = lhs.shape[0]
    step = 256
    theirs = nat[pl.ds(other, HALF), 0:depth]
    for at in range(0, d_model, step):
        piece = dot(theirs, rhs[:, at : at + step]).astype(BF16)
        d_send[:, :, at : at + step] = piece.reshape(RING, RING, step)
    for k in FAR_FIRST + (0,):
        block = (first + k) % RING
        send(d_send.at[block], d_recv.at[block], d_sem.at[0, k], d_sem.at[1, k], partner)
    ours = nat[pl.ds(mine_at, HALF), 0:depth]
    for at in range(0, d_model, step):
        part[:, at : at + step] = dot(ours, rhs[:, at : at + step])
    for k in FAR_FIRST + (0,):
        block = (second + k) % RING
        arrived(d_recv.at[block], d_sem.at[0, k], d_sem.at[1, k])
        rows = pl.ds(pl.multiple_of(block * RING, RING), RING)
        both_cores = part[rows, :] + d_recv[block].astype(F32)
        if k:
            p_send[k - 1] = both_cores.astype(BF16)
            send(p_send.at[k - 1], p_recv.at[k - 1], p_sem.at[0, k], p_sem.at[1, k], on_second(k))
        else:
            summed = both_cores
    own_column = (
        lax.broadcasted_iota(jnp.int32, (HEADS, TOKENS), 1) == me
    ).astype(BF16)
    own = hid_tile + diagonal(dot_nt(own_column, proj_n[...]))
    for k in NEAR_FIRST:
        arrived(p_recv.at[k - 1], p_sem.at[0, k], p_sem.at[1, k])
        summed = summed + p_recv[k - 1].astype(F32)
    for h in range(HEADS):
        tok[pl.ds(h, RING, stride=HEADS), :] = summed[:, h * HEAD_DIM : (h + 1) * HEAD_DIM]
    for k in FAR_FIRST:
        to = pl.multiple_of(((first + k) % RING) * HEADS, HEADS)
        send(tok.at[pl.ds(to, HEADS)], t_recv.at[k - 1], t_sem.at[0, k], t_sem.at[1, k], on_first(k))
    own = own + tok[pl.ds(pl.multiple_of(first * HEADS, HEADS), HEADS), :]
    for k in NEAR_FIRST:
        arrived(t_recv.at[k - 1], t_sem.at[0, k], t_sem.at[1, k])
        own = own + t_recv[k - 1]
    for h in range(HEADS):
        out_ref[:, h * HEAD_DIM : (h + 1) * HEAD_DIM] = own[h : h + 1, :].astype(BF16)
    for copy in sent:
        copy.wait_send()


def body(
    query, key_new, value_new, key_cache, value_cache, lengths, hidden, routes, w_out, ln_gain,
    router, shared_up, shared_down, expert_up, expert_down,
):
    key_cache = key_cache.reshape(key_cache.shape[1:])
    value_cache = value_cache.reshape(value_cache.shape[1:])
    lengths = lengths.reshape(1, 1)
    routes = routes.reshape(1, -1)
    ln_gain = ln_gain.reshape(-1, HEAD_DIM)
    w_out, router, shared_up = w_out.T, router.T, shared_up.T
    args = (
        query, key_new, value_new, key_cache, value_cache, lengths, hidden, routes, w_out, ln_gain,
        router, shared_up, shared_down, expert_up, expert_down,
    )
    d = query.shape[1]
    units = shared_up.shape[0]
    slots = TOKENS * 4 // 32
    tile = (TOKENS, HEADS, HEAD_DIM)

    def own(a):
        return pltpu.VMEM(a.shape, a.dtype)

    dma = pltpu.SemaphoreType.DMA
    scratch = [own(a) for a in args[:10]]
    scratch += [
        pltpu.VMEM((units + router.shape[0], d), BF16),
        pltpu.VMEM((units + slots, d), BF16),
        own(expert_up),
        own(expert_down),
        pltpu.VMEM(tile, BF16),
        pltpu.VMEM(tile, BF16),
        pltpu.VMEM((TOKENS, w_out.shape[0], TOKENS), BF16),
        pltpu.VMEM((TOKENS * HEADS, HEAD_DIM), F32),
        pltpu.VMEM((d, TOKENS), F32),
        pltpu.VMEM((d, TOKENS), F32),
        pltpu.VMEM((TOKENS, d), BF16),
        pltpu.VMEM((d, TOKENS), F32),
        pltpu.VMEM((d, TOKENS), BF16),
        pltpu.VMEM((d, TOKENS), BF16),
        pltpu.VMEM((HALF, d), F32),
        pltpu.VMEM((RING, RING, d), BF16),
        pltpu.VMEM((RING, RING, d), BF16),
        pltpu.VMEM((RING - 1, RING, d), BF16),
        pltpu.VMEM((RING - 1, RING, d), BF16),
        pltpu.VMEM((RING * HEADS, HEAD_DIM), F32),
        pltpu.VMEM((RING - 1, HEADS, HEAD_DIM), F32),
        pltpu.VMEM((units + slots, TOKENS), BF16),
        dma((15,)),
        dma((6, RING)),
        dma((2, RING)),
        dma((2, RING)),
        dma((2, RING)),
    ]
    scratch += 2 * (2 * [dma((1, RING))] + 4 * [dma((RING, RING))])
    return pl.pallas_call(
        kernel,
        out_shape=jax.ShapeDtypeStruct((1, d), BF16),
        in_specs=[pl.BlockSpec(memory_space=pl.ANY)] * 15,
        out_specs=pl.BlockSpec(memory_space=pltpu.VMEM),
        scratch_shapes=scratch,
        compiler_params=pltpu.CompilerParams(collective_id=0, has_side_effects=True),
        name="decode_layer",
    )(*args)


def solution(mesh):
    torus = Mesh(
        mesh.devices.reshape(mesh.shape["group"], RING, RING, 2),
        ("group", "expert_0", "expert_1", "expert_2"),
    )
    placed = (
        P(GROUP_EXPERT, None),
        P(GROUP_EXPERT, None),
        P(GROUP_EXPERT, None),
        P(GROUP_EXPERT, None, None),
        P(GROUP_EXPERT, None, None),
        P(GROUP_EXPERT),
        P(GROUP_EXPERT, None),
        P("group"),
        P(None, EXPERT),
        P(),
        P(),
        P(None, EXPERT),
        P(EXPERT, None),
        P(None, EXPERT),
        P(EXPERT, None),
    )
    return jax.shard_map(
        body, mesh=torus, in_specs=placed, out_specs=P(GROUP_EXPERT, None), check_vma=False
    )
```

```python
import functools
import math

import jax
import jax.numpy as jnp
from jax import lax
from jax.experimental import pallas as pl
from jax.experimental.pallas import tpu as pltpu
from jax.sharding import Mesh
from jax.sharding import PartitionSpec as P

HEADS = 16
HEAD_DIM = 128
FF = 4096
RING = 8
TOKENS = 2 * RING * RING
HALF = RING * RING
EXPERT = ("expert_0", "expert_1", "expert_2")
GROUP_EXPERT = ("group", "expert_0", "expert_1", "expert_2")
MESH = pl.DeviceIdType.MESH
F32 = jnp.float32
BF16 = jnp.bfloat16
FAR_FIRST = (4, 3, 5, 2, 6, 1, 7)
NEAR_FIRST = (1, 7, 2, 6, 3, 5, 4)


def dot(a, b):
    return jnp.dot(a, b, preferred_element_type=F32)


def dot_nt(a, b):
    return lax.dot_general(a, b, (((1,), (1,)), ((), ())), preferred_element_type=F32)


def eye(n):
    return (
        lax.broadcasted_iota(jnp.int32, (n, n), 0) == lax.broadcasted_iota(jnp.int32, (n, n), 1)
    ).astype(BF16)


def diagonal(x):
    row = lax.broadcasted_iota(jnp.int32, (HEADS, HEAD_DIM), 0)
    out = jnp.zeros((HEADS, HEAD_DIM), F32)
    for h in range(HEADS):
        out = jnp.where(row == h, x[:, h * HEAD_DIM : (h + 1) * HEAD_DIM], out)
    return out


def kernel(*refs):
    ins, out_ref, vm, sems = refs[:15], refs[15], refs[16:-9], refs[-9:]
    (
        rows_v, k_v, v_v, len_v, rt_v, wo_t, gain_v, up_t, rhs, eup_v, edn_v, att, hid, pro, big,
        hid_t, gain_b, nat, res, proj_n, norm_t, part, p_send, p_recv, tok, t_recv, lhs,
    ) = vm
    load_sem, att_sem, hid_sem, pro_sem, down_sem, act_sem, slot_sem, p_sem, t_sem = sems
    d_model = rows_v.shape[2]
    experts, shared_units = ins[10].shape[0], ins[11].shape[0]
    slots = TOKENS * 4 // 32

    x = lax.axis_index("expert_0")
    y = lax.axis_index("expert_1")
    core = lax.axis_index("expert_2")
    first = x * (1 - core) + y * core
    second = y * (1 - core) + x * core
    me = core * HALF + second * RING + first

    def on_first(k):
        return {
            "expert_0": (x + k * (1 - core)) % RING,
            "expert_1": (y + k * core) % RING,
            "expert_2": core,
        }

    def on_second(k):
        return {
            "expert_0": (x + k * core) % RING,
            "expert_1": (y + k * (1 - core)) % RING,
            "expert_2": core,
        }

    partner = {"expert_0": x, "expert_1": y, "expert_2": 1 - core}

    barrier = pltpu.get_barrier_semaphore()
    for k in range(1, RING):
        pl.semaphore_signal(barrier, inc=1, device_id=on_first(k), device_id_type=MESH)
        pl.semaphore_signal(barrier, inc=1, device_id=on_second(k), device_id_type=MESH)
    pl.semaphore_signal(barrier, inc=1, device_id=partner, device_id_type=MESH)

    query_v, key_v, value_v, hid_v = (rows_v.at[i] for i in range(4))

    def load(i, target, sem):
        copy = pltpu.make_async_copy(ins[i], target, load_sem.at[sem])
        copy.start()
        return copy

    for i, row in ((0, query_v), (1, key_v), (2, value_v), (6, hid_v)):
        load(i, row, 0)
    rows_load = pltpu.make_async_copy(rows_v, rows_v, load_sem.at[0])
    k_load = load(3, k_v, 1)
    len_load = load(5, len_v, 2)
    v_load = load(4, v_v, 3)
    gain_load = load(9, gain_v, 4)
    rt_load = load(7, rt_v, 5)
    down_load = load(12, rhs.at[pl.ds(0, shared_units)], 6)
    wo_load = load(8, wo_t, 7)
    load(11, up_t.at[pl.ds(0, shared_units)], 8)
    load(10, up_t.at[pl.ds(shared_units, experts)], 8)
    up_load = pltpu.make_async_copy(up_t, up_t, load_sem.at[8])
    eup_load = load(13, eup_v, 9)
    edn_load = load(14, edn_v, 10)

    def send(src, dst, send_sem, recv_sem, to):
        copy = pltpu.make_async_remote_copy(
            src_ref=src, dst_ref=dst, send_sem=send_sem, recv_sem=recv_sem, device_id=to,
            device_id_type=MESH,
        )
        copy.start()

    def wait_for(ref, sem):
        pltpu.make_async_copy(ref, ref, sem).wait()

    def slot_of(k):
        return core * HALF + second * RING + (first - k + RING) % RING

    def row_of(second_k, of=core):
        return pl.ds(of * HALF + ((second - second_k + RING) % RING) * RING, RING)

    def pass_on(buf, sem, k):
        tile = buf.at[pl.ds(slot_of(k), 1)]
        for j in FAR_FIRST:
            send(tile, tile, sem.at[0], sem.at[8 + j], on_second(j))

    def tiles_1(buf, sem):
        tile = buf.at[pl.ds(me, 1)]
        for k in FAR_FIRST:
            send(tile, tile, sem.at[0], sem.at[1 + k], on_first(k))
        pass_on(buf, sem, 0)

    def tiles_2(buf, sem):
        for k in NEAR_FIRST:
            wait_for(buf.at[pl.ds(slot_of(k), 1)], sem.at[1 + k])
            pass_on(buf, sem, k)
        row = buf.at[row_of(0)]
        send(row, row, sem.at[0], sem.at[1], partner)

    def tiles_3(buf, sem):
        for j in NEAR_FIRST:
            row = buf.at[row_of(j)]
            wait_for(row, sem.at[8 + j])
            send(row, row, sem.at[0], sem.at[1], partner)

    def tiles_4(buf, sem):
        wait_for(buf.at[pl.ds((1 - core) * HALF, HALF)], sem.at[1])

    def steps_1(buf, sem):
        tile = buf.at[pl.ds(me, 1)]
        for k in FAR_FIRST:
            send(tile, tile, sem.at[0], sem.at[1], on_first(k))

    def steps_2(buf, sem):
        wait_for(buf.at[pl.ds(0, RING - 1)], sem.at[1])
        row = buf.at[row_of(0)]
        for k in FAR_FIRST:
            send(row, row, sem.at[0], sem.at[2], on_second(k))

    def steps_3(buf, sem):
        wait_for(buf.at[pl.ds(0, HALF - RING)], sem.at[2])
        half = buf.at[pl.ds(core * HALF, HALF)]
        send(half, half, sem.at[0], sem.at[3], partner)

    def steps_4(buf, sem):
        wait_for(buf.at[pl.ds((1 - core) * HALF, HALF)], sem.at[3])

    rows_load.wait()
    head_row = lax.broadcasted_iota(jnp.int32, (HEADS, d_model), 0)
    head_of_lane = lax.broadcasted_iota(jnp.int32, (HEADS, d_model), 1) // HEAD_DIM
    own_head = head_row == head_of_lane
    scale = 1.0 / math.sqrt(HEAD_DIM)

    def spread(ref):
        return jnp.broadcast_to(ref[...].astype(F32), (HEADS, d_model))

    hid_tile = diagonal(spread(hid_v))
    hid[pl.ds(me, 1)] = hid_tile.astype(BF16)[None]
    query = jnp.where(own_head, spread(query_v), 0.0)
    own_score = jnp.sum(query * spread(key_v), axis=1, keepdims=True) * scale
    query = query.astype(BF16)
    k_load.wait()
    len_load.wait()
    scores = dot_nt(query, k_v[...]) * scale
    position = lax.broadcasted_iota(jnp.int32, scores.shape, 1)
    scores = jnp.where(position < jnp.broadcast_to(len_v[...], scores.shape), scores, -1e30)
    top = jnp.maximum(jnp.max(scores, axis=1, keepdims=True), own_score)
    weights = jnp.exp(scores - top)
    own_weight = jnp.exp(own_score - top)
    normalizer = jnp.sum(weights, axis=1, keepdims=True) + own_weight
    weights = (weights / normalizer).astype(BF16)
    own_weight = (own_weight / normalizer).astype(BF16).astype(F32)
    v_load.wait()
    mixed = dot(weights, v_v[...]) + own_weight * spread(value_v)
    att[pl.ds(me, 1)] = diagonal(mixed).astype(BF16)[None]

    pl.semaphore_wait(barrier, 2 * (RING - 1) + 1)
    tiles_1(att, att_sem)
    steps_1(hid, hid_sem)

    gain_load.wait()
    for h in range(HEADS):
        block = gain_v[h : h + 1, :].astype(F32)
        gain_b[h * HEAD_DIM : (h + 1) * HEAD_DIM, :] = jnp.broadcast_to(
            block, (HEAD_DIM, TOKENS)
        ).T
    rt_load.wait()
    nat_id = lax.broadcasted_iota(jnp.int32, (TOKENS, TOKENS), 0)
    lane = lax.broadcasted_iota(jnp.int32, (TOKENS, TOKENS), 1)
    lane_core, lane_second, lane_first = lane // HALF, (lane // RING) % RING, lane % RING
    lane_x = lane_first * (1 - lane_core) + lane_second * lane_core
    lane_y = lane_second * (1 - lane_core) + lane_first * lane_core
    to_slot = (nat_id == (lane_x * RING + lane_y) * 2 + lane_core).astype(BF16)
    routes = dot(
        jnp.broadcast_to(rt_v[...], (8, TOKENS)).astype(F32).astype(BF16), to_slot
    )[0:1].astype(jnp.int32)
    device = (x * RING + y) * 2 + core
    mine = device * eup_v.shape[1] // FF
    member = routes == mine
    rank = dot(
        jnp.broadcast_to(member.astype(F32), (8, TOKENS)).astype(BF16), (nat_id <= lane).astype(BF16)
    )[0:1].astype(jnp.int32) - 1
    slot_id = lax.broadcasted_iota(jnp.int32, (slots, TOKENS), 0)
    placed = jnp.where(
        jnp.broadcast_to(member, (slots, TOKENS))
        & (jnp.broadcast_to(rank, (slots, TOKENS)) == slot_id),
        1.0,
        0.0,
    )
    placed_at, depth = 2 * shared_units, lhs.shape[0]
    lhs[placed_at : placed_at + slots, :] = placed.astype(BF16)
    lhs[placed_at + slots :, :] = placed.astype(BF16)
    down_load.wait()
    send(
        rhs.at[pl.ds(0, shared_units)], rhs.at[pl.ds(shared_units, shared_units)], down_sem.at[0],
        down_sem.at[1], partner,
    )

    tiles_2(att, att_sem)
    tiles_3(att, att_sem)
    steps_2(hid, hid_sem)

    def relayout(buf, at):
        at = pl.multiple_of(at, HALF)
        rows = pl.ds(pl.multiple_of(at * HEADS, HALF * HEADS), HALF * HEADS)
        big[rows, :] = buf[pl.ds(at, HALF)].reshape(HALF * HEADS, HEAD_DIM).astype(F32)

    def att_rows(at):
        relayout(att, at)
        at = pl.multiple_of(at, HALF)
        for h in range(HEADS):
            nat[pl.ds(at, HALF), h * HEAD_DIM : (h + 1) * HEAD_DIM] = big[
                pl.ds(at * HEADS + h, HALF, stride=HEADS), :
            ].astype(BF16)

    att_rows(core * HALF)
    tiles_4(att, att_sem)
    att_rows((1 - core) * HALF)
    wo_load.wait()
    pro[pl.ds(me, 1)] = dot_nt(wo_t[...], nat[...]).astype(BF16)[None]
    tiles_1(pro, pro_sem)
    tiles_2(pro, pro_sem)
    steps_3(hid, hid_sem)
    steps_4(hid, hid_sem)
    big[...] = hid[...].reshape(TOKENS * HEADS, HEAD_DIM).astype(F32)
    for h in range(HEADS):
        hid_t[h * HEAD_DIM : (h + 1) * HEAD_DIM, :] = big[pl.ds(h, TOKENS, stride=HEADS), :].T
    tiles_3(pro, pro_sem)
    tiles_4(pro, pro_sem)

    cols = wo_t.shape[0]
    total = jnp.zeros((cols, TOKENS), F32)
    for n in range(TOKENS):
        n_core, n_y, n_x = n % 2, (n // 2) % RING, n // (2 * RING)
        slot = n_core * HALF + (n_x * RING + n_y if n_core else n_y * RING + n_x)
        rows = slice(n * cols, (n + 1) * cols)
        block = pro[slot]
        proj_n[rows, :] = block
        block = hid_t[rows, :] + block.astype(F32)
        res[rows, :] = block
        total = total + block
    mean = jnp.sum(total, axis=0, keepdims=True) / d_model
    total = jnp.zeros((HEAD_DIM, TOKENS), F32)
    for h in range(HEADS):
        centered = res[h * HEAD_DIM : (h + 1) * HEAD_DIM, :] - mean
        total = total + centered * centered
    variance = jnp.sum(total, axis=0, keepdims=True) / d_model
    inverse = 1.0 / jnp.sqrt(jnp.maximum(variance, 0.25))
    for h in range(HEADS):
        rows = slice(h * HEAD_DIM, (h + 1) * HEAD_DIM)
        norm_t[rows, :] = ((res[rows, :] - mean) * inverse * gain_b[rows, :]).astype(BF16)

    up_load.wait()
    normed = norm_t[...]
    both = dot(up_t[...], normed)
    lhs[0:shared_units, :] = jax.nn.gelu(both[0:shared_units], approximate=True).astype(BF16)
    send(
        lhs.at[pl.ds(0, shared_units)], lhs.at[pl.ds(shared_units, shared_units)], act_sem.at[0],
        act_sem.at[1], partner,
    )
    picked = dot_nt(placed.astype(BF16), normed).astype(BF16)
    expert_row = lax.broadcasted_iota(jnp.int32, (experts, TOKENS), 0)
    chosen = jnp.sum(
        jnp.where(jnp.broadcast_to(routes, (experts, TOKENS)) == expert_row, both[shared_units:], 0.0),
        axis=0,
        keepdims=True,
    )
    gate = 1.0 / (1.0 + jnp.exp(-chosen))
    slot_gate = jnp.sum(placed * gate, axis=1, keepdims=True)
    eup_load.wait()
    inner = jax.nn.gelu(dot(picked, eup_v[...]), approximate=True).astype(BF16)
    edn_load.wait()
    wide = d_model // 2
    theirs = placed_at + slots
    for i in range(2):
        at = i * wide
        result = dot(inner, edn_v[:, at : at + wide])
        rhs[placed_at:theirs, at : at + wide] = (result * slot_gate).astype(BF16)
        send(
            rhs.at[pl.ds(placed_at, slots), pl.ds(at, wide)],
            rhs.at[pl.ds(theirs, slots), pl.ds(at, wide)],
            slot_sem.at[0], slot_sem.at[1 + i], partner,
        )

    wait_for(rhs.at[pl.ds(0, shared_units)], down_sem.at[1])
    wait_for(lhs.at[pl.ds(0, shared_units)], act_sem.at[1])
    chosen_half = (
        lax.broadcasted_iota(jnp.int32, (HALF, TOKENS), 1)
        == lax.broadcasted_iota(jnp.int32, (HALF, TOKENS), 0) + core * HALF
    ).astype(BF16)
    left = dot_nt(chosen_half, lhs[...]).astype(BF16)
    step = 256
    for i in range(2):
        wait_for(rhs.at[pl.ds(theirs, slots), pl.ds(i * wide, wide)], slot_sem.at[1 + i])
        for at in range(i * wide, (i + 1) * wide, step):
            part[:, at : at + step] = dot(left, rhs[:, at : at + step])
    for k in FAR_FIRST:
        rows = pl.ds(pl.multiple_of(((second + k) % RING) * RING, RING), RING)
        p_send[k - 1] = part[rows, :].astype(BF16)
        send(p_send.at[k - 1], p_recv.at[k - 1], p_sem.at[0], p_sem.at[1], on_second(k))
    summed = part[pl.ds(pl.multiple_of(second * RING, RING), RING), :]
    own_column = (
        lax.broadcasted_iota(jnp.int32, (HEADS, TOKENS), 1) == me
    ).astype(BF16)
    own = hid_tile + diagonal(dot_nt(own_column, proj_n[...]))
    wait_for(p_recv, p_sem.at[1])
    for k in range(RING - 1):
        summed = summed + p_recv[k].astype(F32)
    for h in range(HEADS):
        tok[pl.ds(h, RING, stride=HEADS), :] = summed[:, h * HEAD_DIM : (h + 1) * HEAD_DIM]
    for k in FAR_FIRST:
        to = pl.multiple_of(((first + k) % RING) * HEADS, HEADS)
        send(tok.at[pl.ds(to, HEADS)], t_recv.at[k - 1], t_sem.at[0], t_sem.at[1], on_first(k))
    own = own + tok[pl.ds(pl.multiple_of(first * HEADS, HEADS), HEADS), :]
    wait_for(t_recv, t_sem.at[1])
    for k in range(RING - 1):
        own = own + t_recv[k]
    for h in range(HEADS):
        out_ref[:, h * HEAD_DIM : (h + 1) * HEAD_DIM] = own[h : h + 1, :].astype(BF16)
    every_tile = pl.ds(0, TOKENS - 1)
    for buf, sem in ((att, att_sem), (hid, hid_sem), (pro, pro_sem)):
        wait_for(buf.at[every_tile], sem.at[0])
    wait_for(rhs.at[pl.ds(0, shared_units)], down_sem.at[0])
    wait_for(lhs.at[pl.ds(0, shared_units)], act_sem.at[0])
    wait_for(rhs.at[pl.ds(placed_at, slots)], slot_sem.at[0])
    wait_for(p_send, p_sem.at[0])
    wait_for(t_recv, t_sem.at[0])


def body(
    query, key_new, value_new, key_cache, value_cache, lengths, hidden, routes, w_out, ln_gain,
    router, shared_up, shared_down, expert_up, expert_down,
):
    key_cache = key_cache.reshape(key_cache.shape[1:])
    value_cache = value_cache.reshape(value_cache.shape[1:])
    lengths = lengths.reshape(1, 1)
    routes = routes.reshape(1, -1)
    ln_gain = ln_gain.reshape(-1, HEAD_DIM)
    w_out, router, shared_up = w_out.T, router.T, shared_up.T
    args = (
        query, key_new, value_new, key_cache, value_cache, lengths, hidden, routes, w_out, ln_gain,
        router, shared_up, shared_down, expert_up, expert_down,
    )
    d = query.shape[1]
    units = shared_up.shape[0]
    slots = TOKENS * 4 // 32
    tile = (TOKENS, HEADS, HEAD_DIM)

    def own(a):
        return pltpu.VMEM(a.shape, a.dtype)

    dma = pltpu.SemaphoreType.DMA
    scratch = [
        pltpu.VMEM((4, 1, d), BF16),
        own(key_cache),
        own(value_cache),
        own(lengths),
        own(routes),
        own(w_out),
        own(ln_gain),
        pltpu.VMEM((units + router.shape[0], d), BF16),
        pltpu.VMEM((2 * (units + slots), d), BF16),
        own(expert_up),
        own(expert_down),
        pltpu.VMEM(tile, BF16),
        pltpu.VMEM(tile, BF16),
        pltpu.VMEM((TOKENS, w_out.shape[0], TOKENS), BF16),
        pltpu.VMEM((TOKENS * HEADS, HEAD_DIM), F32),
        pltpu.VMEM((d, TOKENS), F32),
        pltpu.VMEM((d, TOKENS), F32),
        pltpu.VMEM((TOKENS, d), BF16),
        pltpu.VMEM((d, TOKENS), F32),
        pltpu.VMEM((d, TOKENS), BF16),
        pltpu.VMEM((d, TOKENS), BF16),
        pltpu.VMEM((HALF, d), F32),
        pltpu.VMEM((RING - 1, RING, d), BF16),
        pltpu.VMEM((RING - 1, RING, d), BF16),
        pltpu.VMEM((RING * HEADS, HEAD_DIM), F32),
        pltpu.VMEM((RING - 1, HEADS, HEAD_DIM), F32),
        pltpu.VMEM((2 * (units + slots), TOKENS), BF16),
    ]
    scratch += [dma((n,)) for n in (11, 16, 4, 16, 2, 2, 3, 2, 2)]
    return pl.pallas_call(
        kernel,
        out_shape=jax.ShapeDtypeStruct((1, d), BF16),
        in_specs=[pl.BlockSpec(memory_space=pl.ANY)] * 15,
        out_specs=pl.BlockSpec(memory_space=pltpu.VMEM),
        scratch_shapes=scratch,
        compiler_params=pltpu.CompilerParams(collective_id=0, has_side_effects=True),
        name="decode_layer",
    )(*args)


def solution(mesh):
    torus = Mesh(
        mesh.devices.reshape(mesh.shape["group"], RING, RING, 2),
        ("group", "expert_0", "expert_1", "expert_2"),
    )
    placed = (
        P(GROUP_EXPERT, None),
        P(GROUP_EXPERT, None),
        P(GROUP_EXPERT, None),
        P(GROUP_EXPERT, None, None),
        P(GROUP_EXPERT, None, None),
        P(GROUP_EXPERT),
        P(GROUP_EXPERT, None),
        P("group"),
        P(None, EXPERT),
        P(),
        P(),
        P(None, EXPERT),
        P(EXPERT, None),
        P(None, EXPERT),
        P(EXPERT, None),
    )
    return jax.shard_map(
        body, mesh=torus, in_specs=placed, out_specs=P(GROUP_EXPERT, None), check_vma=False
    )
```

```python
import functools
import math

import jax
import jax.numpy as jnp
from jax import lax
from jax.experimental import pallas as pl
from jax.experimental.pallas import tpu as pltpu
from jax.sharding import Mesh
from jax.sharding import PartitionSpec as P

HEADS = 16
HEAD_DIM = 128
FF = 4096
RING = 8
TOKENS = 2 * RING * RING
HALF = RING * RING
EXPERT = ("expert_0", "expert_1", "expert_2")
GROUP_EXPERT = ("group", "expert_0", "expert_1", "expert_2")
MESH = pl.DeviceIdType.MESH
QUARTERS = 4
F32 = jnp.float32
BF16 = jnp.bfloat16
FAR = RING // 2
FAR_FIRST = (4, 3, 5, 2, 6, 1, 7)
NEAR_FIRST = (1, 7, 2, 6, 3, 5, 4)


def dot(a, b):
    return jnp.dot(a, b, preferred_element_type=F32)


def dot_nt(a, b):
    return lax.dot_general(a, b, (((1,), (1,)), ((), ())), preferred_element_type=F32)


def eye(n):
    return (
        lax.broadcasted_iota(jnp.int32, (n, n), 0) == lax.broadcasted_iota(jnp.int32, (n, n), 1)
    ).astype(BF16)


def diagonal(x):
    row = lax.broadcasted_iota(jnp.int32, (HEADS, HEAD_DIM), 0)
    out = jnp.zeros((HEADS, HEAD_DIM), F32)
    for h in range(HEADS):
        out = jnp.where(row == h, x[:, h * HEAD_DIM : (h + 1) * HEAD_DIM], out)
    return out


def kernel(*refs):
    ins, out_ref, vm, sems = refs[:15], refs[15], refs[16:-9], refs[-9:]
    (
        rows_v, k_v, v_v, len_v, rt_v, wo_t, gain_v, up_t, rhs, eup_v, edn_v, att, hid, pro, big,
        hid_t, gain_b, nat, res, proj_n, norm_t, p_send, p_recv, tok, t_send, t_recv,
        lhs,
    ) = vm
    load_sem, att_sem, hid_sem, pro_sem, down_sem, act_sem, slot_sem, p_sem, t_sem = sems
    d_model = rows_v.shape[2]
    experts, shared_units = ins[10].shape[0], ins[11].shape[0]
    slots = TOKENS * 4 // 32

    x = lax.axis_index("expert_0")
    y = lax.axis_index("expert_1")
    core = lax.axis_index("expert_2")
    first = x * (1 - core) + y * core
    second = y * (1 - core) + x * core
    me = core * HALF + second * RING + first

    def on_first(k, to=core):
        return {
            "expert_0": (x + k * (1 - core)) % RING,
            "expert_1": (y + k * core) % RING,
            "expert_2": to,
        }

    def on_second(k, to=core):
        return {
            "expert_0": (x + k * core) % RING,
            "expert_1": (y + k * (1 - core)) % RING,
            "expert_2": to,
        }

    partner = {"expert_0": x, "expert_1": y, "expert_2": 1 - core}

    barrier = pltpu.get_barrier_semaphore()
    for k in range(1, RING):
        pl.semaphore_signal(barrier, inc=1, device_id=on_first(k), device_id_type=MESH)
        pl.semaphore_signal(barrier, inc=1, device_id=on_second(k), device_id_type=MESH)
    pl.semaphore_signal(barrier, inc=1, device_id=partner, device_id_type=MESH)
    across = on_first(FAR, 1 - core)
    pl.semaphore_signal(barrier, inc=1, device_id=across, device_id_type=MESH)

    query_v, key_v, value_v, hid_v = (rows_v.at[i] for i in range(4))

    def load(i, target, sem):
        copy = pltpu.make_async_copy(ins[i], target, load_sem.at[sem])
        copy.start()
        return copy

    for i, row in ((0, query_v), (1, key_v), (2, value_v), (6, hid_v)):
        load(i, row, 0)
    rows_load = pltpu.make_async_copy(rows_v, rows_v, load_sem.at[0])
    k_load = load(3, k_v, 1)
    len_load = load(5, len_v, 2)
    v_load = load(4, v_v, 3)
    gain_load = load(9, gain_v, 4)
    rt_load = load(7, rt_v, 5)
    down_load = load(12, rhs.at[pl.ds(0, shared_units)], 6)
    wo_load = load(8, wo_t, 7)
    load(11, up_t.at[pl.ds(0, shared_units)], 8)
    load(10, up_t.at[pl.ds(shared_units, experts)], 8)
    up_load = pltpu.make_async_copy(up_t, up_t, load_sem.at[8])
    eup_load = load(13, eup_v, 9)
    edn_load = load(14, edn_v, 10)

    def send(src, dst, send_sem, recv_sem, to):
        copy = pltpu.make_async_remote_copy(
            src_ref=src, dst_ref=dst, send_sem=send_sem, recv_sem=recv_sem, device_id=to,
            device_id_type=MESH,
        )
        copy.start()

    def wait_for(ref, sem):
        pltpu.make_async_copy(ref, ref, sem).wait()

    def slot_of(k):
        return core * HALF + second * RING + (first - k + RING) % RING

    def row_of(second_k, of=core):
        return pl.ds(of * HALF + ((second - second_k + RING) % RING) * RING, RING)

    def pass_on(buf, sem, k):
        tile = buf.at[pl.ds(slot_of(k), 1)]
        send(tile, tile, sem.at[0], sem.at[16], on_second(FAR, 1 - core))
        for j in FAR_FIRST:
            send(tile, tile, sem.at[0], sem.at[8 + j], on_second(j))

    def tiles_1(buf, sem):
        tile = buf.at[pl.ds(me, 1)]
        for k in FAR_FIRST:
            send(tile, tile, sem.at[0], sem.at[1 + k], on_first(k))
        pass_on(buf, sem, 0)

    def tiles_2(buf, sem):
        for k in NEAR_FIRST:
            wait_for(buf.at[pl.ds(slot_of(k), 1)], sem.at[1 + k])
            pass_on(buf, sem, k)
        row = buf.at[row_of(0)]
        send(row, row, sem.at[0], sem.at[1], partner)

    def tiles_3(buf, sem):
        for j in NEAR_FIRST:
            row = buf.at[row_of(j)]
            wait_for(row, sem.at[8 + j])
            if j != FAR:
                send(row, row, sem.at[0], sem.at[1], partner)

    def tiles_4(buf, sem):
        wait_for(buf.at[pl.ds((1 - core) * HALF, HALF - RING)], sem.at[1])
        wait_for(buf.at[pl.ds((1 - core) * HALF, RING)], sem.at[16])

    def steps_1(buf, sem):
        tile = buf.at[pl.ds(me, 1)]
        for k in FAR_FIRST:
            send(tile, tile, sem.at[0], sem.at[1], on_first(k))

    def steps_2(buf, sem):
        wait_for(buf.at[pl.ds(0, RING - 1)], sem.at[1])
        row = buf.at[row_of(0)]
        for k in FAR_FIRST:
            send(row, row, sem.at[0], sem.at[2], on_second(k))

    def steps_3(buf, sem):
        wait_for(buf.at[pl.ds(0, HALF - RING)], sem.at[2])
        half = buf.at[pl.ds(core * HALF, HALF)]
        send(half, half, sem.at[0], sem.at[3], partner)

    def steps_4(buf, sem):
        wait_for(buf.at[pl.ds((1 - core) * HALF, HALF)], sem.at[3])

    rows_load.wait()
    head_row = lax.broadcasted_iota(jnp.int32, (HEADS, d_model), 0)
    head_of_lane = lax.broadcasted_iota(jnp.int32, (HEADS, d_model), 1) // HEAD_DIM
    own_head = head_row == head_of_lane
    scale = 1.0 / math.sqrt(HEAD_DIM)

    def spread(ref):
        return jnp.broadcast_to(ref[...].astype(F32), (HEADS, d_model))

    hid_tile = diagonal(spread(hid_v))
    hid[pl.ds(me, 1)] = hid_tile.astype(BF16)[None]
    query = jnp.where(own_head, spread(query_v), 0.0)
    own_score = jnp.sum(query * spread(key_v), axis=1, keepdims=True) * scale
    query = query.astype(BF16)
    k_load.wait()
    len_load.wait()
    scores = dot_nt(query, k_v[...]) * scale
    position = lax.broadcasted_iota(jnp.int32, scores.shape, 1)
    scores = jnp.where(position < jnp.broadcast_to(len_v[...], scores.shape), scores, -1e30)
    top = jnp.maximum(jnp.max(scores, axis=1, keepdims=True), own_score)
    weights = jnp.exp(scores - top)
    own_weight = jnp.exp(own_score - top)
    normalizer = jnp.sum(weights, axis=1, keepdims=True) + own_weight
    weights = (weights / normalizer).astype(BF16)
    own_weight = (own_weight / normalizer).astype(BF16).astype(F32)
    v_load.wait()
    mixed = dot(weights, v_v[...]) + own_weight * spread(value_v)
    att[pl.ds(me, 1)] = diagonal(mixed).astype(BF16)[None]

    pl.semaphore_wait(barrier, 2 * RING)
    tiles_1(att, att_sem)
    steps_1(hid, hid_sem)

    gain_load.wait()
    for h in range(HEADS):
        block = gain_v[h : h + 1, :].astype(F32)
        gain_b[h * HEAD_DIM : (h + 1) * HEAD_DIM, :] = jnp.broadcast_to(
            block, (HEAD_DIM, TOKENS)
        ).T
    rt_load.wait()
    nat_id = lax.broadcasted_iota(jnp.int32, (TOKENS, TOKENS), 0)
    lane = lax.broadcasted_iota(jnp.int32, (TOKENS, TOKENS), 1)
    lane_core, lane_second, lane_first = lane // HALF, (lane // RING) % RING, lane % RING
    lane_x = lane_first * (1 - lane_core) + lane_second * lane_core
    lane_y = lane_second * (1 - lane_core) + lane_first * lane_core
    to_slot = (nat_id == (lane_x * RING + lane_y) * 2 + lane_core).astype(BF16)
    routes = dot(
        jnp.broadcast_to(rt_v[...], (8, TOKENS)).astype(F32).astype(BF16), to_slot
    )[0:1].astype(jnp.int32)
    device = (x * RING + y) * 2 + core
    mine = device * eup_v.shape[1] // FF
    member = routes == mine
    rank = dot(
        jnp.broadcast_to(member.astype(F32), (8, TOKENS)).astype(BF16), (nat_id <= lane).astype(BF16)
    )[0:1].astype(jnp.int32) - 1
    slot_id = lax.broadcasted_iota(jnp.int32, (slots, TOKENS), 0)
    placed = jnp.where(
        jnp.broadcast_to(member, (slots, TOKENS))
        & (jnp.broadcast_to(rank, (slots, TOKENS)) == slot_id),
        1.0,
        0.0,
    )
    placed_at, depth = 2 * shared_units, lhs.shape[0]
    lhs[placed_at : placed_at + slots, :] = placed.astype(BF16)
    lhs[placed_at + slots :, :] = placed.astype(BF16)
    down_load.wait()
    send(
        rhs.at[pl.ds(0, shared_units)], rhs.at[pl.ds(shared_units, shared_units)], down_sem.at[0],
        down_sem.at[1], partner,
    )

    tiles_2(att, att_sem)
    tiles_3(att, att_sem)
    steps_2(hid, hid_sem)

    def relayout(buf, at):
        at = pl.multiple_of(at, HALF)
        rows = pl.ds(pl.multiple_of(at * HEADS, HALF * HEADS), HALF * HEADS)
        big[rows, :] = buf[pl.ds(at, HALF)].reshape(HALF * HEADS, HEAD_DIM).astype(F32)

    def att_rows(at):
        relayout(att, at)
        at = pl.multiple_of(at, HALF)
        for h in range(HEADS):
            nat[pl.ds(at, HALF), h * HEAD_DIM : (h + 1) * HEAD_DIM] = big[
                pl.ds(at * HEADS + h, HALF, stride=HEADS), :
            ].astype(BF16)

    att_rows(core * HALF)
    tiles_4(att, att_sem)
    att_rows((1 - core) * HALF)
    wo_load.wait()
    pro[pl.ds(me, 1)] = dot_nt(wo_t[...], nat[...]).astype(BF16)[None]
    tiles_1(pro, pro_sem)
    tiles_2(pro, pro_sem)
    steps_3(hid, hid_sem)
    steps_4(hid, hid_sem)
    big[...] = hid[...].reshape(TOKENS * HEADS, HEAD_DIM).astype(F32)
    for h in range(HEADS):
        hid_t[h * HEAD_DIM : (h + 1) * HEAD_DIM, :] = big[pl.ds(h, TOKENS, stride=HEADS), :].T
    tiles_3(pro, pro_sem)
    tiles_4(pro, pro_sem)

    cols = wo_t.shape[0]
    total = jnp.zeros((cols, TOKENS), F32)
    for n in range(TOKENS):
        n_core, n_y, n_x = n % 2, (n // 2) % RING, n // (2 * RING)
        slot = n_core * HALF + (n_x * RING + n_y if n_core else n_y * RING + n_x)
        rows = slice(n * cols, (n + 1) * cols)
        block = pro[slot]
        proj_n[rows, :] = block
        block = hid_t[rows, :] + block.astype(F32)
        res[rows, :] = block
        total = total + block
    mean = jnp.sum(total, axis=0, keepdims=True) / d_model
    total = jnp.zeros((HEAD_DIM, TOKENS), F32)
    for h in range(HEADS):
        centered = res[h * HEAD_DIM : (h + 1) * HEAD_DIM, :] - mean
        total = total + centered * centered
    variance = jnp.sum(total, axis=0, keepdims=True) / d_model
    inverse = 1.0 / jnp.sqrt(jnp.maximum(variance, 0.25))
    for h in range(HEADS):
        rows = slice(h * HEAD_DIM, (h + 1) * HEAD_DIM)
        norm_t[rows, :] = ((res[rows, :] - mean) * inverse * gain_b[rows, :]).astype(BF16)

    up_load.wait()
    normed = norm_t[...]
    both = dot(up_t[...], normed)
    lhs[0:shared_units, :] = jax.nn.gelu(both[0:shared_units], approximate=True).astype(BF16)
    send(
        lhs.at[pl.ds(0, shared_units)], lhs.at[pl.ds(shared_units, shared_units)], act_sem.at[0],
        act_sem.at[1], partner,
    )
    picked = dot_nt(placed.astype(BF16), normed).astype(BF16)
    expert_row = lax.broadcasted_iota(jnp.int32, (experts, TOKENS), 0)
    chosen = jnp.sum(
        jnp.where(jnp.broadcast_to(routes, (experts, TOKENS)) == expert_row, both[shared_units:], 0.0),
        axis=0,
        keepdims=True,
    )
    gate = 1.0 / (1.0 + jnp.exp(-chosen))
    slot_gate = jnp.sum(placed * gate, axis=1, keepdims=True)
    eup_load.wait()
    inner = jax.nn.gelu(dot(picked, eup_v[...]), approximate=True).astype(BF16)
    edn_load.wait()
    wide = d_model // QUARTERS
    theirs = placed_at + slots
    for i in range(QUARTERS):
        at = i * wide
        result = dot(inner, edn_v[:, at : at + wide])
        rhs[placed_at:theirs, at : at + wide] = (result * slot_gate).astype(BF16)
        send(
            rhs.at[pl.ds(placed_at, slots), pl.ds(at, wide)],
            rhs.at[pl.ds(theirs, slots), pl.ds(at, wide)],
            slot_sem.at[0], slot_sem.at[1 + i], partner,
        )

    wait_for(rhs.at[pl.ds(0, shared_units)], down_sem.at[1])
    wait_for(lhs.at[pl.ds(0, shared_units)], act_sem.at[1])
    chosen_half = (
        lax.broadcasted_iota(jnp.int32, (HALF, TOKENS), 1)
        == lax.broadcasted_iota(jnp.int32, (HALF, TOKENS), 0) + core * HALF
    ).astype(BF16)
    left = dot_nt(chosen_half, lhs[...]).astype(BF16)
    for i in range(QUARTERS):
        columns = pl.ds(i * wide, wide)
        wait_for(rhs.at[pl.ds(theirs, slots), columns], slot_sem.at[1 + i])
        for at in range(i * wide, (i + 1) * wide, 256):
            piece = dot(left, rhs[:, at : at + 256]).astype(BF16)
            p_send[:, :, at : at + 256] = piece.reshape(RING, RING, 256)
        for k in FAR_FIRST:
            block = p_send.at[(second + k) % RING, :, columns]
            send(block, p_recv.at[k - 1, :, columns], p_sem.at[0], p_sem.at[1], on_second(k))
    summed = p_send[second].astype(F32)
    own_column = (
        lax.broadcasted_iota(jnp.int32, (HEADS, TOKENS), 1) == me
    ).astype(BF16)
    own = hid_tile + diagonal(dot_nt(own_column, proj_n[...]))
    wait_for(p_recv, p_sem.at[1])
    for k in range(RING - 1):
        summed = summed + p_recv[k].astype(F32)
    for h in range(HEADS):
        tok[pl.ds(h, RING, stride=HEADS), :] = summed[:, h * HEAD_DIM : (h + 1) * HEAD_DIM]
    t_send[...] = tok[...].astype(BF16)
    for k in FAR_FIRST:
        to = pl.multiple_of(((first + k) % RING) * HEADS, HEADS)
        send(t_send.at[pl.ds(to, HEADS)], t_recv.at[k - 1], t_sem.at[0], t_sem.at[1], on_first(k))
    own = own + tok[pl.ds(pl.multiple_of(first * HEADS, HEADS), HEADS), :]
    wait_for(t_recv, t_sem.at[1])
    for k in range(RING - 1):
        own = own + t_recv[k].astype(F32)
    for h in range(HEADS):
        out_ref[:, h * HEAD_DIM : (h + 1) * HEAD_DIM] = own[h : h + 1, :].astype(BF16)
    every_tile = pl.ds(0, TOKENS - 1)
    for buf, sem in ((att, att_sem), (hid, hid_sem), (pro, pro_sem)):
        wait_for(buf.at[every_tile], sem.at[0])
    wait_for(rhs.at[pl.ds(0, shared_units)], down_sem.at[0])
    wait_for(lhs.at[pl.ds(0, shared_units)], act_sem.at[0])
    wait_for(rhs.at[pl.ds(placed_at, slots)], slot_sem.at[0])
    wait_for(p_recv, p_sem.at[0])
    wait_for(t_recv, t_sem.at[0])


def body(
    query, key_new, value_new, key_cache, value_cache, lengths, hidden, routes, w_out, ln_gain,
    router, shared_up, shared_down, expert_up, expert_down,
):
    key_cache = key_cache.reshape(key_cache.shape[1:])
    value_cache = value_cache.reshape(value_cache.shape[1:])
    lengths = lengths.reshape(1, 1)
    routes = routes.reshape(1, -1)
    ln_gain = ln_gain.reshape(-1, HEAD_DIM)
    w_out, router, shared_up = w_out.T, router.T, shared_up.T
    args = (
        query, key_new, value_new, key_cache, value_cache, lengths, hidden, routes, w_out, ln_gain,
        router, shared_up, shared_down, expert_up, expert_down,
    )
    d = query.shape[1]
    units = shared_up.shape[0]
    slots = TOKENS * 4 // 32
    tile = (TOKENS, HEADS, HEAD_DIM)

    def own(a):
        return pltpu.VMEM(a.shape, a.dtype)

    dma = pltpu.SemaphoreType.DMA
    scratch = [
        pltpu.VMEM((4, 1, d), BF16),
        own(key_cache),
        own(value_cache),
        own(lengths),
        own(routes),
        own(w_out),
        own(ln_gain),
        pltpu.VMEM((units + router.shape[0], d), BF16),
        pltpu.VMEM((2 * (units + slots), d), BF16),
        own(expert_up),
        own(expert_down),
        pltpu.VMEM(tile, BF16),
        pltpu.VMEM(tile, BF16),
        pltpu.VMEM((TOKENS, w_out.shape[0], TOKENS), BF16),
        pltpu.VMEM((TOKENS * HEADS, HEAD_DIM), F32),
        pltpu.VMEM((d, TOKENS), F32),
        pltpu.VMEM((d, TOKENS), F32),
        pltpu.VMEM((TOKENS, d), BF16),
        pltpu.VMEM((d, TOKENS), F32),
        pltpu.VMEM((d, TOKENS), BF16),
        pltpu.VMEM((d, TOKENS), BF16),
        pltpu.VMEM((RING, RING, d), BF16),
        pltpu.VMEM((RING - 1, RING, d), BF16),
        pltpu.VMEM((RING * HEADS, HEAD_DIM), F32),
        pltpu.VMEM((RING * HEADS, HEAD_DIM), BF16),
        pltpu.VMEM((RING - 1, HEADS, HEAD_DIM), BF16),
        pltpu.VMEM((2 * (units + slots), TOKENS), BF16),
    ]
    scratch += [dma((n,)) for n in (11, 17, 4, 17, 2, 2, 1 + QUARTERS, 2, 2)]
    return pl.pallas_call(
        kernel,
        out_shape=jax.ShapeDtypeStruct((1, d), BF16),
        in_specs=[pl.BlockSpec(memory_space=pl.ANY)] * 15,
        out_specs=pl.BlockSpec(memory_space=pltpu.VMEM),
        scratch_shapes=scratch,
        compiler_params=pltpu.CompilerParams(collective_id=0, has_side_effects=True),
        name="decode_layer",
    )(*args)


def solution(mesh):
    torus = Mesh(
        mesh.devices.reshape(mesh.shape["group"], RING, RING, 2),
        ("group", "expert_0", "expert_1", "expert_2"),
    )
    placed = (
        P(GROUP_EXPERT, None),
        P(GROUP_EXPERT, None),
        P(GROUP_EXPERT, None),
        P(GROUP_EXPERT, None, None),
        P(GROUP_EXPERT, None, None),
        P(GROUP_EXPERT),
        P(GROUP_EXPERT, None),
        P("group"),
        P(None, EXPERT),
        P(),
        P(),
        P(None, EXPERT),
        P(EXPERT, None),
        P(None, EXPERT),
        P(EXPERT, None),
    )
    return jax.shard_map(
        body, mesh=torus, in_specs=placed, out_specs=P(GROUP_EXPERT, None), check_vma=False
    )
```

```python
import functools
import math

import jax
import jax.numpy as jnp
from jax import lax
from jax.experimental import pallas as pl
from jax.experimental.pallas import tpu as pltpu
from jax.sharding import Mesh
from jax.sharding import PartitionSpec as P

HEADS = 16
HEAD_DIM = 128
FF = 4096
RING = 8
TOKENS = 2 * RING * RING
HALF = RING * RING
EXPERT = ("expert_0", "expert_1", "expert_2")
GROUP_EXPERT = ("group", "expert_0", "expert_1", "expert_2")
MESH = pl.DeviceIdType.MESH
PIECES = 2
F32 = jnp.float32
BF16 = jnp.bfloat16
FAR_FIRST = (4, 3, 5, 2, 6, 1, 7)
NEAR_FIRST = (1, 7, 2, 6, 3, 5, 4)


def dot(a, b):
    return jnp.dot(a, b, preferred_element_type=F32)


def dot_nt(a, b):
    return lax.dot_general(a, b, (((1,), (1,)), ((), ())), preferred_element_type=F32)


def eye(n):
    return (
        lax.broadcasted_iota(jnp.int32, (n, n), 0) == lax.broadcasted_iota(jnp.int32, (n, n), 1)
    ).astype(BF16)


def diagonal(x):
    row = lax.broadcasted_iota(jnp.int32, (HEADS, HEAD_DIM), 0)
    out = jnp.zeros((HEADS, HEAD_DIM), F32)
    for h in range(HEADS):
        out = jnp.where(row == h, x[:, h * HEAD_DIM : (h + 1) * HEAD_DIM], out)
    return out


def kernel(*refs):
    ins, out_ref, vm, sems = refs[:15], refs[15], refs[16:-9], refs[-9:]
    (
        rows_v, k_v, v_v, len_v, rt_v, wo_t, gain_v, up_t, rhs, eup_v, edn_v, att, hid, pro, big,
        hid_t, gain_b, nat, res, proj_n, norm_t, p_send, p_recv, tok, t_recv, lhs,
    ) = vm
    load_sem, att_sem, hid_sem, pro_sem, down_sem, up_sem, slot_sem, p_sem, t_sem = sems
    d_model = rows_v.shape[2]
    experts, shared_units = ins[10].shape[0], ins[11].shape[0]
    slots = TOKENS * 4 // 32

    x = lax.axis_index("expert_0")
    y = lax.axis_index("expert_1")
    core = lax.axis_index("expert_2")
    first = x * (1 - core) + y * core
    second = y * (1 - core) + x * core
    me = core * HALF + second * RING + first

    def on_first(k):
        return {
            "expert_0": (x + k * (1 - core)) % RING,
            "expert_1": (y + k * core) % RING,
            "expert_2": core,
        }

    def on_second(k):
        return {
            "expert_0": (x + k * core) % RING,
            "expert_1": (y + k * (1 - core)) % RING,
            "expert_2": core,
        }

    partner = {"expert_0": x, "expert_1": y, "expert_2": 1 - core}

    barrier = pltpu.get_barrier_semaphore()
    for k in FAR_FIRST:
        pl.semaphore_signal(barrier, inc=1, device_id=on_first(k), device_id_type=MESH)
        pl.semaphore_signal(barrier, inc=1, device_id=on_second(k), device_id_type=MESH)
    pl.semaphore_signal(barrier, inc=1, device_id=partner, device_id_type=MESH)

    query_v, key_v, value_v, hid_v = (rows_v.at[i] for i in range(4))

    def load(i, target, sem):
        copy = pltpu.make_async_copy(ins[i], target, load_sem.at[sem])
        copy.start()
        return copy

    for i, row in ((0, query_v), (1, key_v), (2, value_v), (6, hid_v)):
        load(i, row, 0)
    rows_load = pltpu.make_async_copy(rows_v, rows_v, load_sem.at[0])
    k_load = load(3, k_v, 1)
    len_load = load(5, len_v, 2)
    v_load = load(4, v_v, 3)
    gain_load = load(9, gain_v, 4)
    rt_load = load(7, rt_v, 5)
    down_load = load(12, rhs.at[pl.ds(0, shared_units)], 6)
    wo_load = load(8, wo_t, 7)
    load(11, up_t.at[pl.ds(0, shared_units)], 8)
    load(10, up_t.at[pl.ds(2 * shared_units, experts)], 8)
    up_load = pltpu.make_async_copy(
        up_t.at[pl.ds(0, shared_units + experts)], up_t.at[pl.ds(0, shared_units + experts)],
        load_sem.at[8],
    )
    eup_load = load(13, eup_v, 9)
    edn_load = load(14, edn_v, 10)

    def send(src, dst, send_sem, recv_sem, to):
        copy = pltpu.make_async_remote_copy(
            src_ref=src, dst_ref=dst, send_sem=send_sem, recv_sem=recv_sem, device_id=to,
            device_id_type=MESH,
        )
        copy.start()

    def wait_for(ref, sem):
        pltpu.make_async_copy(ref, ref, sem).wait()

    def slot_of(k):
        return core * HALF + second * RING + (first - k + RING) % RING

    def row_of(second_k, of=core):
        return pl.ds(of * HALF + ((second - second_k + RING) % RING) * RING, RING)

    def pass_on(buf, sem, k):
        tile = buf.at[pl.ds(slot_of(k), 1)]
        for j in FAR_FIRST:
            send(tile, tile, sem.at[0], sem.at[8 + j], on_second(j))

    def zero_last(at):
        last = NEAR_FIRST[-1]
        order = [k + (last - k) * (1 - ((k - at + RING) % RING + RING - 1) // RING) for k in NEAR_FIRST[:-1]]
        return order + [at + last * (1 - (at + RING - 1) // RING)]

    def tiles_1(buf, sem):
        tile = buf.at[pl.ds(me, 1)]
        for k in FAR_FIRST:
            send(tile, tile, sem.at[0], sem.at[1 + k], on_first(k))
        pass_on(buf, sem, 0)

    def tiles_2(buf, sem, order):
        for k in order:
            wait_for(buf.at[pl.ds(slot_of(k), 1)], sem.at[1 + k])
            pass_on(buf, sem, k)
        row = buf.at[row_of(0)]
        send(row, row, sem.at[0], sem.at[1], partner)

    def tiles_3(buf, sem, order):
        for j in order:
            row = buf.at[row_of(j)]
            wait_for(row, sem.at[8 + j])
            send(row, row, sem.at[0], sem.at[1], partner)

    def tiles_4(buf, sem):
        wait_for(buf.at[pl.ds((1 - core) * HALF, HALF)], sem.at[1])

    def steps_1(buf, sem):
        tile = buf.at[pl.ds(me, 1)]
        for k in FAR_FIRST:
            send(tile, tile, sem.at[0], sem.at[1], on_first(k))

    def steps_2(buf, sem):
        wait_for(buf.at[pl.ds(0, RING - 1)], sem.at[1])
        row = buf.at[row_of(0)]
        for k in FAR_FIRST:
            send(row, row, sem.at[0], sem.at[2], on_second(k))

    def steps_3(buf, sem):
        wait_for(buf.at[pl.ds(0, HALF - RING)], sem.at[2])
        half = buf.at[pl.ds(core * HALF, HALF)]
        send(half, half, sem.at[0], sem.at[3], partner)

    def steps_4(buf, sem):
        wait_for(buf.at[pl.ds((1 - core) * HALF, HALF)], sem.at[3])

    rows_load.wait()
    head_row = lax.broadcasted_iota(jnp.int32, (HEADS, d_model), 0)
    head_of_lane = lax.broadcasted_iota(jnp.int32, (HEADS, d_model), 1) // HEAD_DIM
    own_head = head_row == head_of_lane
    scale = 1.0 / math.sqrt(HEAD_DIM)

    def spread(ref):
        return jnp.broadcast_to(ref[...].astype(F32), (HEADS, d_model))

    hid_tile = diagonal(spread(hid_v))
    hid[pl.ds(me, 1)] = hid_tile.astype(BF16)[None]
    query = jnp.where(own_head, spread(query_v), 0.0)
    own_score = jnp.sum(query * spread(key_v), axis=1, keepdims=True) * scale
    query = query.astype(BF16)
    k_load.wait()
    len_load.wait()
    scores = dot_nt(query, k_v[...]) * scale
    position = lax.broadcasted_iota(jnp.int32, scores.shape, 1)
    scores = jnp.where(position < jnp.broadcast_to(len_v[...], scores.shape), scores, -1e30)
    top = jnp.maximum(jnp.max(scores, axis=1, keepdims=True), own_score)
    weights = jnp.exp(scores - top)
    own_weight = jnp.exp(own_score - top)
    normalizer = jnp.sum(weights, axis=1, keepdims=True) + own_weight
    weights = (weights / normalizer).astype(BF16)
    own_weight = (own_weight / normalizer).astype(BF16).astype(F32)
    v_load.wait()
    mixed = dot(weights, v_v[...]) + own_weight * spread(value_v)
    att[pl.ds(me, 1)] = diagonal(mixed).astype(BF16)[None]

    pl.semaphore_wait(barrier, 2 * (RING - 1) + 1)
    tiles_1(att, att_sem)
    steps_1(hid, hid_sem)

    gain_load.wait()
    for h in range(HEADS):
        block = gain_v[h : h + 1, :].astype(F32)
        gain_b[h * HEAD_DIM : (h + 1) * HEAD_DIM, :] = jnp.broadcast_to(
            block, (HEAD_DIM, TOKENS)
        ).T
    rt_load.wait()
    nat_id = lax.broadcasted_iota(jnp.int32, (TOKENS, TOKENS), 0)
    lane = lax.broadcasted_iota(jnp.int32, (TOKENS, TOKENS), 1)
    lane_core, lane_second, lane_first = lane // HALF, (lane // RING) % RING, lane % RING
    lane_x = lane_first * (1 - lane_core) + lane_second * lane_core
    lane_y = lane_second * (1 - lane_core) + lane_first * lane_core
    to_slot = (nat_id == (lane_x * RING + lane_y) * 2 + lane_core).astype(BF16)
    routes = dot(
        jnp.broadcast_to(rt_v[...], (8, TOKENS)).astype(F32).astype(BF16), to_slot
    )[0:1].astype(jnp.int32)
    device = (x * RING + y) * 2 + core
    mine = device * eup_v.shape[1] // FF
    member = routes == mine
    rank = dot(
        jnp.broadcast_to(member.astype(F32), (8, TOKENS)).astype(BF16), (nat_id <= lane).astype(BF16)
    )[0:1].astype(jnp.int32) - 1
    slot_id = lax.broadcasted_iota(jnp.int32, (slots, TOKENS), 0)
    placed = jnp.where(
        jnp.broadcast_to(member, (slots, TOKENS))
        & (jnp.broadcast_to(rank, (slots, TOKENS)) == slot_id),
        1.0,
        0.0,
    )
    placed_at, depth = 2 * shared_units, lhs.shape[0]
    lhs[placed_at : placed_at + slots, :] = placed.astype(BF16)
    lhs[placed_at + slots :, :] = placed.astype(BF16)
    down_load.wait()
    send(
        rhs.at[pl.ds(0, shared_units)], rhs.at[pl.ds(shared_units, shared_units)], down_sem.at[0],
        down_sem.at[1], partner,
    )
    up_load.wait()
    send(
        up_t.at[pl.ds(0, shared_units)], up_t.at[pl.ds(shared_units, shared_units)], up_sem.at[0],
        up_sem.at[1], partner,
    )

    tiles_2(att, att_sem, zero_last(first))
    tiles_3(att, att_sem, zero_last(second))
    steps_2(hid, hid_sem)

    def projected(at):
        at = pl.multiple_of(at, HALF)
        every = pl.ds(pl.multiple_of(at * HEADS, HALF * HEADS), HALF * HEADS)
        big[every, :] = att[pl.ds(at, HALF)].reshape(HALF * HEADS, HEAD_DIM).astype(F32)
        for h in range(HEADS):
            nat[:, h * HEAD_DIM : (h + 1) * HEAD_DIM] = big[
                pl.ds(at * HEADS + h, HALF, stride=HEADS), :
            ].astype(BF16)
        return dot_nt(wo_t[...], nat[...])

    wo_load.wait()
    here = projected(core * HALF)
    tiles_4(att, att_sem)
    there = projected((1 - core) * HALF)
    pro[me] = jnp.where(
        core == 0,
        jnp.concatenate([here, there], axis=1),
        jnp.concatenate([there, here], axis=1),
    ).astype(BF16)
    tiles_1(pro, pro_sem)
    tiles_2(pro, pro_sem, NEAR_FIRST)
    steps_3(hid, hid_sem)
    steps_4(hid, hid_sem)
    big[...] = hid[...].reshape(TOKENS * HEADS, HEAD_DIM).astype(F32)
    for h in range(HEADS):
        hid_t[h * HEAD_DIM : (h + 1) * HEAD_DIM, :] = big[pl.ds(h, TOKENS, stride=HEADS), :].T
    tiles_3(pro, pro_sem, NEAR_FIRST)
    tiles_4(pro, pro_sem)

    cols = wo_t.shape[0]
    total = jnp.zeros((cols, TOKENS), F32)
    for n in range(TOKENS):
        n_core, n_y, n_x = n % 2, (n // 2) % RING, n // (2 * RING)
        slot = n_core * HALF + (n_x * RING + n_y if n_core else n_y * RING + n_x)
        rows = slice(n * cols, (n + 1) * cols)
        block = pro[slot]
        proj_n[rows, :] = block
        block = hid_t[rows, :] + block.astype(F32)
        res[rows, :] = block
        total = total + block
    mean = jnp.sum(total, axis=0, keepdims=True) / d_model
    total = jnp.zeros((HEAD_DIM, TOKENS), F32)
    for h in range(HEADS):
        centered = res[h * HEAD_DIM : (h + 1) * HEAD_DIM, :] - mean
        total = total + centered * centered
    variance = jnp.sum(total, axis=0, keepdims=True) / d_model
    inverse = 1.0 / jnp.sqrt(jnp.maximum(variance, 0.25))
    for h in range(HEADS):
        rows = slice(h * HEAD_DIM, (h + 1) * HEAD_DIM)
        norm_t[rows, :] = ((res[rows, :] - mean) * inverse * gain_b[rows, :]).astype(BF16)

    normed = norm_t[...]
    picked = dot_nt(placed.astype(BF16), normed).astype(BF16)
    logits = dot(up_t[2 * shared_units :, :], normed)
    expert_row = lax.broadcasted_iota(jnp.int32, (experts, TOKENS), 0)
    chosen = jnp.sum(
        jnp.where(jnp.broadcast_to(routes, (experts, TOKENS)) == expert_row, logits, 0.0),
        axis=0,
        keepdims=True,
    )
    gate = 1.0 / (1.0 + jnp.exp(-chosen))
    slot_gate = jnp.sum(placed * gate, axis=1, keepdims=True)
    eup_load.wait()
    inner = jax.nn.gelu(dot(picked, eup_v[...]), approximate=True).astype(BF16)
    edn_load.wait()
    wide = d_model // PIECES
    theirs = placed_at + slots
    for i in range(PIECES):
        at = i * wide
        result = dot(inner, edn_v[:, at : at + wide])
        rhs[placed_at:theirs, at : at + wide] = (result * slot_gate).astype(BF16)
        send(
            rhs.at[pl.ds(placed_at, slots), pl.ds(at, wide)],
            rhs.at[pl.ds(theirs, slots), pl.ds(at, wide)],
            slot_sem.at[0], slot_sem.at[1 + i], partner,
        )

    wait_for(rhs.at[pl.ds(0, shared_units)], down_sem.at[1])
    wait_for(up_t.at[pl.ds(0, shared_units)], up_sem.at[1])
    both = dot(up_t[0 : 2 * shared_units, :], normed)
    lhs[0 : 2 * shared_units, :] = jax.nn.gelu(both, approximate=True).astype(BF16)
    chosen_half = (
        lax.broadcasted_iota(jnp.int32, (HALF, TOKENS), 1)
        == lax.broadcasted_iota(jnp.int32, (HALF, TOKENS), 0) + core * HALF
    ).astype(BF16)
    left = dot_nt(chosen_half, lhs[...]).astype(BF16)
    for i in range(PIECES):
        columns = pl.ds(i * wide, wide)
        wait_for(rhs.at[pl.ds(theirs, slots), columns], slot_sem.at[1 + i])
        for at in range(i * wide, (i + 1) * wide, 256):
            piece = dot(left, rhs[:, at : at + 256]).astype(BF16)
            p_send[:, :, at : at + 256] = piece.reshape(RING, RING, 256)
        for k in FAR_FIRST:
            block = p_send.at[(second + k) % RING, :, columns]
            send(block, p_recv.at[k - 1, :, columns], p_sem.at[0], p_sem.at[1], on_second(k))
    summed = p_send[second].astype(F32)
    own_column = (
        lax.broadcasted_iota(jnp.int32, (HEADS, TOKENS), 1) == me
    ).astype(BF16)
    own = hid_tile + diagonal(dot_nt(own_column, proj_n[...]))
    wait_for(p_recv, p_sem.at[1])
    for k in range(RING - 1):
        summed = summed + p_recv[k].astype(F32)
    for h in range(HEADS):
        tok[pl.ds(h, RING, stride=HEADS), :] = summed[:, h * HEAD_DIM : (h + 1) * HEAD_DIM]
    for k in FAR_FIRST:
        to = pl.multiple_of(((first + k) % RING) * HEADS, HEADS)
        send(tok.at[pl.ds(to, HEADS)], t_recv.at[k - 1], t_sem.at[0], t_sem.at[1], on_first(k))
    own = own + tok[pl.ds(pl.multiple_of(first * HEADS, HEADS), HEADS), :]
    wait_for(t_recv, t_sem.at[1])
    for k in range(RING - 1):
        own = own + t_recv[k]
    for h in range(HEADS):
        out_ref[:, h * HEAD_DIM : (h + 1) * HEAD_DIM] = own[h : h + 1, :].astype(BF16)
    every_tile = pl.ds(0, TOKENS - 1)
    for buf, sem in ((att, att_sem), (hid, hid_sem), (pro, pro_sem)):
        wait_for(buf.at[every_tile], sem.at[0])
    wait_for(rhs.at[pl.ds(0, shared_units)], down_sem.at[0])
    wait_for(up_t.at[pl.ds(0, shared_units)], up_sem.at[0])
    wait_for(rhs.at[pl.ds(placed_at, slots)], slot_sem.at[0])
    wait_for(p_recv, p_sem.at[0])
    wait_for(t_recv, t_sem.at[0])


def body(
    query, key_new, value_new, key_cache, value_cache, lengths, hidden, routes, w_out, ln_gain,
    router, shared_up, shared_down, expert_up, expert_down,
):
    key_cache = key_cache.reshape(key_cache.shape[1:])
    value_cache = value_cache.reshape(value_cache.shape[1:])
    lengths = lengths.reshape(1, 1)
    routes = routes.reshape(1, -1)
    ln_gain = ln_gain.reshape(-1, HEAD_DIM)
    w_out, router, shared_up = w_out.T, router.T, shared_up.T
    args = (
        query, key_new, value_new, key_cache, value_cache, lengths, hidden, routes, w_out, ln_gain,
        router, shared_up, shared_down, expert_up, expert_down,
    )
    d = query.shape[1]
    units = shared_up.shape[0]
    slots = TOKENS * 4 // 32
    tile = (TOKENS, HEADS, HEAD_DIM)

    def own(a):
        return pltpu.VMEM(a.shape, a.dtype)

    dma = pltpu.SemaphoreType.DMA
    scratch = [
        pltpu.VMEM((4, 1, d), BF16),
        own(key_cache),
        own(value_cache),
        own(lengths),
        own(routes),
        own(w_out),
        own(ln_gain),
        pltpu.VMEM((2 * units + router.shape[0], d), BF16),
        pltpu.VMEM((2 * (units + slots), d), BF16),
        own(expert_up),
        own(expert_down),
        pltpu.VMEM(tile, BF16),
        pltpu.VMEM(tile, BF16),
        pltpu.VMEM((TOKENS, w_out.shape[0], TOKENS), BF16),
        pltpu.VMEM((TOKENS * HEADS, HEAD_DIM), F32),
        pltpu.VMEM((d, TOKENS), F32),
        pltpu.VMEM((d, TOKENS), F32),
        pltpu.VMEM((HALF, d), BF16),
        pltpu.VMEM((d, TOKENS), F32),
        pltpu.VMEM((d, TOKENS), BF16),
        pltpu.VMEM((d, TOKENS), BF16),
        pltpu.VMEM((RING, RING, d), BF16),
        pltpu.VMEM((RING - 1, RING, d), BF16),
        pltpu.VMEM((RING * HEADS, HEAD_DIM), F32),
        pltpu.VMEM((RING - 1, HEADS, HEAD_DIM), F32),
        pltpu.VMEM((2 * (units + slots), TOKENS), BF16),
    ]
    scratch += [dma((n,)) for n in (11, 16, 4, 16, 2, 2, 1 + PIECES, 2, 2)]
    return pl.pallas_call(
        kernel,
        out_shape=jax.ShapeDtypeStruct((1, d), BF16),
        in_specs=[pl.BlockSpec(memory_space=pl.ANY)] * 15,
        out_specs=pl.BlockSpec(memory_space=pltpu.VMEM),
        scratch_shapes=scratch,
        compiler_params=pltpu.CompilerParams(collective_id=0, has_side_effects=True),
        name="decode_layer",
    )(*args)


def solution(mesh):
    torus = Mesh(
        mesh.devices.reshape(mesh.shape["group"], RING, RING, 2),
        ("group", "expert_0", "expert_1", "expert_2"),
    )
    placed = (
        P(GROUP_EXPERT, None),
        P(GROUP_EXPERT, None),
        P(GROUP_EXPERT, None),
        P(GROUP_EXPERT, None, None),
        P(GROUP_EXPERT, None, None),
        P(GROUP_EXPERT),
        P(GROUP_EXPERT, None),
        P("group"),
        P(None, EXPERT),
        P(),
        P(),
        P(None, EXPERT),
        P(EXPERT, None),
        P(None, EXPERT),
        P(EXPERT, None),
    )
    return jax.shard_map(
        body, mesh=torus, in_specs=placed, out_specs=P(GROUP_EXPERT, None), check_vma=False
    )
```

```python
import functools
import math

import jax
import jax.numpy as jnp
from jax import lax
from jax.experimental import pallas as pl
from jax.experimental.pallas import tpu as pltpu
from jax.sharding import Mesh
from jax.sharding import PartitionSpec as P

HEADS = 16
HEAD_DIM = 128
FF = 4096
RING = 8
TOKENS = 2 * RING * RING
HALF = RING * RING
EXPERT = ("expert_0", "expert_1", "expert_2")
GROUP_EXPERT = ("group", "expert_0", "expert_1", "expert_2")
MESH = pl.DeviceIdType.MESH
PIECES = 2
KEPT = 2
F32 = jnp.float32
BF16 = jnp.bfloat16
OWN = 0
PAIRS = ((1, 7), (2, 6), (3, 5), (4,))
FAR_FIRST = (4, 3, 5, 2, 6, 1, 7)
NEAR_FIRST = (1, 7, 2, 6, 3, 5, 4)


def dot(a, b):
    return jnp.dot(a, b, preferred_element_type=F32)


def dot_nt(a, b):
    return lax.dot_general(a, b, (((1,), (1,)), ((), ())), preferred_element_type=F32)


def eye(n):
    return (
        lax.broadcasted_iota(jnp.int32, (n, n), 0) == lax.broadcasted_iota(jnp.int32, (n, n), 1)
    ).astype(BF16)


def diagonal(x):
    row = lax.broadcasted_iota(jnp.int32, (HEADS, HEAD_DIM), 0)
    out = jnp.zeros((HEADS, HEAD_DIM), F32)
    for h in range(HEADS):
        out = jnp.where(row == h, x[:, h * HEAD_DIM : (h + 1) * HEAD_DIM], out)
    return out


def kernel(*refs):
    ins, out_ref, vm, sems = refs[:15], refs[15], refs[16:-10], refs[-10:]
    (
        rows_v, k_v, v_v, len_v, rt_v, wo_t, gain_v, up_t, rhs, eup_v, edn_v, att, hid, pro, big,
        hid_t, gain_b, nat, res, proj_n, norm_t, p_send, p_recv, tok, t_recv, lhs,
    ) = vm
    load_sem, att_sem, hid_sem, pro_sem, down_sem, up_sem, slot_sem, p_sem, t_sem, units_sem = sems
    d_model = rows_v.shape[2]
    experts, shared_units = ins[10].shape[0], ins[11].shape[0]
    slots = TOKENS * 4 // 32

    x = lax.axis_index("expert_0")
    y = lax.axis_index("expert_1")
    core = lax.axis_index("expert_2")
    first = x * (1 - core) + y * core
    second = y * (1 - core) + x * core
    me = core * HALF + second * RING + first

    def on_first(k):
        return {
            "expert_0": (x + k * (1 - core)) % RING,
            "expert_1": (y + k * core) % RING,
            "expert_2": core,
        }

    def on_second(k):
        return {
            "expert_0": (x + k * core) % RING,
            "expert_1": (y + k * (1 - core)) % RING,
            "expert_2": core,
        }

    def along(axis, k, to):
        return {
            "expert_0": (x + k * (1 - axis)) % RING,
            "expert_1": (y + k * axis) % RING,
            "expert_2": to,
        }

    partner = {"expert_0": x, "expert_1": y, "expert_2": 1 - core}

    barrier = pltpu.get_barrier_semaphore()
    for k in FAR_FIRST:
        pl.semaphore_signal(barrier, inc=1, device_id=on_first(k), device_id_type=MESH)
        pl.semaphore_signal(barrier, inc=1, device_id=on_second(k), device_id_type=MESH)
    pl.semaphore_signal(barrier, inc=1, device_id=partner, device_id_type=MESH)

    @pl.when(core == 1)
    def _():
        for k in FAR_FIRST:
            pl.semaphore_signal(barrier, inc=1, device_id=along(0, k, 0), device_id_type=MESH)


    query_v, key_v, value_v, hid_v = (rows_v.at[i] for i in range(4))

    def load(i, target, sem):
        copy = pltpu.make_async_copy(ins[i], target, load_sem.at[sem])
        copy.start()
        return copy

    for i, row in ((0, query_v), (1, key_v), (2, value_v), (6, hid_v)):
        load(i, row, 0)
    rows_load = pltpu.make_async_copy(rows_v, rows_v, load_sem.at[0])
    k_load = load(3, k_v, 1)
    len_load = load(5, len_v, 2)
    v_load = load(4, v_v, 3)
    gain_load = load(9, gain_v, 4)
    rt_load = load(7, rt_v, 5)
    down_load = load(12, rhs.at[pl.ds(0, shared_units)], 6)
    wo_load = load(8, wo_t, 7)
    load(11, up_t.at[pl.ds(0, shared_units)], 8)
    load(10, up_t.at[pl.ds(2 * shared_units, experts)], 8)
    up_load = pltpu.make_async_copy(
        up_t.at[pl.ds(0, shared_units + experts)], up_t.at[pl.ds(0, shared_units + experts)],
        load_sem.at[8],
    )
    units = ins[13].shape[1]
    kept = units // KEPT
    moved = units - kept
    eup_load = load(13, eup_v.at[:, pl.ds(0, units)], 9)
    edn_load = load(14, edn_v.at[pl.ds(0, units)], 10)

    def send(src, dst, send_sem, recv_sem, to):
        copy = pltpu.make_async_remote_copy(
            src_ref=src, dst_ref=dst, send_sem=send_sem, recv_sem=recv_sem, device_id=to,
            device_id_type=MESH,
        )
        copy.start()

    def wait_for(ref, sem):
        pltpu.make_async_copy(ref, ref, sem).wait()

    def row_of(second_k):
        return pl.ds(core * HALF + ((second - second_k + RING) % RING) * RING, RING)

    place = ((x, y), (y, x))

    def tile_at(buf, color, k):
        at, row = place[color]
        return buf.at[pl.ds(color * HALF + row * RING + (at - k + RING) % RING, 1)]

    def row_at(buf, color, j):
        return buf.at[
            pl.ds(color * HALF + ((place[color][1] - j + RING) % RING) * RING, RING)
        ]

    def pass_on(buf, sem, color, k):
        tile = tile_at(buf, color, k)
        for j in FAR_FIRST:
            pair = 19 + 4 * color + min(j, RING - j) - 1
            send(tile, tile, sem.at[1 - color], sem.at[pair], along(1 - color, j, 1))

    def tiles_1(buf, sem):
        tile = buf.at[pl.ds(me, 1)]

        @pl.when(core == 0)
        def _():
            for k in FAR_FIRST:
                send(tile, tile, sem.at[0], sem.at[4 + k], along(0, k, 1))
            send(tile, tile, sem.at[0], sem.at[4], partner)

        @pl.when(core == 1)
        def _():
            for k in FAR_FIRST:
                send(tile, tile, sem.at[0], sem.at[11 + k], along(1, k, 1))
            pass_on(buf, sem, 1, 0)

    def zero_last(at):
        last = NEAR_FIRST[-1]
        order = [
            k + (last - k) * (1 - ((k - at + RING) % RING + RING - 1) // RING)
            for k in NEAR_FIRST[:-1]
        ]
        return order + [at + last * (1 - (at + RING - 1) // RING)]

    def tiles_2(buf, sem, order):
        @pl.when(core == 1)
        def _():
            rows_left = RING - 1
            for color, k in order:
                tile = tile_at(buf, color, k)
                wait_for(tile, sem.at[(4, 11)[color] + k])
                pass_on(buf, sem, color, k)
                if color:
                    rows_left -= 1
                    if not rows_left:
                        row = row_at(buf, 1, 0)
                        send(row, row, sem.at[0], sem.at[2], partner)
                elif k is not OWN:
                    send(tile, tile, sem.at[1], sem.at[3], partner)

    def tiles_3(buf, sem, color):
        @pl.when(core == 1)
        def _():
            for i, pair in enumerate(PAIRS):
                wait_for(buf.at[pl.ds(0, RING * len(pair))], sem.at[19 + 4 * color + i])
                for j in pair:
                    row = row_at(buf, color, j)
                    send(row, row, sem.at[1 - color], sem.at[3 - color], partner)

        @pl.when(core == 0)
        def _():
            wait_for(buf.at[pl.ds(0, HALF - 1 + color)], sem.at[3 - color])

    def tiles_sent(buf, sem):
        @pl.when(core == 1)
        def _():
            wait_for(buf.at[pl.ds(0, 2 * HALF - 1)], sem.at[0])
            wait_for(buf.at[pl.ds(0, 2 * HALF - RING - 1)], sem.at[1])

        @pl.when(core == 0)
        def _():
            wait_for(buf.at[pl.ds(0, RING)], sem.at[0])

    def steps_1(buf, sem):
        tile = buf.at[pl.ds(me, 1)]
        for k in FAR_FIRST:
            send(tile, tile, sem.at[0], sem.at[1], on_first(k))

    def steps_2(buf, sem):
        wait_for(buf.at[pl.ds(0, RING - 1)], sem.at[1])
        row = buf.at[row_of(0)]
        for k in FAR_FIRST:
            send(row, row, sem.at[0], sem.at[2], on_second(k))

    def steps_3(buf, sem):
        wait_for(buf.at[pl.ds(0, HALF - RING)], sem.at[2])
        half = buf.at[pl.ds(core * HALF, HALF)]
        send(half, half, sem.at[0], sem.at[3], partner)

    def steps_4(buf, sem):
        wait_for(buf.at[pl.ds((1 - core) * HALF, HALF)], sem.at[3])

    rows_load.wait()
    head_row = lax.broadcasted_iota(jnp.int32, (HEADS, d_model), 0)
    head_of_lane = lax.broadcasted_iota(jnp.int32, (HEADS, d_model), 1) // HEAD_DIM
    own_head = head_row == head_of_lane
    scale = 1.0 / math.sqrt(HEAD_DIM)

    def spread(ref):
        return jnp.broadcast_to(ref[...].astype(F32), (HEADS, d_model))

    hid_tile = diagonal(spread(hid_v))
    hid[pl.ds(me, 1)] = hid_tile.astype(BF16)[None]
    query = jnp.where(own_head, spread(query_v), 0.0)
    own_score = jnp.sum(query * spread(key_v), axis=1, keepdims=True) * scale
    query = query.astype(BF16)
    k_load.wait()
    len_load.wait()
    scores = dot_nt(query, k_v[...]) * scale
    position = lax.broadcasted_iota(jnp.int32, scores.shape, 1)
    scores = jnp.where(position < jnp.broadcast_to(len_v[...], scores.shape), scores, -1e30)
    top = jnp.maximum(jnp.max(scores, axis=1, keepdims=True), own_score)
    weights = jnp.exp(scores - top)
    own_weight = jnp.exp(own_score - top)
    normalizer = jnp.sum(weights, axis=1, keepdims=True) + own_weight
    weights = (weights / normalizer).astype(BF16)
    own_weight = (own_weight / normalizer).astype(BF16).astype(F32)
    v_load.wait()
    mixed = dot(weights, v_v[...]) + own_weight * spread(value_v)
    att[pl.ds(me, 1)] = diagonal(mixed).astype(BF16)[None]

    pl.semaphore_wait(barrier, (2 + (1 - core)) * (RING - 1) + 1)
    tiles_1(att, att_sem)
    steps_1(hid, hid_sem)

    gain_load.wait()
    for h in range(HEADS):
        block = gain_v[h : h + 1, :].astype(F32)
        gain_b[h * HEAD_DIM : (h + 1) * HEAD_DIM, :] = jnp.broadcast_to(
            block, (HEAD_DIM, TOKENS)
        ).T
    rt_load.wait()
    nat_id = lax.broadcasted_iota(jnp.int32, (TOKENS, TOKENS), 0)
    lane = lax.broadcasted_iota(jnp.int32, (TOKENS, TOKENS), 1)
    lane_core, lane_second, lane_first = lane // HALF, (lane // RING) % RING, lane % RING
    lane_x = lane_first * (1 - lane_core) + lane_second * lane_core
    lane_y = lane_second * (1 - lane_core) + lane_first * lane_core
    to_slot = (nat_id == (lane_x * RING + lane_y) * 2 + lane_core).astype(BF16)
    routes = dot(
        jnp.broadcast_to(rt_v[...], (8, TOKENS)).astype(F32).astype(BF16), to_slot
    )[0:1].astype(jnp.int32)
    device = (x * RING + y) * 2 + core
    mine = device * ins[13].shape[1] // FF
    member = routes == mine
    rank = dot(
        jnp.broadcast_to(member.astype(F32), (8, TOKENS)).astype(BF16), (nat_id <= lane).astype(BF16)
    )[0:1].astype(jnp.int32) - 1
    slot_id = lax.broadcasted_iota(jnp.int32, (slots, TOKENS), 0)
    placed = jnp.where(
        jnp.broadcast_to(member, (slots, TOKENS))
        & (jnp.broadcast_to(rank, (slots, TOKENS)) == slot_id),
        1.0,
        0.0,
    )
    placed_at, depth = 2 * shared_units, lhs.shape[0]
    lhs[placed_at : placed_at + slots, :] = placed.astype(BF16)
    lhs[placed_at + slots :, :] = placed.astype(BF16)
    down_load.wait()
    send(
        rhs.at[pl.ds(0, shared_units)], rhs.at[pl.ds(shared_units, shared_units)], down_sem.at[0],
        down_sem.at[1], partner,
    )

    @pl.when(core == 0)
    def _():
        eup_load.wait()
        send(
            eup_v.at[:, pl.ds(kept, moved)], eup_v.at[:, pl.ds(units, moved)], units_sem.at[0],
            units_sem.at[1], partner,
        )
        edn_load.wait()
        send(
            edn_v.at[pl.ds(kept, moved)], edn_v.at[pl.ds(units, moved)], units_sem.at[2],
            units_sem.at[3], partner,
        )

    up_load.wait()
    send(
        up_t.at[pl.ds(0, shared_units)], up_t.at[pl.ds(shared_units, shared_units)], up_sem.at[0],
        up_sem.at[1], partner,
    )

    late_x = zero_last(x)
    tiles_2(
        att, att_sem,
        [(1, k) for k in zero_last(y)] + [(0, k) for k in late_x[:-1] + [OWN] + late_x[-1:]],
    )
    tiles_3(att, att_sem, 1)

    def projected(at):
        every = pl.ds(at * HEADS, HALF * HEADS)
        big[every, :] = att[pl.ds(at, HALF)].reshape(HALF * HEADS, HEAD_DIM).astype(F32)
        for h in range(HEADS):
            nat[:, h * HEAD_DIM : (h + 1) * HEAD_DIM] = big[
                pl.ds(at * HEADS + h, HALF, stride=HEADS), :
            ].astype(BF16)
        return dot_nt(wo_t[...], nat[...])

    wo_load.wait()
    half_1 = projected(HALF)
    tiles_3(att, att_sem, 0)
    steps_2(hid, hid_sem)
    half_0 = projected(0)
    pro[me] = jnp.concatenate([half_0, half_1], axis=1).astype(BF16)
    tiles_1(pro, pro_sem)
    tiles_2(pro, pro_sem, [(0, OWN)] + [(color, k) for k in NEAR_FIRST for color in (1, 0)])
    steps_3(hid, hid_sem)
    steps_4(hid, hid_sem)
    big[...] = hid[...].reshape(TOKENS * HEADS, HEAD_DIM).astype(F32)
    for h in range(HEADS):
        hid_t[h * HEAD_DIM : (h + 1) * HEAD_DIM, :] = big[pl.ds(h, TOKENS, stride=HEADS), :].T
    tiles_3(pro, pro_sem, 1)
    tiles_3(pro, pro_sem, 0)

    cols = wo_t.shape[0]
    total = jnp.zeros((cols, TOKENS), F32)
    for n in range(TOKENS):
        n_core, n_y, n_x = n % 2, (n // 2) % RING, n // (2 * RING)
        slot = n_core * HALF + (n_x * RING + n_y if n_core else n_y * RING + n_x)
        rows = slice(n * cols, (n + 1) * cols)
        block = pro[slot]
        proj_n[rows, :] = block
        block = hid_t[rows, :] + block.astype(F32)
        res[rows, :] = block
        total = total + block
    mean = jnp.sum(total, axis=0, keepdims=True) / d_model
    total = jnp.zeros((HEAD_DIM, TOKENS), F32)
    for h in range(HEADS):
        centered = res[h * HEAD_DIM : (h + 1) * HEAD_DIM, :] - mean
        total = total + centered * centered
    variance = jnp.sum(total, axis=0, keepdims=True) / d_model
    inverse = 1.0 / jnp.sqrt(jnp.maximum(variance, 0.25))
    for h in range(HEADS):
        rows = slice(h * HEAD_DIM, (h + 1) * HEAD_DIM)
        norm_t[rows, :] = ((res[rows, :] - mean) * inverse * gain_b[rows, :]).astype(BF16)

    normed = norm_t[...]
    picked = dot_nt(placed.astype(BF16), normed).astype(BF16)
    logits = dot(up_t[2 * shared_units :, :], normed)
    expert_row = lax.broadcasted_iota(jnp.int32, (experts, TOKENS), 0)
    chosen = jnp.sum(
        jnp.where(jnp.broadcast_to(routes, (experts, TOKENS)) == expert_row, logits, 0.0),
        axis=0,
        keepdims=True,
    )
    gate = 1.0 / (1.0 + jnp.exp(-chosen))
    slot_gate = jnp.sum(placed * gate, axis=1, keepdims=True)
    wide = d_model // PIECES
    theirs = placed_at + slots

    def expert(count):
        inner = jax.nn.gelu(dot(picked, eup_v[:, 0:count]), approximate=True).astype(BF16)
        for i in range(PIECES):
            at = i * wide
            result = dot(inner, edn_v[0:count, at : at + wide])
            rhs[placed_at:theirs, at : at + wide] = (result * slot_gate).astype(BF16)
            send(
                rhs.at[pl.ds(placed_at, slots), pl.ds(at, wide)],
                rhs.at[pl.ds(theirs, slots), pl.ds(at, wide)],
                slot_sem.at[0], slot_sem.at[1 + i], partner,
            )

    @pl.when(core == 0)
    def _():
        expert(kept)

    @pl.when(core == 1)
    def _():
        eup_load.wait()
        edn_load.wait()
        wait_for(eup_v.at[:, pl.ds(0, moved)], units_sem.at[1])
        wait_for(edn_v.at[pl.ds(0, moved)], units_sem.at[3])
        expert(units + moved)

    wait_for(rhs.at[pl.ds(0, shared_units)], down_sem.at[1])
    wait_for(up_t.at[pl.ds(0, shared_units)], up_sem.at[1])
    both = dot(up_t[0 : 2 * shared_units, :], normed)
    lhs[0 : 2 * shared_units, :] = jax.nn.gelu(both, approximate=True).astype(BF16)
    chosen_half = (
        lax.broadcasted_iota(jnp.int32, (HALF, TOKENS), 1)
        == lax.broadcasted_iota(jnp.int32, (HALF, TOKENS), 0) + core * HALF
    ).astype(BF16)
    left = dot_nt(chosen_half, lhs[...]).astype(BF16)
    for i in range(PIECES):
        columns = pl.ds(i * wide, wide)
        wait_for(rhs.at[pl.ds(theirs, slots), columns], slot_sem.at[1 + i])
        for at in range(i * wide, (i + 1) * wide, 256):
            piece = dot(left, rhs[:, at : at + 256]).astype(BF16)
            p_send[:, :, at : at + 256] = piece.reshape(RING, RING, 256)
        for k in FAR_FIRST:
            block = p_send.at[(second + k) % RING, :, columns]
            send(block, p_recv.at[k - 1, :, columns], p_sem.at[0], p_sem.at[1], on_second(k))
    summed = p_send[second].astype(F32)
    own_column = (
        lax.broadcasted_iota(jnp.int32, (HEADS, TOKENS), 1) == me
    ).astype(BF16)
    own = hid_tile + diagonal(dot_nt(own_column, proj_n[...]))
    wait_for(p_recv, p_sem.at[1])
    for k in range(RING - 1):
        summed = summed + p_recv[k].astype(F32)
    for h in range(HEADS):
        tok[pl.ds(h, RING, stride=HEADS), :] = summed[:, h * HEAD_DIM : (h + 1) * HEAD_DIM]
    for k in FAR_FIRST:
        to = pl.multiple_of(((first + k) % RING) * HEADS, HEADS)
        send(tok.at[pl.ds(to, HEADS)], t_recv.at[k - 1], t_sem.at[0], t_sem.at[1], on_first(k))
    own = own + tok[pl.ds(pl.multiple_of(first * HEADS, HEADS), HEADS), :]
    wait_for(t_recv, t_sem.at[1])
    for k in range(RING - 1):
        own = own + t_recv[k]
    for h in range(HEADS):
        out_ref[:, h * HEAD_DIM : (h + 1) * HEAD_DIM] = own[h : h + 1, :].astype(BF16)
    @pl.when(core == 0)
    def _():
        wait_for(eup_v.at[:, pl.ds(0, moved)], units_sem.at[0])
        wait_for(edn_v.at[pl.ds(0, moved)], units_sem.at[2])

    tiles_sent(att, att_sem)
    wait_for(hid.at[pl.ds(0, TOKENS - 1)], hid_sem.at[0])
    tiles_sent(pro, pro_sem)
    wait_for(rhs.at[pl.ds(0, shared_units)], down_sem.at[0])
    wait_for(up_t.at[pl.ds(0, shared_units)], up_sem.at[0])
    wait_for(rhs.at[pl.ds(placed_at, slots)], slot_sem.at[0])
    wait_for(p_recv, p_sem.at[0])
    wait_for(t_recv, t_sem.at[0])


def body(
    query, key_new, value_new, key_cache, value_cache, lengths, hidden, routes, w_out, ln_gain,
    router, shared_up, shared_down, expert_up, expert_down,
):
    key_cache = key_cache.reshape(key_cache.shape[1:])
    value_cache = value_cache.reshape(value_cache.shape[1:])
    lengths = lengths.reshape(1, 1)
    routes = routes.reshape(1, -1)
    ln_gain = ln_gain.reshape(-1, HEAD_DIM)
    w_out, router, shared_up = w_out.T, router.T, shared_up.T
    args = (
        query, key_new, value_new, key_cache, value_cache, lengths, hidden, routes, w_out, ln_gain,
        router, shared_up, shared_down, expert_up, expert_down,
    )
    d = query.shape[1]
    units = shared_up.shape[0]
    wide_units = 2 * expert_up.shape[1] - expert_up.shape[1] // KEPT
    slots = TOKENS * 4 // 32
    tile = (TOKENS, HEADS, HEAD_DIM)

    def own(a):
        return pltpu.VMEM(a.shape, a.dtype)

    dma = pltpu.SemaphoreType.DMA
    scratch = [
        pltpu.VMEM((4, 1, d), BF16),
        own(key_cache),
        own(value_cache),
        own(lengths),
        own(routes),
        own(w_out),
        own(ln_gain),
        pltpu.VMEM((2 * units + router.shape[0], d), BF16),
        pltpu.VMEM((2 * (units + slots), d), BF16),
        pltpu.VMEM((d, wide_units), BF16),
        pltpu.VMEM((wide_units, d), BF16),
        pltpu.VMEM(tile, BF16),
        pltpu.VMEM(tile, BF16),
        pltpu.VMEM((TOKENS, w_out.shape[0], TOKENS), BF16),
        pltpu.VMEM((TOKENS * HEADS, HEAD_DIM), F32),
        pltpu.VMEM((d, TOKENS), F32),
        pltpu.VMEM((d, TOKENS), F32),
        pltpu.VMEM((HALF, d), BF16),
        pltpu.VMEM((d, TOKENS), F32),
        pltpu.VMEM((d, TOKENS), BF16),
        pltpu.VMEM((d, TOKENS), BF16),
        pltpu.VMEM((RING, RING, d), BF16),
        pltpu.VMEM((RING - 1, RING, d), BF16),
        pltpu.VMEM((RING * HEADS, HEAD_DIM), F32),
        pltpu.VMEM((RING - 1, HEADS, HEAD_DIM), F32),
        pltpu.VMEM((2 * (units + slots), TOKENS), BF16),
    ]
    scratch += [dma((n,)) for n in (11, 27, 4, 27, 2, 2, 1 + PIECES, 2, 2, 4)]
    return pl.pallas_call(
        kernel,
        out_shape=jax.ShapeDtypeStruct((1, d), BF16),
        in_specs=[pl.BlockSpec(memory_space=pl.ANY)] * 15,
        out_specs=pl.BlockSpec(memory_space=pltpu.VMEM),
        scratch_shapes=scratch,
        compiler_params=pltpu.CompilerParams(collective_id=0, has_side_effects=True),
        name="decode_layer",
    )(*args)


def solution(mesh):
    torus = Mesh(
        mesh.devices.reshape(mesh.shape["group"], RING, RING, 2),
        ("group", "expert_0", "expert_1", "expert_2"),
    )
    placed = (
        P(GROUP_EXPERT, None),
        P(GROUP_EXPERT, None),
        P(GROUP_EXPERT, None),
        P(GROUP_EXPERT, None, None),
        P(GROUP_EXPERT, None, None),
        P(GROUP_EXPERT),
        P(GROUP_EXPERT, None),
        P("group"),
        P(None, EXPERT),
        P(),
        P(),
        P(None, EXPERT),
        P(EXPERT, None),
        P(None, EXPERT),
        P(EXPERT, None),
    )
    return jax.shard_map(
        body, mesh=torus, in_specs=placed, out_specs=P(GROUP_EXPERT, None), check_vma=False
    )
```

```python
import functools
import math

import jax
import jax.numpy as jnp
from jax import lax
from jax.experimental import pallas as pl
from jax.experimental.pallas import tpu as pltpu
from jax.sharding import Mesh
from jax.sharding import PartitionSpec as P

HEADS = 16
HEAD_DIM = 128
FF = 4096
RING = 8
TOKENS = 2 * RING * RING
HALF = RING * RING
EXPERT = ("expert_0", "expert_1", "expert_2")
GROUP_EXPERT = ("group", "expert_0", "expert_1", "expert_2")
MESH = pl.DeviceIdType.MESH
PIECES = 2
KEPT = 2
F32 = jnp.float32
BF16 = jnp.bfloat16
OWN = 0
PAIRS = ((1, 7), (2, 6), (3, 5), (4,))
FAR_FIRST = (4, 3, 5, 2, 6, 1, 7)
NEAR_FIRST = (1, 7, 2, 6, 3, 5, 4)


def dot(a, b):
    return jnp.dot(a, b, preferred_element_type=F32)


def dot_nt(a, b):
    return lax.dot_general(a, b, (((1,), (1,)), ((), ())), preferred_element_type=F32)


def eye(n):
    return (
        lax.broadcasted_iota(jnp.int32, (n, n), 0) == lax.broadcasted_iota(jnp.int32, (n, n), 1)
    ).astype(BF16)


def diagonal(x):
    row = lax.broadcasted_iota(jnp.int32, (HEADS, HEAD_DIM), 0)
    out = jnp.zeros((HEADS, HEAD_DIM), F32)
    for h in range(HEADS):
        out = jnp.where(row == h, x[:, h * HEAD_DIM : (h + 1) * HEAD_DIM], out)
    return out


def kernel(*refs):
    ins, out_ref, vm, sems = refs[:15], refs[15], refs[16:-10], refs[-10:]
    (
        rows_v, k_v, v_v, len_v, rt_v, wo_t, gain_v, up_t, rhs, eup_v, edn_v, att, hid, pro, big,
        hid_t, gain_b, nat, res, proj_n, norm_t, p_send, p_recv, tok, t_recv, lhs,
    ) = vm
    load_sem, att_sem, hid_sem, pro_sem, down_sem, up_sem, slot_sem, p_sem, t_sem, units_sem = sems
    d_model = rows_v.shape[2]
    experts, shared_units = ins[10].shape[0], ins[11].shape[0]
    slots = TOKENS * 4 // 32

    x = lax.axis_index("expert_0")
    y = lax.axis_index("expert_1")
    core = lax.axis_index("expert_2")
    first = x * (1 - core) + y * core
    second = y * (1 - core) + x * core
    me = core * HALF + second * RING + first

    def on_first(k):
        return {
            "expert_0": (x + k * (1 - core)) % RING,
            "expert_1": (y + k * core) % RING,
            "expert_2": core,
        }

    def on_second(k):
        return {
            "expert_0": (x + k * core) % RING,
            "expert_1": (y + k * (1 - core)) % RING,
            "expert_2": core,
        }

    def along(axis, k, to):
        return {
            "expert_0": (x + k * (1 - axis)) % RING,
            "expert_1": (y + k * axis) % RING,
            "expert_2": to,
        }

    partner = {"expert_0": x, "expert_1": y, "expert_2": 1 - core}

    barrier = pltpu.get_barrier_semaphore()
    for k in FAR_FIRST:
        pl.semaphore_signal(barrier, inc=1, device_id=on_first(k), device_id_type=MESH)
        pl.semaphore_signal(barrier, inc=1, device_id=on_second(k), device_id_type=MESH)
    pl.semaphore_signal(barrier, inc=1, device_id=partner, device_id_type=MESH)

    @pl.when(core == 1)
    def _():
        for k in FAR_FIRST:
            pl.semaphore_signal(barrier, inc=1, device_id=along(0, k, 0), device_id_type=MESH)


    query_v, key_v, value_v, hid_v = (rows_v.at[i] for i in range(4))

    def load(i, target, sem):
        copy = pltpu.make_async_copy(ins[i], target, load_sem.at[sem])
        copy.start()
        return copy

    for i, row in ((0, query_v), (1, key_v), (2, value_v), (6, hid_v)):
        load(i, row, 0)
    rows_load = pltpu.make_async_copy(rows_v, rows_v, load_sem.at[0])
    k_load = load(3, k_v, 1)
    len_load = load(5, len_v, 2)
    v_load = load(4, v_v, 3)
    gain_load = load(9, gain_v, 4)
    rt_load = load(7, rt_v, 5)
    down_load = load(12, rhs.at[pl.ds(0, shared_units)], 6)
    wo_load = load(8, wo_t, 7)
    load(11, up_t.at[pl.ds(0, shared_units)], 8)
    load(10, up_t.at[pl.ds(2 * shared_units, experts)], 8)
    up_load = pltpu.make_async_copy(
        up_t.at[pl.ds(0, shared_units + experts)], up_t.at[pl.ds(0, shared_units + experts)],
        load_sem.at[8],
    )
    units = ins[13].shape[1]
    kept = units // KEPT
    moved = units - kept
    eup_load = load(13, eup_v.at[:, pl.ds(0, units)], 9)
    edn_load = load(14, edn_v.at[pl.ds(0, units)], 10)

    def send(src, dst, send_sem, recv_sem, to):
        copy = pltpu.make_async_remote_copy(
            src_ref=src, dst_ref=dst, send_sem=send_sem, recv_sem=recv_sem, device_id=to,
            device_id_type=MESH,
        )
        copy.start()

    def wait_for(ref, sem):
        pltpu.make_async_copy(ref, ref, sem).wait()

    def row_of(second_k):
        return pl.ds(core * HALF + ((second - second_k + RING) % RING) * RING, RING)

    place = ((x, y), (y, x))

    def tile_at(buf, color, k):
        at, row = place[color]
        return buf.at[pl.ds(color * HALF + row * RING + (at - k + RING) % RING, 1)]

    def row_at(buf, color, j):
        return buf.at[
            pl.ds(color * HALF + ((place[color][1] - j + RING) % RING) * RING, RING)
        ]

    def pass_on(buf, sem, color, k):
        tile = tile_at(buf, color, k)
        for j in FAR_FIRST:
            pair = 19 + 4 * color + min(j, RING - j) - 1
            send(tile, tile, sem.at[1 - color], sem.at[pair], along(1 - color, j, 1))

    def tiles_1(buf, sem):
        tile = buf.at[pl.ds(me, 1)]

        @pl.when(core == 0)
        def _():
            for k in FAR_FIRST:
                send(tile, tile, sem.at[0], sem.at[4 + k], along(0, k, 1))
            send(tile, tile, sem.at[0], sem.at[4], partner)

        @pl.when(core == 1)
        def _():
            for k in FAR_FIRST:
                send(tile, tile, sem.at[0], sem.at[11 + k], along(1, k, 1))
            pass_on(buf, sem, 1, 0)

    def zero_last(at):
        last = NEAR_FIRST[-1]
        order = [
            k + (last - k) * (1 - ((k - at + RING) % RING + RING - 1) // RING)
            for k in NEAR_FIRST[:-1]
        ]
        return order + [at + last * (1 - (at + RING - 1) // RING)]

    def tiles_2(buf, sem, order):
        @pl.when(core == 1)
        def _():
            rows_left = RING - 1
            for color, k in order:
                tile = tile_at(buf, color, k)
                wait_for(tile, sem.at[(4, 11)[color] + k])
                pass_on(buf, sem, color, k)
                if color:
                    rows_left -= 1
                    if not rows_left:
                        row = row_at(buf, 1, 0)
                        send(row, row, sem.at[0], sem.at[2], partner)
                elif k is not OWN:
                    send(tile, tile, sem.at[1], sem.at[3], partner)

    def tiles_3(buf, sem, color):
        @pl.when(core == 1)
        def _():
            for i, pair in enumerate(PAIRS):
                wait_for(buf.at[pl.ds(0, RING * len(pair))], sem.at[19 + 4 * color + i])
                for j in pair:
                    row = row_at(buf, color, j)
                    send(row, row, sem.at[1 - color], sem.at[3 - color], partner)

        @pl.when(core == 0)
        def _():
            wait_for(buf.at[pl.ds(0, HALF - 1 + color)], sem.at[3 - color])

    def tiles_sent(buf, sem):
        @pl.when(core == 1)
        def _():
            wait_for(buf.at[pl.ds(0, 2 * HALF - 1)], sem.at[0])
            wait_for(buf.at[pl.ds(0, 2 * HALF - RING - 1)], sem.at[1])

        @pl.when(core == 0)
        def _():
            wait_for(buf.at[pl.ds(0, RING)], sem.at[0])

    def steps_1(buf, sem):
        tile = buf.at[pl.ds(me, 1)]
        for k in FAR_FIRST:
            send(tile, tile, sem.at[0], sem.at[1], on_first(k))

    def steps_2(buf, sem):
        wait_for(buf.at[pl.ds(0, RING - 1)], sem.at[1])
        row = buf.at[row_of(0)]
        for k in FAR_FIRST:
            send(row, row, sem.at[0], sem.at[2], on_second(k))

    def steps_3(buf, sem):
        wait_for(buf.at[pl.ds(0, HALF - RING)], sem.at[2])
        half = buf.at[pl.ds(core * HALF, HALF)]
        send(half, half, sem.at[0], sem.at[3], partner)

    def steps_4(buf, sem):
        wait_for(buf.at[pl.ds((1 - core) * HALF, HALF)], sem.at[3])

    rows_load.wait()
    head_row = lax.broadcasted_iota(jnp.int32, (HEADS, d_model), 0)
    head_of_lane = lax.broadcasted_iota(jnp.int32, (HEADS, d_model), 1) // HEAD_DIM
    own_head = head_row == head_of_lane
    scale = 1.0 / math.sqrt(HEAD_DIM)

    def spread(ref):
        return jnp.broadcast_to(ref[...].astype(F32), (HEADS, d_model))

    hid_tile = diagonal(spread(hid_v))
    hid[pl.ds(me, 1)] = hid_tile.astype(BF16)[None]
    query = jnp.where(own_head, spread(query_v), 0.0)
    own_score = jnp.sum(query * spread(key_v), axis=1, keepdims=True) * scale
    query = query.astype(BF16)
    k_load.wait()
    len_load.wait()
    scores = dot_nt(query, k_v[...]) * scale
    position = lax.broadcasted_iota(jnp.int32, scores.shape, 1)
    scores = jnp.where(position < jnp.broadcast_to(len_v[...], scores.shape), scores, -1e30)
    top = jnp.maximum(jnp.max(scores, axis=1, keepdims=True), own_score)
    weights = jnp.exp(scores - top)
    own_weight = jnp.exp(own_score - top)
    normalizer = jnp.sum(weights, axis=1, keepdims=True) + own_weight
    weights = (weights / normalizer).astype(BF16)
    own_weight = (own_weight / normalizer).astype(BF16).astype(F32)
    v_load.wait()
    mixed = dot(weights, v_v[...]) + own_weight * spread(value_v)
    att[pl.ds(me, 1)] = diagonal(mixed).astype(BF16)[None]

    pl.semaphore_wait(barrier, (2 + (1 - core)) * (RING - 1) + 1)
    tiles_1(att, att_sem)
    steps_1(hid, hid_sem)

    gain_load.wait()
    for h in range(HEADS):
        block = gain_v[h : h + 1, :].astype(F32)
        gain_b[h * HEAD_DIM : (h + 1) * HEAD_DIM, :] = jnp.broadcast_to(
            block, (HEAD_DIM, TOKENS)
        ).T
    rt_load.wait()
    nat_id = lax.broadcasted_iota(jnp.int32, (TOKENS, TOKENS), 0)
    lane = lax.broadcasted_iota(jnp.int32, (TOKENS, TOKENS), 1)
    lane_core, lane_second, lane_first = lane // HALF, (lane // RING) % RING, lane % RING
    lane_x = lane_first * (1 - lane_core) + lane_second * lane_core
    lane_y = lane_second * (1 - lane_core) + lane_first * lane_core
    to_slot = (nat_id == (lane_x * RING + lane_y) * 2 + lane_core).astype(BF16)
    routes = dot(
        jnp.broadcast_to(rt_v[...], (8, TOKENS)).astype(F32).astype(BF16), to_slot
    )[0:1].astype(jnp.int32)
    device = (x * RING + y) * 2 + core
    mine = device * ins[13].shape[1] // FF
    member = routes == mine
    rank = dot(
        jnp.broadcast_to(member.astype(F32), (8, TOKENS)).astype(BF16), (nat_id <= lane).astype(BF16)
    )[0:1].astype(jnp.int32) - 1
    slot_id = lax.broadcasted_iota(jnp.int32, (slots, TOKENS), 0)
    placed = jnp.where(
        jnp.broadcast_to(member, (slots, TOKENS))
        & (jnp.broadcast_to(rank, (slots, TOKENS)) == slot_id),
        1.0,
        0.0,
    )
    placed_at, depth = 2 * shared_units, lhs.shape[0]
    lhs[placed_at : placed_at + slots, :] = placed.astype(BF16)
    lhs[placed_at + slots :, :] = placed.astype(BF16)
    down_load.wait()
    send(
        rhs.at[pl.ds(0, shared_units)], rhs.at[pl.ds(shared_units, shared_units)], down_sem.at[0],
        down_sem.at[1], partner,
    )

    @pl.when(core == 0)
    def _():
        eup_load.wait()
        send(
            eup_v.at[:, pl.ds(kept, moved)], eup_v.at[:, pl.ds(units, moved)], units_sem.at[0],
            units_sem.at[1], partner,
        )
        edn_load.wait()
        send(
            edn_v.at[pl.ds(kept, moved)], edn_v.at[pl.ds(units, moved)], units_sem.at[2],
            units_sem.at[3], partner,
        )

    up_load.wait()
    send(
        up_t.at[pl.ds(0, shared_units)], up_t.at[pl.ds(shared_units, shared_units)], up_sem.at[0],
        up_sem.at[1], partner,
    )

    late_x = zero_last(x)
    tiles_2(
        att, att_sem,
        [(1, k) for k in zero_last(y)] + [(0, k) for k in late_x[:-1] + [OWN] + late_x[-1:]],
    )
    tiles_3(att, att_sem, 1)

    def projected(at):
        every = pl.ds(at * HEADS, HALF * HEADS)
        big[every, :] = att[pl.ds(at, HALF)].reshape(HALF * HEADS, HEAD_DIM).astype(F32)
        for h in range(HEADS):
            nat[:, h * HEAD_DIM : (h + 1) * HEAD_DIM] = big[
                pl.ds(at * HEADS + h, HALF, stride=HEADS), :
            ].astype(BF16)
        return dot_nt(wo_t[...], nat[...])

    wo_load.wait()
    half_1 = projected(HALF)
    tiles_3(att, att_sem, 0)
    steps_2(hid, hid_sem)
    half_0 = projected(0)
    pro[me] = jnp.concatenate([half_0, half_1], axis=1).astype(BF16)
    tiles_1(pro, pro_sem)
    tiles_2(pro, pro_sem, [(0, OWN)] + [(color, k) for k in NEAR_FIRST for color in (1, 0)])
    steps_3(hid, hid_sem)
    steps_4(hid, hid_sem)
    big[...] = hid[...].reshape(TOKENS * HEADS, HEAD_DIM).astype(F32)
    for h in range(HEADS):
        hid_t[h * HEAD_DIM : (h + 1) * HEAD_DIM, :] = big[pl.ds(h, TOKENS, stride=HEADS), :].T
    tiles_3(pro, pro_sem, 1)
    tiles_3(pro, pro_sem, 0)

    cols = wo_t.shape[0]
    total = jnp.zeros((cols, TOKENS), F32)
    for n in range(TOKENS):
        n_core, n_y, n_x = n % 2, (n // 2) % RING, n // (2 * RING)
        slot = n_core * HALF + (n_x * RING + n_y if n_core else n_y * RING + n_x)
        rows = slice(n * cols, (n + 1) * cols)
        block = pro[slot]
        proj_n[rows, :] = block
        block = hid_t[rows, :] + block.astype(F32)
        res[rows, :] = block
        total = total + block
    mean = jnp.sum(total, axis=0, keepdims=True) / d_model
    total = jnp.zeros((HEAD_DIM, TOKENS), F32)
    for h in range(HEADS):
        centered = res[h * HEAD_DIM : (h + 1) * HEAD_DIM, :] - mean
        total = total + centered * centered
    variance = jnp.sum(total, axis=0, keepdims=True) / d_model
    inverse = 1.0 / jnp.sqrt(jnp.maximum(variance, 0.25))
    for h in range(HEADS):
        rows = slice(h * HEAD_DIM, (h + 1) * HEAD_DIM)
        norm_t[rows, :] = ((res[rows, :] - mean) * inverse * gain_b[rows, :]).astype(BF16)

    normed = norm_t[...]
    picked = dot_nt(placed.astype(BF16), normed).astype(BF16)
    logits = dot(up_t[2 * shared_units :, :], normed)
    expert_row = lax.broadcasted_iota(jnp.int32, (experts, TOKENS), 0)
    chosen = jnp.sum(
        jnp.where(jnp.broadcast_to(routes, (experts, TOKENS)) == expert_row, logits, 0.0),
        axis=0,
        keepdims=True,
    )
    gate = 1.0 / (1.0 + jnp.exp(-chosen))
    slot_gate = jnp.sum(placed * gate, axis=1, keepdims=True)
    wide = d_model // PIECES
    theirs = placed_at + slots

    def expert(count):
        inner = jax.nn.gelu(dot(picked, eup_v[:, 0:count]), approximate=True).astype(BF16)
        for i in range(PIECES):
            at = i * wide
            result = dot(inner, edn_v[0:count, at : at + wide])
            rhs[placed_at:theirs, at : at + wide] = (result * slot_gate).astype(BF16)
            send(
                rhs.at[pl.ds(placed_at, slots), pl.ds(at, wide)],
                rhs.at[pl.ds(theirs, slots), pl.ds(at, wide)],
                slot_sem.at[0], slot_sem.at[1 + i], partner,
            )

    @pl.when(core == 0)
    def _():
        expert(kept)

    @pl.when(core == 1)
    def _():
        eup_load.wait()
        edn_load.wait()
        wait_for(eup_v.at[:, pl.ds(0, moved)], units_sem.at[1])
        wait_for(edn_v.at[pl.ds(0, moved)], units_sem.at[3])
        expert(units + moved)

    wait_for(rhs.at[pl.ds(0, shared_units)], down_sem.at[1])
    wait_for(up_t.at[pl.ds(0, shared_units)], up_sem.at[1])
    both = dot(up_t[0 : 2 * shared_units, :], normed)
    lhs[0 : 2 * shared_units, :] = jax.nn.gelu(both, approximate=True).astype(BF16)
    chosen_half = (
        lax.broadcasted_iota(jnp.int32, (HALF, TOKENS), 1)
        == lax.broadcasted_iota(jnp.int32, (HALF, TOKENS), 0) + core * HALF
    ).astype(BF16)
    left = dot_nt(chosen_half, lhs[...]).astype(BF16)
    for i in range(PIECES):
        columns = pl.ds(i * wide, wide)
        wait_for(rhs.at[pl.ds(theirs, slots), columns], slot_sem.at[1 + i])
        for at in range(i * wide, (i + 1) * wide, 256):
            piece = dot(left, rhs[:, at : at + 256]).astype(BF16)
            p_send[:, :, at : at + 256] = piece.reshape(RING, RING, 256)
        for k in FAR_FIRST:
            block = p_send.at[(second + k) % RING, :, columns]
            send(block, p_recv.at[k - 1, :, columns], p_sem.at[0], p_sem.at[1], on_second(k))
    summed = p_send[second].astype(F32)
    own_column = (
        lax.broadcasted_iota(jnp.int32, (HEADS, TOKENS), 1) == me
    ).astype(BF16)
    own = hid_tile + diagonal(dot_nt(own_column, proj_n[...]))
    wait_for(p_recv, p_sem.at[1])
    for k in range(RING - 1):
        summed = summed + p_recv[k].astype(F32)
    for h in range(HEADS):
        tok[pl.ds(h, RING, stride=HEADS), :] = summed[:, h * HEAD_DIM : (h + 1) * HEAD_DIM]
    for k in FAR_FIRST:
        to = pl.multiple_of(((first + k) % RING) * HEADS, HEADS)
        send(tok.at[pl.ds(to, HEADS)], t_recv.at[k - 1], t_sem.at[0], t_sem.at[1], on_first(k))
    own = own + tok[pl.ds(pl.multiple_of(first * HEADS, HEADS), HEADS), :]
    wait_for(t_recv, t_sem.at[1])
    for k in range(RING - 1):
        own = own + t_recv[k]
    for h in range(HEADS):
        out_ref[:, h * HEAD_DIM : (h + 1) * HEAD_DIM] = own[h : h + 1, :].astype(BF16)
    @pl.when(core == 0)
    def _():
        wait_for(eup_v.at[:, pl.ds(0, moved)], units_sem.at[0])
        wait_for(edn_v.at[pl.ds(0, moved)], units_sem.at[2])

    tiles_sent(att, att_sem)
    wait_for(hid.at[pl.ds(0, TOKENS - 1)], hid_sem.at[0])
    tiles_sent(pro, pro_sem)
    wait_for(rhs.at[pl.ds(0, shared_units)], down_sem.at[0])
    wait_for(up_t.at[pl.ds(0, shared_units)], up_sem.at[0])
    wait_for(rhs.at[pl.ds(placed_at, slots)], slot_sem.at[0])
    wait_for(p_recv, p_sem.at[0])
    wait_for(t_recv, t_sem.at[0])


def body(
    query, key_new, value_new, key_cache, value_cache, lengths, hidden, routes, w_out, ln_gain,
    router, shared_up, shared_down, expert_up, expert_down,
):
    key_cache = key_cache.reshape(key_cache.shape[1:])
    value_cache = value_cache.reshape(value_cache.shape[1:])
    lengths = lengths.reshape(1, 1)
    routes = routes.reshape(1, -1)
    ln_gain = ln_gain.reshape(-1, HEAD_DIM)
    w_out, router, shared_up = w_out.T, router.T, shared_up.T
    args = (
        query, key_new, value_new, key_cache, value_cache, lengths, hidden, routes, w_out, ln_gain,
        router, shared_up, shared_down, expert_up, expert_down,
    )
    d = query.shape[1]
    units = shared_up.shape[0]
    wide_units = 2 * expert_up.shape[1] - expert_up.shape[1] // KEPT
    slots = TOKENS * 4 // 32
    tile = (TOKENS, HEADS, HEAD_DIM)

    def own(a):
        return pltpu.VMEM(a.shape, a.dtype)

    dma = pltpu.SemaphoreType.DMA
    scratch = [
        pltpu.VMEM((4, 1, d), BF16),
        own(key_cache),
        own(value_cache),
        own(lengths),
        own(routes),
        own(w_out),
        own(ln_gain),
        pltpu.VMEM((2 * units + router.shape[0], d), BF16),
        pltpu.VMEM((2 * (units + slots), d), BF16),
        pltpu.VMEM((d, wide_units), BF16),
        pltpu.VMEM((wide_units, d), BF16),
        pltpu.VMEM(tile, BF16),
        pltpu.VMEM(tile, BF16),
        pltpu.VMEM((TOKENS, w_out.shape[0], TOKENS), BF16),
        pltpu.VMEM((TOKENS * HEADS, HEAD_DIM), F32),
        pltpu.VMEM((d, TOKENS), F32),
        pltpu.VMEM((d, TOKENS), F32),
        pltpu.VMEM((HALF, d), BF16),
        pltpu.VMEM((d, TOKENS), F32),
        pltpu.VMEM((d, TOKENS), BF16),
        pltpu.VMEM((d, TOKENS), BF16),
        pltpu.VMEM((RING, RING, d), BF16),
        pltpu.VMEM((RING - 1, RING, d), BF16),
        pltpu.VMEM((RING * HEADS, HEAD_DIM), F32),
        pltpu.VMEM((RING - 1, HEADS, HEAD_DIM), F32),
        pltpu.VMEM((2 * (units + slots), TOKENS), BF16),
    ]
    scratch += [dma((n,)) for n in (11, 27, 4, 27, 2, 2, 1 + PIECES, 2, 2, 4)]
    return pl.pallas_call(
        kernel,
        out_shape=pltpu.VMEM((1, d), BF16),
        in_specs=[pl.BlockSpec(memory_space=pl.ANY)] * 15,
        out_specs=pl.BlockSpec(memory_space=pltpu.VMEM),
        scratch_shapes=scratch,
        compiler_params=pltpu.CompilerParams(collective_id=0, has_side_effects=True),
        name="decode_layer",
    )(*args)


def solution(mesh):
    torus = Mesh(
        mesh.devices.reshape(mesh.shape["group"], RING, RING, 2),
        ("group", "expert_0", "expert_1", "expert_2"),
    )
    placed = (
        P(GROUP_EXPERT, None),
        P(GROUP_EXPERT, None),
        P(GROUP_EXPERT, None),
        P(GROUP_EXPERT, None, None),
        P(GROUP_EXPERT, None, None),
        P(GROUP_EXPERT),
        P(GROUP_EXPERT, None),
        P("group"),
        P(None, EXPERT),
        P(),
        P(),
        P(None, EXPERT),
        P(EXPERT, None),
        P(None, EXPERT),
        P(EXPERT, None),
    )
    return jax.shard_map(
        body, mesh=torus, in_specs=placed, out_specs=P(GROUP_EXPERT, None), check_vma=False
    )
```

```python
import functools
import math

import jax
import jax.numpy as jnp
from jax import lax
from jax.experimental import pallas as pl
from jax.experimental.pallas import tpu as pltpu
from jax.sharding import Mesh
from jax.sharding import PartitionSpec as P

HEADS = 16
HEAD_DIM = 128
FF = 4096
RING = 8
TOKENS = 2 * RING * RING
HALF = RING * RING
EXPERT = ("expert_0", "expert_1", "expert_2")
GROUP_EXPERT = ("group", "expert_0", "expert_1", "expert_2")
MESH = pl.DeviceIdType.MESH
PIECES = 2
KEPT = 2
F32 = jnp.float32
BF16 = jnp.bfloat16
OWN = 0
PAIRS = ((1, 7), (2, 6), (3, 5), (4,))
FAR_FIRST = (4, 3, 5, 2, 6, 1, 7)
NEAR_FIRST = (1, 7, 2, 6, 3, 5, 4)


def dot(a, b):
    return jnp.dot(a, b, preferred_element_type=F32)


def dot_nt(a, b):
    return lax.dot_general(a, b, (((1,), (1,)), ((), ())), preferred_element_type=F32)


def eye(n):
    return (
        lax.broadcasted_iota(jnp.int32, (n, n), 0) == lax.broadcasted_iota(jnp.int32, (n, n), 1)
    ).astype(BF16)


def diagonal(x):
    row = lax.broadcasted_iota(jnp.int32, (HEADS, HEAD_DIM), 0)
    out = jnp.zeros((HEADS, HEAD_DIM), F32)
    for h in range(HEADS):
        out = jnp.where(row == h, x[:, h * HEAD_DIM : (h + 1) * HEAD_DIM], out)
    return out


def kernel(*refs):
    ins, out_ref, vm, sems = refs[:15], refs[15], refs[16:-10], refs[-10:]
    (
        rows_v, k_v, v_v, len_v, rt_v, wo_t, gain_v, up_t, rhs, eup_v, edn_v, att, hid, pro, big,
        hid_t, gain_b, nat, res, proj_n, norm_t, p_send, p_recv, tok, t_recv, lhs,
    ) = vm
    load_sem, att_sem, hid_sem, pro_sem, down_sem, up_sem, slot_sem, p_sem, t_sem, units_sem = sems
    d_model = rows_v.shape[2]
    experts, shared_units = ins[10].shape[0], ins[11].shape[0]
    slots = TOKENS * 4 // 32

    x = lax.axis_index("expert_0")
    y = lax.axis_index("expert_1")
    core = lax.axis_index("expert_2")
    first = x * (1 - core) + y * core
    second = y * (1 - core) + x * core
    me = core * HALF + second * RING + first

    def on_first(k):
        return {
            "expert_0": (x + k * (1 - core)) % RING,
            "expert_1": (y + k * core) % RING,
            "expert_2": core,
        }

    def on_second(k):
        return {
            "expert_0": (x + k * core) % RING,
            "expert_1": (y + k * (1 - core)) % RING,
            "expert_2": core,
        }

    def along(axis, k, to):
        return {
            "expert_0": (x + k * (1 - axis)) % RING,
            "expert_1": (y + k * axis) % RING,
            "expert_2": to,
        }

    partner = {"expert_0": x, "expert_1": y, "expert_2": 1 - core}

    barrier = pltpu.get_barrier_semaphore()
    for k in FAR_FIRST:
        pl.semaphore_signal(barrier, inc=1, device_id=on_first(k), device_id_type=MESH)
        pl.semaphore_signal(barrier, inc=1, device_id=on_second(k), device_id_type=MESH)
    pl.semaphore_signal(barrier, inc=1, device_id=partner, device_id_type=MESH)

    @pl.when(core == 1)
    def _():
        for k in FAR_FIRST:
            pl.semaphore_signal(barrier, inc=1, device_id=along(0, k, 0), device_id_type=MESH)


    query_v, key_v, value_v, hid_v = (rows_v.at[i] for i in range(4))

    def load(i, target, sem):
        copy = pltpu.make_async_copy(ins[i], target, load_sem.at[sem])
        copy.start()
        return copy

    for i, row in ((0, query_v), (1, key_v), (2, value_v), (6, hid_v)):
        load(i, row, 0)
    rows_load = pltpu.make_async_copy(rows_v, rows_v, load_sem.at[0])
    k_load = load(3, k_v, 1)
    len_load = load(5, len_v, 2)
    v_load = load(4, v_v, 3)
    gain_load = load(9, gain_v, 4)
    rt_load = load(7, rt_v, 5)
    down_load = load(12, rhs.at[pl.ds(0, shared_units)], 6)
    wo_load = load(8, wo_t, 7)
    load(11, up_t.at[pl.ds(0, shared_units)], 8)
    load(10, up_t.at[pl.ds(2 * shared_units, experts)], 8)
    up_load = pltpu.make_async_copy(
        up_t.at[pl.ds(0, shared_units + experts)], up_t.at[pl.ds(0, shared_units + experts)],
        load_sem.at[8],
    )
    units = ins[13].shape[1]
    kept = units // KEPT
    moved = units - kept
    eup_load = load(13, eup_v.at[:, pl.ds(0, units)], 9)
    edn_load = load(14, edn_v.at[pl.ds(0, units)], 10)

    def send(src, dst, send_sem, recv_sem, to):
        copy = pltpu.make_async_remote_copy(
            src_ref=src, dst_ref=dst, send_sem=send_sem, recv_sem=recv_sem, device_id=to,
            device_id_type=MESH,
        )
        copy.start()

    def wait_for(ref, sem):
        pltpu.make_async_copy(ref, ref, sem).wait()

    def row_of(second_k):
        return pl.ds(core * HALF + ((second - second_k + RING) % RING) * RING, RING)

    place = ((x, y), (y, x))

    def tile_at(buf, color, k):
        at, row = place[color]
        return buf.at[pl.ds(color * HALF + row * RING + (at - k + RING) % RING, 1)]

    def row_at(buf, color, j):
        return buf.at[
            pl.ds(color * HALF + ((place[color][1] - j + RING) % RING) * RING, RING)
        ]

    def pass_on(buf, sem, color, k):
        tile = tile_at(buf, color, k)
        for j in FAR_FIRST:
            pair = 19 + 4 * color + min(j, RING - j) - 1
            send(tile, tile, sem.at[1 - color], sem.at[pair], along(1 - color, j, 1))

    def tiles_1(buf, sem):
        tile = buf.at[pl.ds(me, 1)]

        @pl.when(core == 0)
        def _():
            for k in FAR_FIRST:
                send(tile, tile, sem.at[0], sem.at[4 + k], along(0, k, 1))
            send(tile, tile, sem.at[0], sem.at[4], partner)

        @pl.when(core == 1)
        def _():
            for k in FAR_FIRST:
                send(tile, tile, sem.at[0], sem.at[11 + k], along(1, k, 1))
            pass_on(buf, sem, 1, 0)

    def zero_last(at):
        last = NEAR_FIRST[-1]
        order = [
            k + (last - k) * (1 - ((k - at + RING) % RING + RING - 1) // RING)
            for k in NEAR_FIRST[:-1]
        ]
        return order + [at + last * (1 - (at + RING - 1) // RING)]

    def tiles_2(buf, sem, order):
        @pl.when(core == 1)
        def _():
            rows_left = RING - 1
            for color, k in order:
                tile = tile_at(buf, color, k)
                wait_for(tile, sem.at[(4, 11)[color] + k])
                pass_on(buf, sem, color, k)
                if color:
                    rows_left -= 1
                    if not rows_left:
                        row = row_at(buf, 1, 0)
                        send(row, row, sem.at[0], sem.at[2], partner)
                elif k is not OWN:
                    send(tile, tile, sem.at[1], sem.at[3], partner)

    def tiles_3(buf, sem, color):
        @pl.when(core == 1)
        def _():
            for i, pair in enumerate(PAIRS):
                wait_for(buf.at[pl.ds(0, RING * len(pair))], sem.at[19 + 4 * color + i])
                for j in pair:
                    row = row_at(buf, color, j)
                    send(row, row, sem.at[1 - color], sem.at[3 - color], partner)

        @pl.when(core == 0)
        def _():
            wait_for(buf.at[pl.ds(0, HALF - 1 + color)], sem.at[3 - color])

    def tiles_sent(buf, sem):
        @pl.when(core == 1)
        def _():
            wait_for(buf.at[pl.ds(0, 2 * HALF - 1)], sem.at[0])
            wait_for(buf.at[pl.ds(0, 2 * HALF - RING - 1)], sem.at[1])

        @pl.when(core == 0)
        def _():
            wait_for(buf.at[pl.ds(0, RING)], sem.at[0])

    def steps_1(buf, sem):
        tile = buf.at[pl.ds(me, 1)]
        for k in FAR_FIRST:
            send(tile, tile, sem.at[0], sem.at[1], on_first(k))

    def steps_2(buf, sem):
        wait_for(buf.at[pl.ds(0, RING - 1)], sem.at[1])
        row = buf.at[row_of(0)]
        for k in FAR_FIRST:
            send(row, row, sem.at[0], sem.at[2], on_second(k))

    def steps_3(buf, sem):
        wait_for(buf.at[pl.ds(0, HALF - RING)], sem.at[2])
        half = buf.at[pl.ds(core * HALF, HALF)]
        send(half, half, sem.at[0], sem.at[3], partner)

    def steps_4(buf, sem):
        wait_for(buf.at[pl.ds((1 - core) * HALF, HALF)], sem.at[3])

    rows_load.wait()
    head_row = lax.broadcasted_iota(jnp.int32, (HEADS, d_model), 0)
    head_of_lane = lax.broadcasted_iota(jnp.int32, (HEADS, d_model), 1) // HEAD_DIM
    own_head = head_row == head_of_lane
    scale = 1.0 / math.sqrt(HEAD_DIM)

    def spread(ref):
        return jnp.broadcast_to(ref[...].astype(F32), (HEADS, d_model))

    hid_tile = diagonal(spread(hid_v))
    hid[pl.ds(me, 1)] = hid_tile.astype(BF16)[None]
    query = jnp.where(own_head, spread(query_v), 0.0)
    own_score = jnp.sum(query * spread(key_v), axis=1, keepdims=True) * scale
    query = query.astype(BF16)
    k_load.wait()
    len_load.wait()
    scores = dot_nt(query, k_v[...]) * scale
    position = lax.broadcasted_iota(jnp.int32, scores.shape, 1)
    scores = jnp.where(position < jnp.broadcast_to(len_v[...], scores.shape), scores, -1e30)
    top = jnp.maximum(jnp.max(scores, axis=1, keepdims=True), own_score)
    weights = jnp.exp(scores - top)
    own_weight = jnp.exp(own_score - top)
    normalizer = jnp.sum(weights, axis=1, keepdims=True) + own_weight
    weights = (weights / normalizer).astype(BF16)
    own_weight = (own_weight / normalizer).astype(BF16).astype(F32)
    v_load.wait()
    mixed = dot(weights, v_v[...]) + own_weight * spread(value_v)
    att[pl.ds(me, 1)] = diagonal(mixed).astype(BF16)[None]

    pl.semaphore_wait(barrier, (2 + (1 - core)) * (RING - 1) + 1)
    tiles_1(att, att_sem)
    steps_1(hid, hid_sem)

    gain_load.wait()
    for h in range(HEADS):
        block = gain_v[h : h + 1, :].astype(F32)
        gain_b[h * HEAD_DIM : (h + 1) * HEAD_DIM, :] = jnp.broadcast_to(
            block, (HEAD_DIM, TOKENS)
        ).T
    rt_load.wait()
    nat_id = lax.broadcasted_iota(jnp.int32, (TOKENS, TOKENS), 0)
    lane = lax.broadcasted_iota(jnp.int32, (TOKENS, TOKENS), 1)
    lane_core, lane_second, lane_first = lane // HALF, (lane // RING) % RING, lane % RING
    lane_x = lane_first * (1 - lane_core) + lane_second * lane_core
    lane_y = lane_second * (1 - lane_core) + lane_first * lane_core
    to_slot = (nat_id == (lane_x * RING + lane_y) * 2 + lane_core).astype(BF16)
    routes = dot(
        jnp.broadcast_to(rt_v[...], (8, TOKENS)).astype(F32).astype(BF16), to_slot
    )[0:1].astype(jnp.int32)
    device = (x * RING + y) * 2 + core
    mine = device * ins[13].shape[1] // FF
    member = routes == mine
    rank = dot(
        jnp.broadcast_to(member.astype(F32), (8, TOKENS)).astype(BF16), (nat_id <= lane).astype(BF16)
    )[0:1].astype(jnp.int32) - 1
    slot_id = lax.broadcasted_iota(jnp.int32, (slots, TOKENS), 0)
    placed = jnp.where(
        jnp.broadcast_to(member, (slots, TOKENS))
        & (jnp.broadcast_to(rank, (slots, TOKENS)) == slot_id),
        1.0,
        0.0,
    )
    placed_at, depth = 2 * shared_units, lhs.shape[0]
    lhs[placed_at : placed_at + slots, :] = placed.astype(BF16)
    lhs[placed_at + slots :, :] = placed.astype(BF16)
    down_load.wait()
    send(
        rhs.at[pl.ds(0, shared_units)], rhs.at[pl.ds(shared_units, shared_units)], down_sem.at[0],
        down_sem.at[1], partner,
    )

    @pl.when(core == 0)
    def _():
        eup_load.wait()
        send(
            eup_v.at[:, pl.ds(kept, moved)], eup_v.at[:, pl.ds(units, moved)], units_sem.at[0],
            units_sem.at[1], partner,
        )
        edn_load.wait()
        send(
            edn_v.at[pl.ds(kept, moved)], edn_v.at[pl.ds(units, moved)], units_sem.at[2],
            units_sem.at[3], partner,
        )

    up_load.wait()
    send(
        up_t.at[pl.ds(0, shared_units)], up_t.at[pl.ds(shared_units, shared_units)], up_sem.at[0],
        up_sem.at[1], partner,
    )

    late_x = zero_last(x)
    tiles_2(
        att, att_sem,
        [(1, k) for k in zero_last(y)] + [(0, k) for k in late_x[:-1] + [OWN] + late_x[-1:]],
    )
    tiles_3(att, att_sem, 1)

    def projected(at):
        every = pl.ds(at * HEADS, HALF * HEADS)
        big[every, :] = att[pl.ds(at, HALF)].reshape(HALF * HEADS, HEAD_DIM).astype(F32)
        for h in range(HEADS):
            nat[:, h * HEAD_DIM : (h + 1) * HEAD_DIM] = big[
                pl.ds(at * HEADS + h, HALF, stride=HEADS), :
            ].astype(BF16)
        return dot_nt(wo_t[...], nat[...])

    wo_load.wait()
    half_1 = projected(HALF)
    tiles_3(att, att_sem, 0)
    half_0 = projected(0)
    pro[me] = jnp.concatenate([half_0, half_1], axis=1).astype(BF16)
    tiles_1(pro, pro_sem)
    steps_2(hid, hid_sem)
    tiles_2(pro, pro_sem, [(0, OWN)] + [(color, k) for k in NEAR_FIRST for color in (1, 0)])
    steps_3(hid, hid_sem)
    steps_4(hid, hid_sem)
    big[...] = hid[...].reshape(TOKENS * HEADS, HEAD_DIM).astype(F32)
    for h in range(HEADS):
        hid_t[h * HEAD_DIM : (h + 1) * HEAD_DIM, :] = big[pl.ds(h, TOKENS, stride=HEADS), :].T
    tiles_3(pro, pro_sem, 1)
    tiles_3(pro, pro_sem, 0)

    cols = wo_t.shape[0]
    total = jnp.zeros((cols, TOKENS), F32)
    for n in range(TOKENS):
        n_core, n_y, n_x = n % 2, (n // 2) % RING, n // (2 * RING)
        slot = n_core * HALF + (n_x * RING + n_y if n_core else n_y * RING + n_x)
        rows = slice(n * cols, (n + 1) * cols)
        block = pro[slot]
        proj_n[rows, :] = block
        block = hid_t[rows, :] + block.astype(F32)
        res[rows, :] = block
        total = total + block
    mean = jnp.sum(total, axis=0, keepdims=True) / d_model
    total = jnp.zeros((HEAD_DIM, TOKENS), F32)
    for h in range(HEADS):
        centered = res[h * HEAD_DIM : (h + 1) * HEAD_DIM, :] - mean
        total = total + centered * centered
    variance = jnp.sum(total, axis=0, keepdims=True) / d_model
    inverse = 1.0 / jnp.sqrt(jnp.maximum(variance, 0.25))
    for h in range(HEADS):
        rows = slice(h * HEAD_DIM, (h + 1) * HEAD_DIM)
        norm_t[rows, :] = ((res[rows, :] - mean) * inverse * gain_b[rows, :]).astype(BF16)

    normed = norm_t[...]
    picked = dot_nt(placed.astype(BF16), normed).astype(BF16)
    logits = dot(up_t[2 * shared_units :, :], normed)
    expert_row = lax.broadcasted_iota(jnp.int32, (experts, TOKENS), 0)
    chosen = jnp.sum(
        jnp.where(jnp.broadcast_to(routes, (experts, TOKENS)) == expert_row, logits, 0.0),
        axis=0,
        keepdims=True,
    )
    gate = 1.0 / (1.0 + jnp.exp(-chosen))
    slot_gate = jnp.sum(placed * gate, axis=1, keepdims=True)
    wide = d_model // PIECES
    theirs = placed_at + slots

    def expert(count):
        inner = jax.nn.gelu(dot(picked, eup_v[:, 0:count]), approximate=True).astype(BF16)
        for i in range(PIECES):
            at = i * wide
            result = dot(inner, edn_v[0:count, at : at + wide])
            rhs[placed_at:theirs, at : at + wide] = (result * slot_gate).astype(BF16)
            send(
                rhs.at[pl.ds(placed_at, slots), pl.ds(at, wide)],
                rhs.at[pl.ds(theirs, slots), pl.ds(at, wide)],
                slot_sem.at[0], slot_sem.at[1 + i], partner,
            )

    @pl.when(core == 0)
    def _():
        expert(kept)

    @pl.when(core == 1)
    def _():
        eup_load.wait()
        edn_load.wait()
        wait_for(eup_v.at[:, pl.ds(0, moved)], units_sem.at[1])
        wait_for(edn_v.at[pl.ds(0, moved)], units_sem.at[3])
        expert(units + moved)

    wait_for(rhs.at[pl.ds(0, shared_units)], down_sem.at[1])
    wait_for(up_t.at[pl.ds(0, shared_units)], up_sem.at[1])
    both = dot(up_t[0 : 2 * shared_units, :], normed)
    lhs[0 : 2 * shared_units, :] = jax.nn.gelu(both, approximate=True).astype(BF16)
    chosen_half = (
        lax.broadcasted_iota(jnp.int32, (HALF, TOKENS), 1)
        == lax.broadcasted_iota(jnp.int32, (HALF, TOKENS), 0) + core * HALF
    ).astype(BF16)
    left = dot_nt(chosen_half, lhs[...]).astype(BF16)
    for i in range(PIECES):
        columns = pl.ds(i * wide, wide)
        wait_for(rhs.at[pl.ds(theirs, slots), columns], slot_sem.at[1 + i])
        for at in range(i * wide, (i + 1) * wide, 256):
            piece = dot(left, rhs[:, at : at + 256]).astype(BF16)
            p_send[:, :, at : at + 256] = piece.reshape(RING, RING, 256)
        for k in FAR_FIRST:
            block = p_send.at[(second + k) % RING, :, columns]
            send(block, p_recv.at[k - 1, :, columns], p_sem.at[0], p_sem.at[1], on_second(k))
    summed = p_send[second].astype(F32)
    own_column = (
        lax.broadcasted_iota(jnp.int32, (HEADS, TOKENS), 1) == me
    ).astype(BF16)
    own = hid_tile + diagonal(dot_nt(own_column, proj_n[...]))
    wait_for(p_recv, p_sem.at[1])
    for k in range(RING - 1):
        summed = summed + p_recv[k].astype(F32)
    for h in range(HEADS):
        tok[pl.ds(h, RING, stride=HEADS), :] = summed[:, h * HEAD_DIM : (h + 1) * HEAD_DIM]
    for k in FAR_FIRST:
        to = pl.multiple_of(((first + k) % RING) * HEADS, HEADS)
        send(tok.at[pl.ds(to, HEADS)], t_recv.at[k - 1], t_sem.at[0], t_sem.at[1], on_first(k))
    own = own + tok[pl.ds(pl.multiple_of(first * HEADS, HEADS), HEADS), :]
    wait_for(t_recv, t_sem.at[1])
    for k in range(RING - 1):
        own = own + t_recv[k]
    for h in range(HEADS):
        out_ref[:, h * HEAD_DIM : (h + 1) * HEAD_DIM] = own[h : h + 1, :].astype(BF16)
    @pl.when(core == 0)
    def _():
        wait_for(eup_v.at[:, pl.ds(0, moved)], units_sem.at[0])
        wait_for(edn_v.at[pl.ds(0, moved)], units_sem.at[2])

    tiles_sent(att, att_sem)
    wait_for(hid.at[pl.ds(0, TOKENS - 1)], hid_sem.at[0])
    tiles_sent(pro, pro_sem)
    wait_for(rhs.at[pl.ds(0, shared_units)], down_sem.at[0])
    wait_for(up_t.at[pl.ds(0, shared_units)], up_sem.at[0])
    wait_for(rhs.at[pl.ds(placed_at, slots)], slot_sem.at[0])
    wait_for(p_recv, p_sem.at[0])
    wait_for(t_recv, t_sem.at[0])


def body(
    query, key_new, value_new, key_cache, value_cache, lengths, hidden, routes, w_out, ln_gain,
    router, shared_up, shared_down, expert_up, expert_down,
):
    key_cache = key_cache.reshape(key_cache.shape[1:])
    value_cache = value_cache.reshape(value_cache.shape[1:])
    lengths = lengths.reshape(1, 1)
    routes = routes.reshape(1, -1)
    ln_gain = ln_gain.reshape(-1, HEAD_DIM)
    w_out, router, shared_up = w_out.T, router.T, shared_up.T
    args = (
        query, key_new, value_new, key_cache, value_cache, lengths, hidden, routes, w_out, ln_gain,
        router, shared_up, shared_down, expert_up, expert_down,
    )
    d = query.shape[1]
    units = shared_up.shape[0]
    wide_units = 2 * expert_up.shape[1] - expert_up.shape[1] // KEPT
    slots = TOKENS * 4 // 32
    tile = (TOKENS, HEADS, HEAD_DIM)

    def own(a):
        return pltpu.VMEM(a.shape, a.dtype)

    dma = pltpu.SemaphoreType.DMA
    scratch = [
        pltpu.VMEM((4, 1, d), BF16),
        own(key_cache),
        own(value_cache),
        own(lengths),
        own(routes),
        own(w_out),
        own(ln_gain),
        pltpu.VMEM((2 * units + router.shape[0], d), BF16),
        pltpu.VMEM((2 * (units + slots), d), BF16),
        pltpu.VMEM((d, wide_units), BF16),
        pltpu.VMEM((wide_units, d), BF16),
        pltpu.VMEM(tile, BF16),
        pltpu.VMEM(tile, BF16),
        pltpu.VMEM((TOKENS, w_out.shape[0], TOKENS), BF16),
        pltpu.VMEM((TOKENS * HEADS, HEAD_DIM), F32),
        pltpu.VMEM((d, TOKENS), F32),
        pltpu.VMEM((d, TOKENS), F32),
        pltpu.VMEM((HALF, d), BF16),
        pltpu.VMEM((d, TOKENS), F32),
        pltpu.VMEM((d, TOKENS), BF16),
        pltpu.VMEM((d, TOKENS), BF16),
        pltpu.VMEM((RING, RING, d), BF16),
        pltpu.VMEM((RING - 1, RING, d), BF16),
        pltpu.VMEM((RING * HEADS, HEAD_DIM), F32),
        pltpu.VMEM((RING - 1, HEADS, HEAD_DIM), F32),
        pltpu.VMEM((2 * (units + slots), TOKENS), BF16),
    ]
    scratch += [dma((n,)) for n in (11, 27, 4, 27, 2, 2, 1 + PIECES, 2, 2, 4)]
    return pl.pallas_call(
        kernel,
        out_shape=pltpu.VMEM((1, d), BF16),
        in_specs=[pl.BlockSpec(memory_space=pl.ANY)] * 15,
        out_specs=pl.BlockSpec(memory_space=pltpu.VMEM),
        scratch_shapes=scratch,
        compiler_params=pltpu.CompilerParams(collective_id=0, has_side_effects=True),
        name="decode_layer",
    )(*args)


def solution(mesh):
    torus = Mesh(
        mesh.devices.reshape(mesh.shape["group"], RING, RING, 2),
        ("group", "expert_0", "expert_1", "expert_2"),
    )
    placed = (
        P(GROUP_EXPERT, None),
        P(GROUP_EXPERT, None),
        P(GROUP_EXPERT, None),
        P(GROUP_EXPERT, None, None),
        P(GROUP_EXPERT, None, None),
        P(GROUP_EXPERT),
        P(GROUP_EXPERT, None),
        P("group"),
        P(None, EXPERT),
        P(),
        P(),
        P(None, EXPERT),
        P(EXPERT, None),
        P(None, EXPERT),
        P(EXPERT, None),
    )
    return jax.shard_map(
        body, mesh=torus, in_specs=placed, out_specs=P(GROUP_EXPERT, None), check_vma=False
    )
```
